16 devices in a mesh: tp: 2 (over z), dp: 8 (over y, x, core).
Axes of the slice: x: 2, y: 2, z: 2, core: 2. Of those that a mesh axis runs over, the one named last changes fastest.
Arguments:
- x_in: bfloat16 [128, 3072], P(('dp', 'tp'))
- w_gate: bfloat16 [3072, 24576], P('dp', 'tp')
- w_up: bfloat16 [3072, 24576], P('dp', 'tp')
- w_down: bfloat16 [24576, 3072], P('tp', 'dp')
- grad_y: bfloat16 [128, 3072], P(('dp', 'tp'))
Outputs:
- output 1: bfloat16 [128, 3072], P(('dp', 'tp'))
- output 2: bfloat16 [128, 3072], P(('dp', 'tp'))
- output 3: float32 [3072, 24576], P('dp', 'tp')
- output 4: float32 [3072, 24576], P('dp', 'tp')
- output 5: float32 [24576, 3072], P('tp', 'dp')
All inputs are finite; a program needn't handle non-finite values.
Results may differ from the reference program's by a relative error of at most 0.0018.
Values are sent between devices in bfloat16 or wider.
A program may use at most 1 GiB of HBM per device.

```python
import jax
import jax.numpy as jnp

D = 3072
FF = 24576
TOKENS = 128


def setup_inputs(seed: int = 0) -> dict:
    base_key = jax.random.key(seed)
    key_list = jax.random.split(base_key, 5)
    x_in = jax.random.normal(key_list[0], (TOKENS, D), jnp.float32).astype(jnp.bfloat16)
    w_gate = (jax.random.normal(key_list[1], (D, FF), jnp.float32) * D ** -0.5).astype(jnp.bfloat16)
    w_up = (jax.random.normal(key_list[2], (D, FF), jnp.float32) * D ** -0.5).astype(jnp.bfloat16)
    w_down = (jax.random.normal(key_list[3], (FF, D), jnp.float32) * FF ** -0.5).astype(jnp.bfloat16)
    grad_y = jax.random.normal(key_list[4], (TOKENS, D), jnp.float32).astype(jnp.bfloat16)
    return {"x_in": x_in, "w_gate": w_gate, "w_up": w_up, "w_down": w_down, "grad_y": grad_y}


def reference(x_in, w_gate, w_up, w_down, grad_y):
    gate_pre = jnp.dot(x_in, w_gate, preferred_element_type=jnp.float32)
    up_pre = jnp.dot(x_in, w_up, preferred_element_type=jnp.float32)
    sig_gate = jax.nn.sigmoid(gate_pre)
    silu_gate = gate_pre * sig_gate
    hidden = (silu_gate * up_pre).astype(jnp.bfloat16)
    y_out = (x_in.astype(jnp.float32) + jnp.dot(hidden, w_down, preferred_element_type=jnp.float32)).astype(jnp.bfloat16)
    grad_h = jnp.dot(grad_y, w_down.T, preferred_element_type=jnp.float32)
    silu_deriv = sig_gate * (1.0 + gate_pre * (1.0 - sig_gate))
    grad_gate = (grad_h * up_pre * silu_deriv).astype(jnp.bfloat16)
    grad_up = (grad_h * silu_gate).astype(jnp.bfloat16)
    grad_x = (grad_y.astype(jnp.float32)
              + jnp.dot(grad_gate, w_gate.T, preferred_element_type=jnp.float32)
              + jnp.dot(grad_up, w_up.T, preferred_element_type=jnp.float32)).astype(jnp.bfloat16)
    grad_w_gate = jnp.dot(x_in.T, grad_gate, preferred_element_type=jnp.float32)
    grad_w_up = jnp.dot(x_in.T, grad_up, preferred_element_type=jnp.float32)
    grad_w_down = jnp.dot(hidden.T, grad_y, preferred_element_type=jnp.float32)
    return (y_out, grad_x, grad_w_gate, grad_w_up, grad_w_down)
```

```python
import functools

import jax
import jax.numpy as jnp
from jax import lax
from jax.experimental import pallas as pl
from jax.experimental.pallas import tpu as pltpu
from jax.sharding import PartitionSpec as P

MESH = pl.DeviceIdType.MESH
BF = jnp.bfloat16
F32 = jnp.float32

D = 3072
FF_LOC = 12288
DL = 384
NP = 8
FC = FF_LOC // (2 * NP)
NSUB = 256


def _dot(a, b, ca, cb):
    return lax.dot_general(a, b, (((ca,), (cb,)), ((), ())), preferred_element_type=F32)


def comm_kernel(x_ref, gy_ref, wg_hbm, wu_hbm, wd_hbm,
                y_ref, gx_ref, xs_ref, g_hbm,
                wg, wu, wd, xin, part, rd, r2, r3, gat, acc, rz, ob, orx,
                w_sem, x_send, x_recv, d_send, d_recv, s2_send, s2_recv, s3_send, s3_recv,
                s4_send, s4_recv, s5_send, s5_recv, s6_send, s6_recv, g_sem,
                z_send, z_recv, o_send, o_recv):
    tp = lax.axis_index("tp")
    dp = lax.axis_index("dp")
    c = lax.rem(dp, 2)
    mx = lax.rem(dp // 2, 2)
    my = dp // 4

    def dpi(cc, yy, xx):
        return yy * 4 + xx * 2 + cc

    core_nb = (tp, dpi(1 - c, my, mx))
    x_nb = (tp, dpi(c, my, 1 - mx))
    y_nb = (tp, dpi(c, 1 - my, mx))
    z_nb = (1 - tp, dp)

    def w_copies(p):
        cols = pl.ds(pl.multiple_of(p * 2 * FC, 2 * FC), 2 * FC)
        return (pltpu.make_async_copy(wg_hbm.at[:, cols], wg.at[p], w_sem.at[0, p]),
                pltpu.make_async_copy(wu_hbm.at[:, cols], wu.at[p], w_sem.at[1, p]),
                pltpu.make_async_copy(wd_hbm.at[cols, :], wd.at[p], w_sem.at[2, p]))

    @pl.loop(0, NP)
    def _(p):
        for cp in w_copies(p):
            cp.start()

    barrier = pltpu.get_barrier_semaphore()
    me = tp * 8 + dp

    @pl.loop(1, 16)
    def _(k):
        o = lax.rem(me + k, 16)
        pl.semaphore_signal(barrier, inc=1, device_id=(o // 8, lax.rem(o, 8)), device_id_type=MESH)
    pl.semaphore_wait(barrier, 15)

    def blk(tt, dd):
        return (lax.rem(dd, 2) * 4 + (dd // 4) * 2 + lax.rem(dd // 2, 2)) * 2 + tt

    def x_copy(k, j):
        o = lax.rem(me + k, 16)
        ot, od = o // 8, lax.rem(o, 8)
        src = (x_ref, gy_ref)[j].at[:, pl.ds(pl.multiple_of(od * DL, DL), DL)]
        return pltpu.make_async_remote_copy(
            src_ref=src, dst_ref=xin.at[blk(tp, dp), j], send_sem=x_send.at[k, j],
            recv_sem=x_recv.at[blk(tp, dp), j], device_id=(ot, od), device_id_type=MESH)

    def x_wait(k, j):
        o = lax.rem(me + k, 16)
        ot, od = o // 8, lax.rem(o, 8)
        return pltpu.make_async_remote_copy(
            src_ref=x_ref.at[:, pl.ds(0, DL)], dst_ref=xin.at[blk(ot, od), j], send_sem=x_send.at[k, j],
            recv_sem=x_recv.at[blk(ot, od), j], device_id=(ot, od), device_id_type=MESH)

    @pl.loop(1, 16)
    def _(k):
        for j in range(2):
            x_copy(k, j).start()

    mine = blk(tp, dp)
    own = pl.ds(pl.multiple_of(dp * DL, DL), DL)
    xin[mine, 0] = x_ref[:, own]
    xin[mine, 1] = gy_ref[:, own]
    acc[...] = jnp.zeros_like(acc)

    @pl.loop(1, 16)
    def _(k):
        for j in range(2):
            x_wait(k, j).wait_recv()

    for j in range(2):
        xs_ref[j] = xin[:, j].astype(F32).reshape(128, DL).astype(BF)

    def d_copy(p):
        s = lax.rem(p, 2)
        return pltpu.make_async_remote_copy(
            src_ref=part.at[s, 1 - c], dst_ref=rd.at[p], send_sem=d_send.at[p], recv_sem=d_recv.at[p],
            device_id=core_nb, device_id_type=MESH)

    def s2_copies(p):
        return (pltpu.make_async_remote_copy(
                    src_ref=rd.at[p, 0, :, :, 1 - mx], dst_ref=r2.at[p, 0], send_sem=s2_send.at[0, p],
                    recv_sem=s2_recv.at[0, p], device_id=x_nb, device_id_type=MESH),
                pltpu.make_async_remote_copy(
                    src_ref=rd.at[p, 1, :, 1 - my], dst_ref=r2.at[p, 1], send_sem=s2_send.at[1, p],
                    recv_sem=s2_recv.at[1, p], device_id=y_nb, device_id_type=MESH))

    def s3_copies(p):
        return (pltpu.make_async_remote_copy(
                    src_ref=r2.at[p, 0, :, 1 - my], dst_ref=r3.at[p, 0], send_sem=s3_send.at[0, p],
                    recv_sem=s3_recv.at[0, p], device_id=y_nb, device_id_type=MESH),
                pltpu.make_async_remote_copy(
                    src_ref=r2.at[p, 1, :, 1 - mx], dst_ref=r3.at[p, 1], send_sem=s3_send.at[1, p],
                    recv_sem=s3_recv.at[1, p], device_id=x_nb, device_id_type=MESH))

    def s4_copies(p, yy0, xx1):
        return (pltpu.make_async_remote_copy(
                    src_ref=gat.at[p, 0, c, yy0, mx], dst_ref=gat.at[p, 0, c, yy0, mx],
                    send_sem=s4_send.at[0, p], recv_sem=s4_recv.at[0, p], device_id=y_nb, device_id_type=MESH),
                pltpu.make_async_remote_copy(
                    src_ref=gat.at[p, 1, c, my, xx1], dst_ref=gat.at[p, 1, c, my, xx1],
                    send_sem=s4_send.at[1, p], recv_sem=s4_recv.at[1, p], device_id=x_nb, device_id_type=MESH))

    def s5_copies(p, xx0, yy1):
        return (pltpu.make_async_remote_copy(
                    src_ref=gat.at[p, 0, c, :, xx0], dst_ref=gat.at[p, 0, c, :, xx0],
                    send_sem=s5_send.at[0, p], recv_sem=s5_recv.at[0, p], device_id=x_nb, device_id_type=MESH),
                pltpu.make_async_remote_copy(
                    src_ref=gat.at[p, 1, c, yy1], dst_ref=gat.at[p, 1, c, yy1],
                    send_sem=s5_send.at[1, p], recv_sem=s5_recv.at[1, p], device_id=y_nb, device_id_type=MESH))

    def s6_copy(p, cc):
        return pltpu.make_async_remote_copy(
            src_ref=gat.at[p, :, cc], dst_ref=gat.at[p, :, cc], send_sem=s6_send.at[p],
            recv_sem=s6_recv.at[p], device_id=core_nb, device_id_type=MESH)

    def g_copy(p):
        return pltpu.make_async_copy(gat.at[p], g_hbm.at[p], g_sem.at[p])

    def products(p):
        s = lax.rem(p, 2)
        for cp in w_copies(p):
            cp.wait()

        @pl.when(p >= 2)
        def _():
            d_copy(p - 2).wait_send()

        for ab in range(2):
            for n in range(FC // NSUB):
                lo = ab * FC + n * NSUB
                cols = pl.ds(lo, NSUB)
                dst = pl.ds(n * NSUB, NSUB)
                vals = (_dot(xs_ref[0], wg[p, :, cols], 1, 0),
                        _dot(xs_ref[0], wu[p, :, cols], 1, 0),
                        _dot(xs_ref[1], wd[p, cols, :], 1, 1))
                for t in range(3):
                    v = vals[t].reshape(2, 2, 2, 16, NSUB)
                    for cc in range(2):
                        part[s, cc, ab, t, :, :, :, dst] = v[cc]
        d_copy(p).start()

    def stage2(p):
        s = lax.rem(p, 2)
        d_copy(p).wait_recv()
        for ab in range(2):
            for t in range(3):
                rd[p, ab, t] = rd[p, ab, t] + part[s, c, ab, t]
        for cp in s2_copies(p):
            cp.start()

    def stage3(p):
        for cp in s2_copies(p):
            cp.wait_recv()
        for t in range(3):
            r2[p, 0, t] = r2[p, 0, t] + rd[p, 0, t, :, mx]
            r2[p, 1, t] = r2[p, 1, t] + rd[p, 1, t, my]
        for cp in s3_copies(p):
            cp.start()

    def stage4(p):
        for cp in s3_copies(p):
            cp.wait_recv()
        for ab in range(2):
            keep = my if ab == 0 else mx
            a = r3[p, ab, 0] + r2[p, ab, 0, keep]
            b = r3[p, ab, 1] + r2[p, ab, 1, keep]
            g = r3[p, ab, 2] + r2[p, ab, 2, keep]
            s = jax.nn.sigmoid(a)
            silu = a * s
            gat[p, ab, c, my, mx, 0] = (silu * b).astype(BF)
            gat[p, ab, c, my, mx, 1] = (g * b * (s * (1.0 + a * (1.0 - s)))).astype(BF)
            gat[p, ab, c, my, mx, 2] = (g * silu).astype(BF)
        for cp in s4_copies(p, my, mx):
            cp.start()

    def stage5(p):
        for cp in s4_copies(p, 1 - my, 1 - mx):
            cp.wait_recv()
        for cp in s5_copies(p, mx, my):
            cp.start()

    def stage6(p):
        for cp in s5_copies(p, 1 - mx, 1 - my):
            cp.wait_recv()
        s6_copy(p, c).start()

    def stage7(p):
        s6_copy(p, 1 - c).wait_recv()
        g_copy(p).start()
        for ab in range(2):
            cols = pl.ds(ab * FC, FC)
            h = gat[p, ab, :, :, :, 0].reshape(128, FC)
            acc[0] = acc[0] + _dot(h, wd[p, cols, :], 1, 0)
            da = gat[p, ab, :, :, :, 1].reshape(128, FC)
            db = gat[p, ab, :, :, :, 2].reshape(128, FC)
            acc[1] = acc[1] + (_dot(da, wg[p, :, cols], 1, 1) + _dot(db, wu[p, :, cols], 1, 1))

    products(0)

    @pl.loop(0, NP + 5)
    def _(i):
        pl.when(i < NP)(lambda: stage2(i))
        pl.when((i >= 1) & (i < NP + 1))(lambda: stage3(i - 1))
        pl.when((i >= 2) & (i < NP + 2))(lambda: stage4(i - 2))
        pl.when((i >= 3) & (i < NP + 3))(lambda: stage5(i - 3))
        pl.when((i >= 4) & (i < NP + 4))(lambda: stage6(i - 4))
        pl.when(i < NP - 1)(lambda: products(i + 1))
        pl.when(i >= 5)(lambda: stage7(i - 5))

    accv = acc.reshape(2, 8, 2, 8, DL)
    zc = pltpu.make_async_remote_copy(
        src_ref=accv.at[:, :, 1 - tp], dst_ref=rz, send_sem=z_send, recv_sem=z_recv,
        device_id=z_nb, device_id_type=MESH)
    zc.start()
    zc.wait_recv()
    for q in range(8):
        for j in range(2):
            tot = accv[j, q, tp] + rz[j, q] + xin[2 * q + tp, j].astype(F32)
            ob[q, j] = tot.astype(BF)

    def q_of(dd):
        return lax.rem(dd, 2) * 4 + (dd // 4) * 2 + lax.rem(dd // 2, 2)

    def o_copy(k, src_dp):
        od = lax.rem(dp + k, 8)
        return pltpu.make_async_remote_copy(
            src_ref=ob.at[q_of(od)], dst_ref=orx.at[src_dp], send_sem=o_send.at[k],
            recv_sem=o_recv.at[src_dp], device_id=(tp, od), device_id_type=MESH)

    @pl.loop(1, 8)
    def _(k):
        o_copy(k, dp).start()

    orx[dp] = ob[q_of(dp)]

    @pl.loop(0, NP)
    def _(p):
        for cp in (*s2_copies(p), *s3_copies(p), *s4_copies(p, my, mx), *s5_copies(p, mx, my), s6_copy(p, c)):
            cp.wait_send()
        g_copy(p).wait()
    for p in (NP - 2, NP - 1):
        d_copy(p).wait_send()

    @pl.loop(1, 16)
    def _(k):
        for j in range(2):
            x_copy(k, j).wait_send()
    zc.wait_send()

    @pl.loop(1, 8)
    def _(k):
        o_copy(k, lax.rem(dp + k, 8)).wait_recv()

    for dd in range(8):
        y_ref[:, dd * DL:(dd + 1) * DL] = orx[dd, 0]
        gx_ref[:, dd * DL:(dd + 1) * DL] = orx[dd, 1]

    @pl.loop(1, 8)
    def _(k):
        o_copy(k, dp).wait_send()


def wgrad_kernel(xs_ref, g_ref, dwg_ref, dwu_ref, dwd_ref):
    h = g_ref[0, 0, :, :, :, 0].reshape(128, FC)
    da = g_ref[0, 0, :, :, :, 1].reshape(128, FC)
    db = g_ref[0, 0, :, :, :, 2].reshape(128, FC)
    dwg_ref[...] = _dot(xs_ref[0], da, 0, 0)
    dwu_ref[...] = _dot(xs_ref[0], db, 0, 0)
    dwd_ref[...] = _dot(h, xs_ref[1], 0, 0)


def local_step(x_loc, wg_loc, wu_loc, wd_loc, gy_loc):
    vm = pl.BlockSpec(memory_space=pltpu.VMEM)
    hb = pl.BlockSpec(memory_space=pl.ANY)
    dma = pltpu.SemaphoreType.DMA
    y_rows, gx_rows, xs, gathered = pl.pallas_call(
        comm_kernel,
        out_shape=(jax.ShapeDtypeStruct((8, D), BF), jax.ShapeDtypeStruct((8, D), BF),
                   jax.ShapeDtypeStruct((2, 128, DL), BF),
                   jax.ShapeDtypeStruct((NP, 2, 2, 2, 2, 3, 16, FC), BF)),
        in_specs=[vm, vm, hb, hb, hb],
        out_specs=(vm, vm, vm, hb),
        scratch_shapes=[
            pltpu.VMEM((NP, DL, 2 * FC), BF),
            pltpu.VMEM((NP, DL, 2 * FC), BF),
            pltpu.VMEM((NP, 2 * FC, DL), BF),
            pltpu.VMEM((16, 2, 8, DL), BF),
            pltpu.VMEM((2, 2, 2, 3, 2, 2, 16, FC), F32),
            pltpu.VMEM((NP, 2, 3, 2, 2, 16, FC), F32),
            pltpu.VMEM((NP, 2, 3, 2, 16, FC), F32),
            pltpu.VMEM((NP, 2, 3, 16, FC), F32),
            pltpu.VMEM((NP, 2, 2, 2, 2, 3, 16, FC), BF),
            pltpu.VMEM((2, 128, DL), F32),
            pltpu.VMEM((2, 8, 8, DL), F32),
            pltpu.VMEM((8, 2, 8, DL), BF),
            pltpu.VMEM((8, 2, 8, DL), BF),
            dma((3, NP)), dma((16, 2)), dma((16, 2)), dma((NP,)), dma((NP,)),
            dma((2, NP)), dma((2, NP)), dma((2, NP)), dma((2, NP)),
            dma((2, NP)), dma((2, NP)), dma((2, NP)), dma((2, NP)),
            dma((NP,)), dma((NP,)), dma((NP,)),
            dma(()), dma(()), dma((8,)), dma((8,)),
        ],
        compiler_params=pltpu.CompilerParams(
            collective_id=0, has_side_effects=True, vmem_limit_bytes=60 * 1024 * 1024),
        name="mlp_comm",
    )(x_loc, gy_loc, wg_loc, wu_loc, wd_loc)

    grad_wg, grad_wu, grad_wd = pl.pallas_call(
        wgrad_kernel,
        grid=(2 * NP,),
        out_shape=(jax.ShapeDtypeStruct((DL, FF_LOC), F32), jax.ShapeDtypeStruct((DL, FF_LOC), F32),
                   jax.ShapeDtypeStruct((FF_LOC, DL), F32)),
        in_specs=[pl.BlockSpec((2, 128, DL), lambda k: (0, 0, 0)),
                  pl.BlockSpec((1, 1, 2, 2, 2, 3, 16, FC), lambda k: (k // 2, lax.rem(k, 2), 0, 0, 0, 0, 0, 0))],
        out_specs=(pl.BlockSpec((DL, FC), lambda k: (0, k)), pl.BlockSpec((DL, FC), lambda k: (0, k)),
                   pl.BlockSpec((FC, DL), lambda k: (k, 0))),
        compiler_params=pltpu.CompilerParams(dimension_semantics=("arbitrary",), vmem_limit_bytes=48 * 1024 * 1024),
        name="mlp_wgrad",
    )(xs, gathered)
    return y_rows, gx_rows, grad_wg, grad_wu, grad_wd


def solution(mesh):
    row_spec = P(("dp", "tp"), None)
    up_spec = P("dp", "tp")
    down_spec = P("tp", "dp")
    return jax.shard_map(local_step, mesh=mesh,
                         in_specs=(row_spec, up_spec, up_spec, down_spec, row_spec),
                         out_specs=(row_spec, row_spec, up_spec, up_spec, down_spec),
                         check_vma=False)
```

```python
import functools

import jax
import jax.numpy as jnp
from jax import lax
from jax.experimental import pallas as pl
from jax.experimental.pallas import tpu as pltpu
from jax.sharding import PartitionSpec as P

MESH = pl.DeviceIdType.MESH
BF = jnp.bfloat16
F32 = jnp.float32

D = 3072
FF_LOC = 12288
DL = 384
NP = 16
FC = FF_LOC // (2 * NP)
NSUB = 384


def _dot(a, b, ca, cb):
    return lax.dot_general(a, b, (((ca,), (cb,)), ((), ())), preferred_element_type=F32)


def comm_kernel(x_ref, gy_ref, wg_hbm, wu_hbm, wd_hbm,
                y_ref, gx_ref, xs_ref, g_hbm,
                wg, wu, wd, xin, part, rd, r2, r3, gat, acc, rz, ob, orx,
                w_sem, x_send, x_recv, d_send, d_recv, s2_send, s2_recv, s3_send, s3_recv,
                s4_send, s4_recv, s5_send, s5_recv, s6_send, s6_recv, g_sem,
                z_send, z_recv, o_send, o_recv):
    tp = lax.axis_index("tp")
    dp = lax.axis_index("dp")
    c = lax.rem(dp, 2)
    mx = lax.rem(dp // 2, 2)
    my = dp // 4

    def dpi(cc, yy, xx):
        return yy * 4 + xx * 2 + cc

    core_nb = (tp, dpi(1 - c, my, mx))
    x_nb = (tp, dpi(c, my, 1 - mx))
    y_nb = (tp, dpi(c, 1 - my, mx))
    z_nb = (1 - tp, dp)

    def w_copies(p):
        cols = pl.ds(pl.multiple_of(p * 2 * FC, 2 * FC), 2 * FC)
        return (pltpu.make_async_copy(wg_hbm.at[:, cols], wg.at[p], w_sem.at[0, p]),
                pltpu.make_async_copy(wu_hbm.at[:, cols], wu.at[p], w_sem.at[1, p]),
                pltpu.make_async_copy(wd_hbm.at[cols, :], wd.at[p], w_sem.at[2, p]))

    @pl.loop(0, NP)
    def _(p):
        for cp in w_copies(p):
            cp.start()

    barrier = pltpu.get_barrier_semaphore()
    me = tp * 8 + dp

    @pl.loop(1, 16)
    def _(k):
        o = lax.rem(me + k, 16)
        pl.semaphore_signal(barrier, inc=1, device_id=(o // 8, lax.rem(o, 8)), device_id_type=MESH)
    pl.semaphore_wait(barrier, 15)

    def blk(tt, dd):
        return (lax.rem(dd, 2) * 4 + (dd // 4) * 2 + lax.rem(dd // 2, 2)) * 2 + tt

    def x_copy(k, j):
        o = lax.rem(me + k, 16)
        ot, od = o // 8, lax.rem(o, 8)
        src = (x_ref, gy_ref)[j].at[:, pl.ds(pl.multiple_of(od * DL, DL), DL)]
        return pltpu.make_async_remote_copy(
            src_ref=src, dst_ref=xin.at[blk(tp, dp), j], send_sem=x_send.at[k, j],
            recv_sem=x_recv.at[blk(tp, dp), j], device_id=(ot, od), device_id_type=MESH)

    def x_wait(k, j):
        o = lax.rem(me + k, 16)
        ot, od = o // 8, lax.rem(o, 8)
        return pltpu.make_async_remote_copy(
            src_ref=x_ref.at[:, pl.ds(0, DL)], dst_ref=xin.at[blk(ot, od), j], send_sem=x_send.at[k, j],
            recv_sem=x_recv.at[blk(ot, od), j], device_id=(ot, od), device_id_type=MESH)

    @pl.loop(1, 16)
    def _(k):
        for j in range(2):
            x_copy(k, j).start()

    mine = blk(tp, dp)
    own = pl.ds(pl.multiple_of(dp * DL, DL), DL)
    xin[mine, 0] = x_ref[:, own]
    xin[mine, 1] = gy_ref[:, own]
    acc[...] = jnp.zeros_like(acc)

    @pl.loop(1, 16)
    def _(k):
        for j in range(2):
            x_wait(k, j).wait_recv()

    for j in range(2):
        xs_ref[j] = xin[:, j].astype(F32).reshape(128, DL).astype(BF)

    def d_copy(p):
        s = lax.rem(p, 2)
        return pltpu.make_async_remote_copy(
            src_ref=part.at[s, 1 - c], dst_ref=rd.at[p], send_sem=d_send.at[p], recv_sem=d_recv.at[p],
            device_id=core_nb, device_id_type=MESH)

    def s2_copies(p):
        return (pltpu.make_async_remote_copy(
                    src_ref=rd.at[p, 0, :, :, 1 - mx], dst_ref=r2.at[p, 0], send_sem=s2_send.at[0, p],
                    recv_sem=s2_recv.at[0, p], device_id=x_nb, device_id_type=MESH),
                pltpu.make_async_remote_copy(
                    src_ref=rd.at[p, 1, :, 1 - my], dst_ref=r2.at[p, 1], send_sem=s2_send.at[1, p],
                    recv_sem=s2_recv.at[1, p], device_id=y_nb, device_id_type=MESH))

    def s3_copies(p):
        return (pltpu.make_async_remote_copy(
                    src_ref=r2.at[p, 0, :, 1 - my], dst_ref=r3.at[p, 0], send_sem=s3_send.at[0, p],
                    recv_sem=s3_recv.at[0, p], device_id=y_nb, device_id_type=MESH),
                pltpu.make_async_remote_copy(
                    src_ref=r2.at[p, 1, :, 1 - mx], dst_ref=r3.at[p, 1], send_sem=s3_send.at[1, p],
                    recv_sem=s3_recv.at[1, p], device_id=x_nb, device_id_type=MESH))

    def s4_copies(p, yy0, xx1):
        return (pltpu.make_async_remote_copy(
                    src_ref=gat.at[p, 0, c, yy0, mx], dst_ref=gat.at[p, 0, c, yy0, mx],
                    send_sem=s4_send.at[0, p], recv_sem=s4_recv.at[0, p], device_id=y_nb, device_id_type=MESH),
                pltpu.make_async_remote_copy(
                    src_ref=gat.at[p, 1, c, my, xx1], dst_ref=gat.at[p, 1, c, my, xx1],
                    send_sem=s4_send.at[1, p], recv_sem=s4_recv.at[1, p], device_id=x_nb, device_id_type=MESH))

    def s5_copies(p, xx0, yy1):
        return (pltpu.make_async_remote_copy(
                    src_ref=gat.at[p, 0, c, :, xx0], dst_ref=gat.at[p, 0, c, :, xx0],
                    send_sem=s5_send.at[0, p], recv_sem=s5_recv.at[0, p], device_id=x_nb, device_id_type=MESH),
                pltpu.make_async_remote_copy(
                    src_ref=gat.at[p, 1, c, yy1], dst_ref=gat.at[p, 1, c, yy1],
                    send_sem=s5_send.at[1, p], recv_sem=s5_recv.at[1, p], device_id=y_nb, device_id_type=MESH))

    def s6_copy(p, cc):
        return pltpu.make_async_remote_copy(
            src_ref=gat.at[p, :, cc], dst_ref=gat.at[p, :, cc], send_sem=s6_send.at[p],
            recv_sem=s6_recv.at[p], device_id=core_nb, device_id_type=MESH)

    def g_copy(p):
        return pltpu.make_async_copy(gat.at[p], g_hbm.at[p], g_sem.at[p])

    def products(p):
        s = lax.rem(p, 2)
        for cp in w_copies(p):
            cp.wait()

        @pl.when(p >= 2)
        def _():
            d_copy(p - 2).wait_send()

        for ab in range(2):
            for n in range(FC // NSUB):
                lo = ab * FC + n * NSUB
                cols = pl.ds(lo, NSUB)
                dst = pl.ds(n * NSUB, NSUB)
                vals = (_dot(xs_ref[0], wg[p, :, cols], 1, 0),
                        _dot(xs_ref[0], wu[p, :, cols], 1, 0),
                        _dot(xs_ref[1], wd[p, cols, :], 1, 1))
                for t in range(3):
                    v = vals[t].reshape(2, 2, 2, 16, NSUB)
                    for cc in range(2):
                        part[s, cc, ab, t, :, :, :, dst] = v[cc]
        d_copy(p).start()

    def stage2(p):
        s = lax.rem(p, 2)
        d_copy(p).wait_recv()
        for ab in range(2):
            for t in range(3):
                rd[p, ab, t] = rd[p, ab, t] + part[s, c, ab, t]
        for cp in s2_copies(p):
            cp.start()

    def stage3(p):
        for cp in s2_copies(p):
            cp.wait_recv()
        for t in range(3):
            r2[p, 0, t] = r2[p, 0, t] + rd[p, 0, t, :, mx]
            r2[p, 1, t] = r2[p, 1, t] + rd[p, 1, t, my]
        for cp in s3_copies(p):
            cp.start()

    def stage4(p):
        for cp in s3_copies(p):
            cp.wait_recv()
        for ab in range(2):
            keep = my if ab == 0 else mx
            a = r3[p, ab, 0] + r2[p, ab, 0, keep]
            b = r3[p, ab, 1] + r2[p, ab, 1, keep]
            g = r3[p, ab, 2] + r2[p, ab, 2, keep]
            s = jax.nn.sigmoid(a)
            silu = a * s
            gat[p, ab, c, my, mx, 0] = (silu * b).astype(BF)
            gat[p, ab, c, my, mx, 1] = (g * b * (s * (1.0 + a * (1.0 - s)))).astype(BF)
            gat[p, ab, c, my, mx, 2] = (g * silu).astype(BF)
        for cp in s4_copies(p, my, mx):
            cp.start()

    def stage5(p):
        for cp in s4_copies(p, 1 - my, 1 - mx):
            cp.wait_recv()
        for cp in s5_copies(p, mx, my):
            cp.start()

    def stage6(p):
        for cp in s5_copies(p, 1 - mx, 1 - my):
            cp.wait_recv()
        s6_copy(p, c).start()

    def stage7(p):
        s6_copy(p, 1 - c).wait_recv()
        g_copy(p).start()
        for ab in range(2):
            cols = pl.ds(ab * FC, FC)
            h = gat[p, ab, :, :, :, 0].reshape(128, FC)
            acc[0] = acc[0] + _dot(h, wd[p, cols, :], 1, 0)
            da = gat[p, ab, :, :, :, 1].reshape(128, FC)
            db = gat[p, ab, :, :, :, 2].reshape(128, FC)
            acc[1] = acc[1] + (_dot(da, wg[p, :, cols], 1, 1) + _dot(db, wu[p, :, cols], 1, 1))

    products(0)

    @pl.loop(0, NP + 5)
    def _(i):
        pl.when(i < NP)(lambda: stage2(i))
        pl.when((i >= 1) & (i < NP + 1))(lambda: stage3(i - 1))
        pl.when((i >= 2) & (i < NP + 2))(lambda: stage4(i - 2))
        pl.when((i >= 3) & (i < NP + 3))(lambda: stage5(i - 3))
        pl.when((i >= 4) & (i < NP + 4))(lambda: stage6(i - 4))
        pl.when(i < NP - 1)(lambda: products(i + 1))
        pl.when(i >= 5)(lambda: stage7(i - 5))

    accv = acc.reshape(2, 8, 2, 8, DL)
    zc = pltpu.make_async_remote_copy(
        src_ref=accv.at[:, :, 1 - tp], dst_ref=rz, send_sem=z_send, recv_sem=z_recv,
        device_id=z_nb, device_id_type=MESH)
    zc.start()
    zc.wait_recv()
    for q in range(8):
        for j in range(2):
            tot = accv[j, q, tp] + rz[j, q] + xin[2 * q + tp, j].astype(F32)
            ob[q, j] = tot.astype(BF)

    def q_of(dd):
        return lax.rem(dd, 2) * 4 + (dd // 4) * 2 + lax.rem(dd // 2, 2)

    def o_copy(k, src_dp):
        od = lax.rem(dp + k, 8)
        return pltpu.make_async_remote_copy(
            src_ref=ob.at[q_of(od)], dst_ref=orx.at[src_dp], send_sem=o_send.at[k],
            recv_sem=o_recv.at[src_dp], device_id=(tp, od), device_id_type=MESH)

    @pl.loop(1, 8)
    def _(k):
        o_copy(k, dp).start()

    orx[dp] = ob[q_of(dp)]

    @pl.loop(0, NP)
    def _(p):
        for cp in (*s2_copies(p), *s3_copies(p), *s4_copies(p, my, mx), *s5_copies(p, mx, my), s6_copy(p, c)):
            cp.wait_send()
        g_copy(p).wait()
    for p in (NP - 2, NP - 1):
        d_copy(p).wait_send()

    @pl.loop(1, 16)
    def _(k):
        for j in range(2):
            x_copy(k, j).wait_send()
    zc.wait_send()

    @pl.loop(1, 8)
    def _(k):
        o_copy(k, lax.rem(dp + k, 8)).wait_recv()

    for dd in range(8):
        y_ref[:, dd * DL:(dd + 1) * DL] = orx[dd, 0]
        gx_ref[:, dd * DL:(dd + 1) * DL] = orx[dd, 1]

    @pl.loop(1, 8)
    def _(k):
        o_copy(k, dp).wait_send()


def wgrad_kernel(xs_ref, g_ref, dwg_ref, dwu_ref, dwd_ref):
    h = g_ref[0, 0, :, :, :, 0].reshape(128, FC)
    da = g_ref[0, 0, :, :, :, 1].reshape(128, FC)
    db = g_ref[0, 0, :, :, :, 2].reshape(128, FC)
    dwg_ref[...] = _dot(xs_ref[0], da, 0, 0)
    dwu_ref[...] = _dot(xs_ref[0], db, 0, 0)
    dwd_ref[...] = _dot(h, xs_ref[1], 0, 0)


def local_step(x_loc, wg_loc, wu_loc, wd_loc, gy_loc):
    vm = pl.BlockSpec(memory_space=pltpu.VMEM)
    hb = pl.BlockSpec(memory_space=pl.ANY)
    dma = pltpu.SemaphoreType.DMA
    y_rows, gx_rows, xs, gathered = pl.pallas_call(
        comm_kernel,
        out_shape=(jax.ShapeDtypeStruct((8, D), BF), jax.ShapeDtypeStruct((8, D), BF),
                   jax.ShapeDtypeStruct((2, 128, DL), BF),
                   jax.ShapeDtypeStruct((NP, 2, 2, 2, 2, 3, 16, FC), BF)),
        in_specs=[vm, vm, hb, hb, hb],
        out_specs=(vm, vm, vm, hb),
        scratch_shapes=[
            pltpu.VMEM((NP, DL, 2 * FC), BF),
            pltpu.VMEM((NP, DL, 2 * FC), BF),
            pltpu.VMEM((NP, 2 * FC, DL), BF),
            pltpu.VMEM((16, 2, 8, DL), BF),
            pltpu.VMEM((2, 2, 2, 3, 2, 2, 16, FC), F32),
            pltpu.VMEM((NP, 2, 3, 2, 2, 16, FC), F32),
            pltpu.VMEM((NP, 2, 3, 2, 16, FC), F32),
            pltpu.VMEM((NP, 2, 3, 16, FC), F32),
            pltpu.VMEM((NP, 2, 2, 2, 2, 3, 16, FC), BF),
            pltpu.VMEM((2, 128, DL), F32),
            pltpu.VMEM((2, 8, 8, DL), F32),
            pltpu.VMEM((8, 2, 8, DL), BF),
            pltpu.VMEM((8, 2, 8, DL), BF),
            dma((3, NP)), dma((16, 2)), dma((16, 2)), dma((NP,)), dma((NP,)),
            dma((2, NP)), dma((2, NP)), dma((2, NP)), dma((2, NP)),
            dma((2, NP)), dma((2, NP)), dma((2, NP)), dma((2, NP)),
            dma((NP,)), dma((NP,)), dma((NP,)),
            dma(()), dma(()), dma((8,)), dma((8,)),
        ],
        compiler_params=pltpu.CompilerParams(
            collective_id=0, has_side_effects=True, vmem_limit_bytes=60 * 1024 * 1024),
        name="mlp_comm",
    )(x_loc, gy_loc, wg_loc, wu_loc, wd_loc)

    grad_wg, grad_wu, grad_wd = pl.pallas_call(
        wgrad_kernel,
        grid=(2 * NP,),
        out_shape=(jax.ShapeDtypeStruct((DL, FF_LOC), F32), jax.ShapeDtypeStruct((DL, FF_LOC), F32),
                   jax.ShapeDtypeStruct((FF_LOC, DL), F32)),
        in_specs=[pl.BlockSpec((2, 128, DL), lambda k: (0, 0, 0)),
                  pl.BlockSpec((1, 1, 2, 2, 2, 3, 16, FC), lambda k: (k // 2, lax.rem(k, 2), 0, 0, 0, 0, 0, 0))],
        out_specs=(pl.BlockSpec((DL, FC), lambda k: (0, k)), pl.BlockSpec((DL, FC), lambda k: (0, k)),
                   pl.BlockSpec((FC, DL), lambda k: (k, 0))),
        compiler_params=pltpu.CompilerParams(dimension_semantics=("arbitrary",), vmem_limit_bytes=48 * 1024 * 1024),
        name="mlp_wgrad",
    )(xs, gathered)
    return y_rows, gx_rows, grad_wg, grad_wu, grad_wd


def solution(mesh):
    row_spec = P(("dp", "tp"), None)
    up_spec = P("dp", "tp")
    down_spec = P("tp", "dp")
    return jax.shard_map(local_step, mesh=mesh,
                         in_specs=(row_spec, up_spec, up_spec, down_spec, row_spec),
                         out_specs=(row_spec, row_spec, up_spec, up_spec, down_spec),
                         check_vma=False)
```

```python
import functools

import jax
import jax.numpy as jnp
from jax import lax
from jax.experimental import pallas as pl
from jax.experimental.pallas import tpu as pltpu
from jax.sharding import PartitionSpec as P

MESH = pl.DeviceIdType.MESH
BF = jnp.bfloat16
F32 = jnp.float32

D = 3072
FF_LOC = 12288
DL = 384
NP = 8
FC = FF_LOC // (2 * NP)
NS = 3
SUB = FC // NS


def _dot(a, b, ca, cb):
    return lax.dot_general(a, b, (((ca,), (cb,)), ((), ())), preferred_element_type=F32)


def comm_kernel(x_ref, gy_ref, wg_hbm, wu_hbm, wd_hbm,
                y_ref, gx_ref, xs_ref, g_hbm,
                wg, wu, wd, st, xin, part, rd, r2, r3, gat, acc, fin,
                w_sem, x_send, x_recv, d_send, d_recv, d0_send, d0_recv, s2_send, s2_recv, s20_send, s20_recv,
                s3_send, s3_recv, s4_send, s4_recv, s5_send, s5_recv, s5l_send, s5l_recv,
                s6_send, s6_recv, s6l_send, s6l_recv, g_sem, o_send, o_recv):
    tp = lax.axis_index("tp")
    dp = lax.axis_index("dp")
    c = lax.rem(dp, 2)
    mx = lax.rem(dp // 2, 2)
    my = dp // 4
    me = tp * 8 + dp
    last = NP - 1

    def dpi(cc, yy, xx):
        return yy * 4 + xx * 2 + cc

    core_nb = (tp, dpi(1 - c, my, mx))
    x_nb = (tp, dpi(c, my, 1 - mx))
    y_nb = (tp, dpi(c, 1 - my, mx))

    def remote(src, dst, send, recv, dev):
        return pltpu.make_async_remote_copy(src_ref=src, dst_ref=dst, send_sem=send, recv_sem=recv,
                                            device_id=dev, device_id_type=MESH)

    def w_copies(p):
        cols = pl.ds(pl.multiple_of(p * 2 * FC, 2 * FC), 2 * FC)
        return (pltpu.make_async_copy(wg_hbm.at[:, cols], wg.at[p], w_sem.at[0, p]),
                pltpu.make_async_copy(wu_hbm.at[:, cols], wu.at[p], w_sem.at[1, p]),
                pltpu.make_async_copy(wd_hbm.at[cols, :], wd.at[p], w_sem.at[2, p]))

    barrier = pltpu.get_barrier_semaphore()

    def other(k):
        o = lax.rem(me + k, 16)
        return o // 8, lax.rem(o, 8)

    @pl.loop(1, 16)
    def _(k):
        pl.semaphore_signal(barrier, inc=1, device_id=other(k), device_id_type=MESH)

    @pl.loop(0, NP)
    def _(p):
        for cp in w_copies(p):
            cp.start()

    for dd in range(8):
        st[dd, 0] = x_ref[:, dd * DL:(dd + 1) * DL]
        st[dd, 1] = gy_ref[:, dd * DL:(dd + 1) * DL]
    acc[...] = jnp.zeros_like(acc)
    pl.semaphore_wait(barrier, 15)

    def blk(tt, dd):
        return (lax.rem(dd, 2) * 4 + (dd // 4) * 2 + lax.rem(dd // 2, 2)) * 2 + tt

    mine = blk(tp, dp)

    def x_copy(k, b):
        ot, od = other(k)
        return remote(st.at[od], xin.at[b], x_send.at[k], x_recv.at[b], (ot, od))

    @pl.loop(1, 16)
    def _(k):
        x_copy(k, mine).start()

    xin[mine] = st[dp]

    @pl.loop(1, 16)
    def _(k):
        x_copy(k, blk(*other(k))).wait_recv()

    for j in range(2):
        xs_ref[j] = xin[:, j].astype(F32).reshape(128, DL).astype(BF)

    def sub(n):
        return pl.ds(n * SUB, SUB)

    def d_copy(p, ab, n=None):
        s = lax.rem(p, 2)
        if n is None:
            return remote(part.at[s, 1 - c, ab], rd.at[p, ab], d_send.at[ab, p], d_recv.at[ab, p], core_nb)
        return remote(part.at[s, 1 - c, ab, :, :, :, :, sub(n)], rd.at[p, ab, :, :, :, :, sub(n)],
                      d0_send.at[ab, n], d0_recv.at[ab, n], core_nb)

    def s2_copy(p, ab, n=None):
        src = rd.at[p, 0, :, :, 1 - mx] if ab == 0 else rd.at[p, 1, :, 1 - my]
        dst = r2.at[p, ab]
        dev = x_nb if ab == 0 else y_nb
        if n is None:
            return remote(src, dst, s2_send.at[ab, p], s2_recv.at[ab, p], dev)
        return remote(src.at[:, :, :, sub(n)], dst.at[:, :, :, sub(n)], s20_send.at[ab, n], s20_recv.at[ab, n], dev)

    def s3_copies(p):
        return (remote(r2.at[p, 0, :, 1 - my], r3.at[p, 0], s3_send.at[0, p], s3_recv.at[0, p], y_nb),
                remote(r2.at[p, 1, :, 1 - mx], r3.at[p, 1], s3_send.at[1, p], s3_recv.at[1, p], x_nb))

    def s4_copies(p, yy0, xx1):
        b0, b1 = gat.at[p, 0, c, yy0, mx], gat.at[p, 1, c, my, xx1]
        return (remote(b0, b0, s4_send.at[0, p], s4_recv.at[0, p], y_nb),
                remote(b1, b1, s4_send.at[1, p], s4_recv.at[1, p], x_nb))

    def s5_copies(p, xx0, yy1, n=None):
        b0, b1 = gat.at[p, 0, c, :, xx0], gat.at[p, 1, c, yy1]
        if n is None:
            return (remote(b0, b0, s5_send.at[0, p], s5_recv.at[0, p], x_nb),
                    remote(b1, b1, s5_send.at[1, p], s5_recv.at[1, p], y_nb))
        b0, b1 = b0.at[:, :, :, sub(n)], b1.at[:, :, :, sub(n)]
        return (remote(b0, b0, s5l_send.at[0, n], s5l_recv.at[0, n], x_nb),
                remote(b1, b1, s5l_send.at[1, n], s5l_recv.at[1, n], y_nb))

    def s6_copy(p, cc, n=None):
        b = gat.at[p, :, cc]
        if n is None:
            return remote(b, b, s6_send.at[p], s6_recv.at[p], core_nb)
        b = b.at[:, :, :, :, :, sub(n)]
        return remote(b, b, s6l_send.at[n], s6l_recv.at[n], core_nb)

    def g_copy(p):
        return pltpu.make_async_copy(gat.at[p], g_hbm.at[p], g_sem.at[p])

    def product(p, ab, n):
        s = lax.rem(p, 2)
        cols = pl.ds(ab * FC + n * SUB, SUB)
        vals = (_dot(xs_ref[0], wg[p, :, cols], 1, 0),
                _dot(xs_ref[0], wu[p, :, cols], 1, 0),
                _dot(xs_ref[1], wd[p, cols, :], 1, 1))
        for t in range(3):
            v = vals[t].reshape(2, 2, 2, 16, SUB)
            for cc in range(2):
                part[s, cc, ab, t, :, :, :, sub(n)] = v[cc]

    def products(p):
        for cp in w_copies(p):
            cp.wait()
        for ab in range(2):
            @pl.when(p >= 3)
            def _():
                d_copy(p - 2, ab).wait_send()

            @pl.when(p == 2)
            def _():
                for n in range(NS):
                    d_copy(0, ab, n).wait_send()
            for n in range(NS):
                product(p, ab, n)
            d_copy(p, ab).start()

    def stage2(p):
        s = lax.rem(p, 2)
        for ab in range(2):
            d_copy(p, ab).wait_recv()
            for t in range(3):
                rd[p, ab, t] = rd[p, ab, t] + part[s, c, ab, t]
            s2_copy(p, ab).start()

    def stage3(p):
        for ab in range(2):
            @pl.when(p == 0)
            def _():
                for n in range(NS):
                    s2_copy(0, ab, n).wait_recv()

            @pl.when(p > 0)
            def _():
                s2_copy(p, ab).wait_recv()
            for t in range(3):
                r2[p, ab, t] = r2[p, ab, t] + (rd[p, 0, t, :, mx] if ab == 0 else rd[p, 1, t, my])
            s3_copies(p)[ab].start()

    def stage4(p):
        for ab in range(2):
            s3_copies(p)[ab].wait_recv()
            keep = my if ab == 0 else mx
            a = r3[p, ab, 0] + r2[p, ab, 0, keep]
            b = r3[p, ab, 1] + r2[p, ab, 1, keep]
            g = r3[p, ab, 2] + r2[p, ab, 2, keep]
            s = jax.nn.sigmoid(a)
            silu = a * s
            gat[p, ab, c, my, mx, 0] = (silu * b).astype(BF)
            gat[p, ab, c, my, mx, 1] = (g * b * (s * (1.0 + a * (1.0 - s)))).astype(BF)
            gat[p, ab, c, my, mx, 2] = (g * silu).astype(BF)
            s4_copies(p, my, mx)[ab].start()

    def stage5(p):
        for ab in range(2):
            s4_copies(p, 1 - my, 1 - mx)[ab].wait_recv()

            @pl.when(p < last)
            def _():
                s5_copies(p, mx, my)[ab].start()

            @pl.when(p == last)
            def _():
                for n in range(NS):
                    s5_copies(last, mx, my, n)[ab].start()

    def stage6(p):
        for cp in s5_copies(p, 1 - mx, 1 - my):
            cp.wait_recv()
        s6_copy(p, c).start()

    def accumulate(j, v):
        acc[j] = acc[j] + v.reshape(16, 8, DL)

    def y_part(p, lo, w):
        v = None
        for ab in range(2):
            h = gat[p, ab, :, :, :, 0, :, lo:lo + w].reshape(128, w)
            d = _dot(h, wd[p, ab * FC + lo:ab * FC + lo + w, :], 1, 0)
            v = d if v is None else v + d
        accumulate(0, v)

    def dx_part(p, lo, w):
        v = None
        for ab in range(2):
            for t, wt in ((1, wg), (2, wu)):
                z = gat[p, ab, :, :, :, t, :, lo:lo + w].reshape(128, w)
                d = _dot(z, wt[p, :, ab * FC + lo:ab * FC + lo + w], 1, 1)
                v = d if v is None else v + d
        accumulate(1, v)

    def stage7(p):
        s6_copy(p, 1 - c).wait_recv()
        g_copy(p).start()
        y_part(p, 0, FC)
        dx_part(p, 0, FC)

    for cp in w_copies(0):
        cp.wait()
    for n in range(NS):
        for ab in range(2):
            product(0, ab, n)
            d_copy(0, ab, n).start()
    for n in range(NS):
        for ab in range(2):
            d_copy(0, ab, n).wait_recv()
            rd[0, ab, :, :, :, :, sub(n)] = rd[0, ab, :, :, :, :, sub(n)] + part[0, c, ab, :, :, :, :, sub(n)]
            s2_copy(0, ab, n).start()

    @pl.loop(0, NP + 4)
    def _(i):
        pl.when((i >= 1) & (i < NP))(lambda: stage2(i))
        pl.when((i >= 1) & (i < NP + 1))(lambda: stage3(i - 1))
        pl.when((i >= 2) & (i < NP + 2))(lambda: stage4(i - 2))
        pl.when((i >= 3) & (i < NP + 3))(lambda: stage5(i - 3))
        pl.when((i >= 4) & (i < NP + 3))(lambda: stage6(i - 4))
        pl.when(i < NP - 1)(lambda: products(i + 1))
        pl.when(i >= 5)(lambda: stage7(i - 5))

    def o_copy(j, k, slot):
        ot, od = other(k)
        return remote(acc.at[j, blk(ot, od)], fin.at[j, slot], o_send.at[j, k], o_recv.at[j, slot], (ot, od))

    def send_out(j):
        @pl.loop(1, 16)
        def _(k):
            o_copy(j, k, me).start()
        fin[j, me] = acc[j, mine]

    for n in range(NS):
        for cp in s5_copies(last, 1 - mx, 1 - my, n):
            cp.wait_recv()
        s6_copy(last, c, n).start()
    for n in range(NS):
        s6_copy(last, 1 - c, n).wait_recv()
        if n == NS - 1:
            g_copy(last).start()
        y_part(last, n * SUB, SUB)
        if n == NS - 1:
            send_out(0)
        dx_part(last, n * SUB, SUB)
    send_out(1)

    @pl.loop(0, NP)
    def _(p):
        for cp in (*s3_copies(p), *s4_copies(p, my, mx)):
            cp.wait_send()
        g_copy(p).wait()

    @pl.loop(1, NP)
    def _(p):
        for ab in range(2):
            s2_copy(p, ab).wait_send()

    @pl.loop(0, NP - 1)
    def _(p):
        for cp in (*s5_copies(p, mx, my), s6_copy(p, c)):
            cp.wait_send()
    for n in range(NS):
        for ab in range(2):
            s2_copy(0, ab, n).wait_send()
            s5_copies(last, mx, my, n)[ab].wait_send()
        s6_copy(last, c, n).wait_send()
    for p in (NP - 2, NP - 1):
        for ab in range(2):
            d_copy(p, ab).wait_send()

    @pl.loop(1, 16)
    def _(k):
        x_copy(k, mine).wait_send()

    for j, (out, res) in enumerate(((y_ref, x_ref), (gx_ref, gy_ref))):
        @pl.loop(1, 16)
        def _(k):
            ot, od = other(k)
            o_copy(j, k, ot * 8 + od).wait_recv()
        for dd in range(8):
            cols = slice(dd * DL, (dd + 1) * DL)
            out[:, cols] = (res[:, cols].astype(F32) + (fin[j, dd] + fin[j, 8 + dd])).astype(BF)

    @pl.loop(1, 16)
    def _(k):
        for j in range(2):
            o_copy(j, k, me).wait_send()


def wgrad_kernel(xs_ref, g_ref, y_ref, gx_ref, yo_ref, gxo_ref, dwg_ref, dwu_ref, dwd_ref):
    @pl.when(pl.program_id(0) == 0)
    def _():
        yo_ref[...] = y_ref[...]
        gxo_ref[...] = gx_ref[...]
    h = g_ref[0, 0, :, :, :, 0].reshape(128, FC)
    da = g_ref[0, 0, :, :, :, 1].reshape(128, FC)
    db = g_ref[0, 0, :, :, :, 2].reshape(128, FC)
    dwg_ref[...] = _dot(xs_ref[0], da, 0, 0)
    dwu_ref[...] = _dot(xs_ref[0], db, 0, 0)
    dwd_ref[...] = _dot(h, xs_ref[1], 0, 0)


def local_step(x_loc, wg_loc, wu_loc, wd_loc, gy_loc):
    vm = pl.BlockSpec(memory_space=pltpu.VMEM)
    hb = pl.BlockSpec(memory_space=pl.ANY)
    dma = pltpu.SemaphoreType.DMA
    row = jax.ShapeDtypeStruct((8, D), BF)
    y_rows, gx_rows, xs, gathered = pl.pallas_call(
        comm_kernel,
        out_shape=(row, row, jax.ShapeDtypeStruct((2, 128, DL), BF),
                   jax.ShapeDtypeStruct((NP, 2, 2, 2, 2, 3, 16, FC), BF)),
        in_specs=[vm, vm, hb, hb, hb],
        out_specs=(vm, vm, vm, hb),
        scratch_shapes=[
            pltpu.VMEM((NP, DL, 2 * FC), BF),
            pltpu.VMEM((NP, DL, 2 * FC), BF),
            pltpu.VMEM((NP, 2 * FC, DL), BF),
            pltpu.VMEM((8, 2, 8, DL), BF),
            pltpu.VMEM((16, 2, 8, DL), BF),
            pltpu.VMEM((2, 2, 2, 3, 2, 2, 16, FC), F32),
            pltpu.VMEM((NP, 2, 3, 2, 2, 16, FC), F32),
            pltpu.VMEM((NP, 2, 3, 2, 16, FC), F32),
            pltpu.VMEM((NP, 2, 3, 16, FC), F32),
            pltpu.VMEM((NP, 2, 2, 2, 2, 3, 16, FC), BF),
            pltpu.VMEM((2, 16, 8, DL), F32),
            pltpu.VMEM((2, 16, 8, DL), F32),
            dma((3, NP)), dma((16,)), dma((16,)),
            dma((2, NP)), dma((2, NP)), dma((2, NS)), dma((2, NS)),
            dma((2, NP)), dma((2, NP)), dma((2, NS)), dma((2, NS)),
            dma((2, NP)), dma((2, NP)), dma((2, NP)), dma((2, NP)),
            dma((2, NP)), dma((2, NP)), dma((2, NS)), dma((2, NS)),
            dma((NP,)), dma((NP,)), dma((NS,)), dma((NS,)),
            dma((NP,)), dma((2, 16)), dma((2, 16)),
        ],
        compiler_params=pltpu.CompilerParams(
            collective_id=0, has_side_effects=True, vmem_limit_bytes=60 * 1024 * 1024),
        name="mlp_comm",
    )(x_loc, gy_loc, wg_loc, wu_loc, wd_loc)

    rows_spec = pl.BlockSpec((8, D), lambda k: (0, 0))
    return pl.pallas_call(
        wgrad_kernel,
        grid=(2 * NP,),
        out_shape=(row, row,
                   jax.ShapeDtypeStruct((DL, FF_LOC), F32), jax.ShapeDtypeStruct((DL, FF_LOC), F32),
                   jax.ShapeDtypeStruct((FF_LOC, DL), F32)),
        in_specs=[pl.BlockSpec((2, 128, DL), lambda k: (0, 0, 0)),
                  pl.BlockSpec((1, 1, 2, 2, 2, 3, 16, FC), lambda k: (k // 2, lax.rem(k, 2), 0, 0, 0, 0, 0, 0)),
                  rows_spec, rows_spec],
        out_specs=(rows_spec, rows_spec,
                   pl.BlockSpec((DL, FC), lambda k: (0, k)), pl.BlockSpec((DL, FC), lambda k: (0, k)),
                   pl.BlockSpec((FC, DL), lambda k: (k, 0))),
        compiler_params=pltpu.CompilerParams(dimension_semantics=("arbitrary",), vmem_limit_bytes=60 * 1024 * 1024),
        name="mlp_wgrad",
    )(xs, gathered, y_rows, gx_rows)


def solution(mesh):
    row_spec = P(("dp", "tp"), None)
    up_spec = P("dp", "tp")
    down_spec = P("tp", "dp")
    return jax.shard_map(local_step, mesh=mesh,
                         in_specs=(row_spec, up_spec, up_spec, down_spec, row_spec),
                         out_specs=(row_spec, row_spec, up_spec, up_spec, down_spec),
                         check_vma=False)
```

```python
import functools

import jax
import jax.numpy as jnp
from jax import lax
from jax.experimental import pallas as pl
from jax.experimental.pallas import tpu as pltpu
from jax.sharding import PartitionSpec as P

MESH = pl.DeviceIdType.MESH
BF = jnp.bfloat16
F32 = jnp.float32

D = 3072
FF_LOC = 12288
DL = 384
NP = 8
FC = FF_LOC // (2 * NP)
NS = 3
SUB = FC // NS


def _dot(a, b, ca, cb):
    return lax.dot_general(a, b, (((ca,), (cb,)), ((), ())), preferred_element_type=F32)


def comm_kernel(x_hbm, gy_hbm, wg_hbm, wu_hbm, wd_hbm,
                y_ref, gx_ref, xs_ref, gat,
                rows, wg, wu, wd, st, xin, part, rd, r2, r3, acc, fin,
                in_sem, w_sem, x_send, x_recv, d_send, d_recv, d0_send, d0_recv, s2_send, s2_recv, s20_send, s20_recv,
                s3_send, s3_recv, s4_send, s4_recv, s5_send, s5_recv, s5l_send, s5l_recv,
                s6_send, s6_recv, s6l_send, s6l_recv, o_send, o_recv):
    tp = lax.axis_index("tp")
    dp = lax.axis_index("dp")
    c = lax.rem(dp, 2)
    mx = lax.rem(dp // 2, 2)
    my = dp // 4
    me = tp * 8 + dp
    last = NP - 1

    def dpi(cc, yy, xx):
        return yy * 4 + xx * 2 + cc

    core_nb = (tp, dpi(1 - c, my, mx))
    x_nb = (tp, dpi(c, my, 1 - mx))
    y_nb = (tp, dpi(c, 1 - my, mx))

    def remote(src, dst, send, recv, dev):
        return pltpu.make_async_remote_copy(src_ref=src, dst_ref=dst, send_sem=send, recv_sem=recv,
                                            device_id=dev, device_id_type=MESH)

    def w_copies(p):
        cols = pl.ds(pl.multiple_of(p * 2 * FC, 2 * FC), 2 * FC)
        return (pltpu.make_async_copy(wg_hbm.at[:, cols], wg.at[p], w_sem.at[0, p]),
                pltpu.make_async_copy(wu_hbm.at[:, cols], wu.at[p], w_sem.at[1, p]),
                pltpu.make_async_copy(wd_hbm.at[cols, :], wd.at[p], w_sem.at[2, p]))

    in_copies = [pltpu.make_async_copy(r, rows.at[j], in_sem.at[j]) for j, r in enumerate((x_hbm, gy_hbm))]
    for cp in in_copies:
        cp.start()
    barrier = pltpu.get_barrier_semaphore()

    def other(k):
        o = lax.rem(me + k, 16)
        return o // 8, lax.rem(o, 8)

    @pl.loop(1, 16)
    def _(k):
        pl.semaphore_signal(barrier, inc=1, device_id=other(k), device_id_type=MESH)

    @pl.loop(0, NP)
    def _(p):
        for cp in w_copies(p):
            cp.start()

    acc[...] = jnp.zeros_like(acc)
    for j in range(2):
        in_copies[j].wait()
        for dd in range(8):
            st[dd, j] = rows[j, :, dd * DL:(dd + 1) * DL]
    pl.semaphore_wait(barrier, 15)

    def blk(tt, dd):
        return (lax.rem(dd, 2) * 4 + (dd // 4) * 2 + lax.rem(dd // 2, 2)) * 2 + tt

    mine = blk(tp, dp)

    def x_copy(k, b):
        ot, od = other(k)
        return remote(st.at[od], xin.at[b], x_send.at[k], x_recv.at[b], (ot, od))

    @pl.loop(1, 16)
    def _(k):
        x_copy(k, mine).start()

    xin[mine] = st[dp]

    @pl.loop(1, 16)
    def _(k):
        x_copy(k, blk(*other(k))).wait_recv()

    for j in range(2):
        xs_ref[j] = xin[:, j].astype(F32).reshape(128, DL).astype(BF)

    def sub(n):
        return pl.ds(n * SUB, SUB)

    def d_copy(p, ab, n=None):
        s = lax.rem(p, 2)
        if n is None:
            return remote(part.at[s, 1 - c, ab], rd.at[p, ab], d_send.at[ab, p], d_recv.at[ab, p], core_nb)
        return remote(part.at[s, 1 - c, ab, :, :, :, :, sub(n)], rd.at[p, ab, :, :, :, :, sub(n)],
                      d0_send.at[ab, n], d0_recv.at[ab, n], core_nb)

    def s2_copy(p, ab, n=None):
        src = rd.at[p, 0, :, :, 1 - mx] if ab == 0 else rd.at[p, 1, :, 1 - my]
        dst = r2.at[p, ab]
        dev = x_nb if ab == 0 else y_nb
        if n is None:
            return remote(src, dst, s2_send.at[ab, p], s2_recv.at[ab, p], dev)
        return remote(src.at[:, :, :, sub(n)], dst.at[:, :, :, sub(n)], s20_send.at[ab, n], s20_recv.at[ab, n], dev)

    def s3_copies(p):
        return (remote(r2.at[p, 0, :, 1 - my], r3.at[p, 0], s3_send.at[0, p], s3_recv.at[0, p], y_nb),
                remote(r2.at[p, 1, :, 1 - mx], r3.at[p, 1], s3_send.at[1, p], s3_recv.at[1, p], x_nb))

    def s4_copies(p, yy0, xx1):
        b0, b1 = gat.at[p, 0, c, yy0, mx], gat.at[p, 1, c, my, xx1]
        return (remote(b0, b0, s4_send.at[0, p], s4_recv.at[0, p], y_nb),
                remote(b1, b1, s4_send.at[1, p], s4_recv.at[1, p], x_nb))

    def s5_copies(p, xx0, yy1, n=None):
        b0, b1 = gat.at[p, 0, c, :, xx0], gat.at[p, 1, c, yy1]
        if n is None:
            return (remote(b0, b0, s5_send.at[0, p], s5_recv.at[0, p], x_nb),
                    remote(b1, b1, s5_send.at[1, p], s5_recv.at[1, p], y_nb))
        b0, b1 = b0.at[:, :, :, sub(n)], b1.at[:, :, :, sub(n)]
        return (remote(b0, b0, s5l_send.at[0, n], s5l_recv.at[0, n], x_nb),
                remote(b1, b1, s5l_send.at[1, n], s5l_recv.at[1, n], y_nb))

    def s6_copy(p, cc, n=None):
        b = gat.at[p, :, cc]
        if n is None:
            return remote(b, b, s6_send.at[p], s6_recv.at[p], core_nb)
        b = b.at[:, :, :, :, :, sub(n)]
        return remote(b, b, s6l_send.at[n], s6l_recv.at[n], core_nb)

    def product(p, ab, n):
        s = lax.rem(p, 2)
        cols = pl.ds(ab * FC + n * SUB, SUB)
        vals = (_dot(xs_ref[0], wg[p, :, cols], 1, 0),
                _dot(xs_ref[0], wu[p, :, cols], 1, 0),
                _dot(xs_ref[1], wd[p, cols, :], 1, 1))
        for t in range(3):
            v = vals[t].reshape(2, 2, 2, 16, SUB)
            for cc in range(2):
                part[s, cc, ab, t, :, :, :, sub(n)] = v[cc]

    def products(p):
        for cp in w_copies(p):
            cp.wait()
        for ab in range(2):
            @pl.when(p >= 3)
            def _():
                d_copy(p - 2, ab).wait_send()

            @pl.when(p == 2)
            def _():
                for n in range(NS):
                    d_copy(0, ab, n).wait_send()
            for n in range(NS):
                product(p, ab, n)
            d_copy(p, ab).start()

    def stage2(p):
        s = lax.rem(p, 2)
        for ab in range(2):
            d_copy(p, ab).wait_recv()
            for t in range(3):
                rd[p, ab, t] = rd[p, ab, t] + part[s, c, ab, t]
            s2_copy(p, ab).start()

    def stage3(p):
        for ab in range(2):
            @pl.when(p == 0)
            def _():
                for n in range(NS):
                    s2_copy(0, ab, n).wait_recv()

            @pl.when(p > 0)
            def _():
                s2_copy(p, ab).wait_recv()
            for t in range(3):
                r2[p, ab, t] = r2[p, ab, t] + (rd[p, 0, t, :, mx] if ab == 0 else rd[p, 1, t, my])
            s3_copies(p)[ab].start()

    def stage4(p):
        for ab in range(2):
            s3_copies(p)[ab].wait_recv()
            keep = my if ab == 0 else mx
            a = r3[p, ab, 0] + r2[p, ab, 0, keep]
            b = r3[p, ab, 1] + r2[p, ab, 1, keep]
            g = r3[p, ab, 2] + r2[p, ab, 2, keep]
            s = jax.nn.sigmoid(a)
            silu = a * s
            gat[p, ab, c, my, mx, 0] = (silu * b).astype(BF)
            gat[p, ab, c, my, mx, 1] = (g * b * (s * (1.0 + a * (1.0 - s)))).astype(BF)
            gat[p, ab, c, my, mx, 2] = (g * silu).astype(BF)
            s4_copies(p, my, mx)[ab].start()

    def stage5(p):
        for ab in range(2):
            s4_copies(p, 1 - my, 1 - mx)[ab].wait_recv()

            @pl.when(p < last)
            def _():
                s5_copies(p, mx, my)[ab].start()

            @pl.when(p == last)
            def _():
                for n in range(NS):
                    s5_copies(last, mx, my, n)[ab].start()

    def stage6(p):
        for cp in s5_copies(p, 1 - mx, 1 - my):
            cp.wait_recv()
        s6_copy(p, c).start()

    def accumulate(j, v):
        acc[j] = acc[j] + v.reshape(16, 8, DL)

    def y_part(p, lo, w):
        v = None
        for ab in range(2):
            h = gat[p, ab, :, :, :, 0, :, lo:lo + w].reshape(128, w)
            d = _dot(h, wd[p, ab * FC + lo:ab * FC + lo + w, :], 1, 0)
            v = d if v is None else v + d
        accumulate(0, v)

    def dx_part(p, lo, w):
        v = None
        for ab in range(2):
            for t, wt in ((1, wg), (2, wu)):
                z = gat[p, ab, :, :, :, t, :, lo:lo + w].reshape(128, w)
                d = _dot(z, wt[p, :, ab * FC + lo:ab * FC + lo + w], 1, 1)
                v = d if v is None else v + d
        accumulate(1, v)

    def stage7(p):
        s6_copy(p, 1 - c).wait_recv()
        y_part(p, 0, FC)
        dx_part(p, 0, FC)

    for cp in w_copies(0):
        cp.wait()
    for n in range(NS):
        for ab in range(2):
            product(0, ab, n)
            d_copy(0, ab, n).start()
    for n in range(NS):
        for ab in range(2):
            d_copy(0, ab, n).wait_recv()
            rd[0, ab, :, :, :, :, sub(n)] = rd[0, ab, :, :, :, :, sub(n)] + part[0, c, ab, :, :, :, :, sub(n)]
            s2_copy(0, ab, n).start()

    @pl.loop(0, NP + 4)
    def _(i):
        pl.when((i >= 1) & (i < NP))(lambda: stage2(i))
        pl.when((i >= 1) & (i < NP + 1))(lambda: stage3(i - 1))
        pl.when((i >= 2) & (i < NP + 2))(lambda: stage4(i - 2))
        pl.when((i >= 3) & (i < NP + 3))(lambda: stage5(i - 3))
        pl.when((i >= 4) & (i < NP + 3))(lambda: stage6(i - 4))
        pl.when(i < NP - 1)(lambda: products(i + 1))
        pl.when(i >= 5)(lambda: stage7(i - 5))

    def o_copy(j, k, slot):
        ot, od = other(k)
        return remote(acc.at[j, blk(ot, od)], fin.at[j, slot], o_send.at[j, k], o_recv.at[j, slot], (ot, od))

    def send_out(j):
        @pl.loop(1, 16)
        def _(k):
            o_copy(j, k, me).start()
        fin[j, me] = acc[j, mine]

    for n in range(NS):
        for cp in s5_copies(last, 1 - mx, 1 - my, n):
            cp.wait_recv()
        s6_copy(last, c, n).start()
    for n in range(NS):
        s6_copy(last, 1 - c, n).wait_recv()
        y_part(last, n * SUB, SUB)
        if n == NS - 1:
            send_out(0)
        dx_part(last, n * SUB, SUB)
    send_out(1)

    @pl.loop(0, NP)
    def _(p):
        for cp in (*s3_copies(p), *s4_copies(p, my, mx)):
            cp.wait_send()

    @pl.loop(1, NP)
    def _(p):
        for ab in range(2):
            s2_copy(p, ab).wait_send()

    @pl.loop(0, NP - 1)
    def _(p):
        for cp in (*s5_copies(p, mx, my), s6_copy(p, c)):
            cp.wait_send()
    for n in range(NS):
        for ab in range(2):
            s2_copy(0, ab, n).wait_send()
            s5_copies(last, mx, my, n)[ab].wait_send()
        s6_copy(last, c, n).wait_send()
    for p in (NP - 2, NP - 1):
        for ab in range(2):
            d_copy(p, ab).wait_send()

    @pl.loop(1, 16)
    def _(k):
        x_copy(k, mine).wait_send()

    for j, out in enumerate((y_ref, gx_ref)):
        @pl.loop(1, 16)
        def _(k):
            ot, od = other(k)
            o_copy(j, k, ot * 8 + od).wait_recv()
        for dd in range(8):
            cols = slice(dd * DL, (dd + 1) * DL)
            out[:, cols] = (rows[j, :, cols].astype(F32) + (fin[j, dd] + fin[j, 8 + dd])).astype(BF)

    @pl.loop(1, 16)
    def _(k):
        for j in range(2):
            o_copy(j, k, me).wait_send()


def wgrad_kernel(xs_ref, g_ref, y_ref, gx_ref, yo_ref, gxo_ref, dwg_ref, dwu_ref, dwd_ref):
    @pl.when(pl.program_id(0) == 0)
    def _():
        yo_ref[...] = y_ref[...]
        gxo_ref[...] = gx_ref[...]
    p, ab = pl.program_id(0) // 2, lax.rem(pl.program_id(0), 2)
    h = g_ref[p, ab, :, :, :, 0].reshape(128, FC)
    da = g_ref[p, ab, :, :, :, 1].reshape(128, FC)
    db = g_ref[p, ab, :, :, :, 2].reshape(128, FC)
    dwg_ref[...] = _dot(xs_ref[0], da, 0, 0)
    dwu_ref[...] = _dot(xs_ref[0], db, 0, 0)
    dwd_ref[...] = _dot(h, xs_ref[1], 0, 0)


def local_step(x_loc, wg_loc, wu_loc, wd_loc, gy_loc):
    vm = pl.BlockSpec(memory_space=pltpu.VMEM)
    hb = pl.BlockSpec(memory_space=pl.ANY)
    dma = pltpu.SemaphoreType.DMA
    row = jax.ShapeDtypeStruct((8, D), BF)
    y_rows, gx_rows, xs, gathered = pl.pallas_call(
        comm_kernel,
        out_shape=(pltpu.VMEM((8, D), BF), pltpu.VMEM((8, D), BF), pltpu.VMEM((2, 128, DL), BF),
                   pltpu.VMEM((NP, 2, 2, 2, 2, 3, 16, FC), BF)),
        in_specs=[pl.BlockSpec(memory_space=pltpu.HBM)] * 2 + [hb, hb, hb],
        out_specs=(vm, vm, vm, vm),
        scratch_shapes=[
            pltpu.VMEM((2, 8, D), BF),
            pltpu.VMEM((NP, DL, 2 * FC), BF),
            pltpu.VMEM((NP, DL, 2 * FC), BF),
            pltpu.VMEM((NP, 2 * FC, DL), BF),
            pltpu.VMEM((8, 2, 8, DL), BF),
            pltpu.VMEM((16, 2, 8, DL), BF),
            pltpu.VMEM((2, 2, 2, 3, 2, 2, 16, FC), F32),
            pltpu.VMEM((NP, 2, 3, 2, 2, 16, FC), F32),
            pltpu.VMEM((NP, 2, 3, 2, 16, FC), F32),
            pltpu.VMEM((NP, 2, 3, 16, FC), F32),
            pltpu.VMEM((2, 16, 8, DL), F32),
            pltpu.VMEM((2, 16, 8, DL), F32),
            dma((2,)), dma((3, NP)), dma((16,)), dma((16,)),
            dma((2, NP)), dma((2, NP)), dma((2, NS)), dma((2, NS)),
            dma((2, NP)), dma((2, NP)), dma((2, NS)), dma((2, NS)),
            dma((2, NP)), dma((2, NP)), dma((2, NP)), dma((2, NP)),
            dma((2, NP)), dma((2, NP)), dma((2, NS)), dma((2, NS)),
            dma((NP,)), dma((NP,)), dma((NS,)), dma((NS,)),
            dma((2, 16)), dma((2, 16)),
        ],
        compiler_params=pltpu.CompilerParams(
            collective_id=0, has_side_effects=True, vmem_limit_bytes=51000 * 1024),
        name="mlp_comm",
    )(x_loc, gy_loc, wg_loc, wu_loc, wd_loc)

    rows_spec = pl.BlockSpec((8, D), lambda k: (0, 0))
    return pl.pallas_call(
        wgrad_kernel,
        grid=(2 * NP,),
        out_shape=(row, row,
                   jax.ShapeDtypeStruct((DL, FF_LOC), F32), jax.ShapeDtypeStruct((DL, FF_LOC), F32),
                   jax.ShapeDtypeStruct((FF_LOC, DL), F32)),
        in_specs=[vm, vm, vm, vm],
        out_specs=(rows_spec, rows_spec,
                   pl.BlockSpec((DL, FC), lambda k: (0, k)), pl.BlockSpec((DL, FC), lambda k: (0, k)),
                   pl.BlockSpec((FC, DL), lambda k: (k, 0))),
        compiler_params=pltpu.CompilerParams(dimension_semantics=("arbitrary",), vmem_limit_bytes=20000 * 1024),
        name="mlp_wgrad",
    )(xs, gathered, y_rows, gx_rows)


def solution(mesh):
    row_spec = P(("dp", "tp"), None)
    up_spec = P("dp", "tp")
    down_spec = P("tp", "dp")
    return jax.shard_map(local_step, mesh=mesh,
                         in_specs=(row_spec, up_spec, up_spec, down_spec, row_spec),
                         out_specs=(row_spec, row_spec, up_spec, up_spec, down_spec),
                         check_vma=False)
```

```python
import functools

import jax
import jax.numpy as jnp
from jax import lax
from jax.experimental import pallas as pl
from jax.experimental.pallas import tpu as pltpu
from jax.sharding import PartitionSpec as P

MESH = pl.DeviceIdType.MESH
BF = jnp.bfloat16
F32 = jnp.float32

D = 3072
FF_LOC = 12288
DL = 384
NP = 8
N1 = 5
NB = NP - N1
FC = FF_LOC // (2 * NP)
NS = 3
SUB = FC // NS


def _dot(a, b, ca, cb):
    return lax.dot_general(a, b, (((ca,), (cb,)), ((), ())), preferred_element_type=F32)


def remote(src, dst, send, recv, dev):
    return pltpu.make_async_remote_copy(src_ref=src, dst_ref=dst, send_sem=send, recv_sem=recv,
                                        device_id=dev, device_id_type=MESH)


def sub(n):
    return pl.ds(n * SUB, SUB)


def blk(tt, dd):
    return (lax.rem(dd, 2) * 4 + (dd // 4) * 2 + lax.rem(dd // 2, 2)) * 2 + tt


class Place:
    def __init__(self):
        tp, dp = lax.axis_index("tp"), lax.axis_index("dp")
        c, x, y = lax.rem(dp, 2), lax.rem(dp // 2, 2), dp // 4
        self.tp, self.dp, self.c, self.x, self.y = tp, dp, c, x, y
        self.me = tp * 8 + dp
        self.core_nb = (tp, y * 4 + x * 2 + (1 - c))
        self.x_nb = (tp, y * 4 + (1 - x) * 2 + c)
        self.y_nb = (tp, (1 - y) * 4 + x * 2 + c)
        self.mine = blk(tp, dp)

    def other(self, k):
        o = lax.rem(self.me + k, 16)
        return o // 8, lax.rem(o, 8)

    def greet(self):
        barrier = pltpu.get_barrier_semaphore()

        @pl.loop(1, 16)
        def _(k):
            pl.semaphore_signal(barrier, inc=1, device_id=self.other(k), device_id_type=MESH)
        return barrier


def silu_parts(a, b, g):
    s = jax.nn.sigmoid(a)
    silu = a * s
    return ((silu * b).astype(BF), (g * b * (s * (1.0 + a * (1.0 - s)))).astype(BF), (g * silu).astype(BF))


def accumulate(acc, j, v):
    acc[j] = acc[j] + v.reshape(16, 8, DL)


def y_part(acc, gat, wd, q, lo, w):
    v = None
    for ab in range(2):
        h = gat[q, ab, :, :, :, 0, :, lo:lo + w].reshape(128, w)
        d = _dot(h, wd(q, ab * FC + lo, w), 1, 0)
        v = d if v is None else v + d
    accumulate(acc, 0, v)


def dx_part(acc, gat, wg, wu, q, lo, w):
    v = None
    for ab in range(2):
        for t, wt in ((1, wg), (2, wu)):
            z = gat[q, ab, :, :, :, t, :, lo:lo + w].reshape(128, w)
            d = _dot(z, wt(q, ab * FC + lo, w), 1, 1)
            v = d if v is None else v + d
    accumulate(acc, 1, v)


class Gather:
    def __init__(self, at, gat, s4, s5, s6, s5l=None, s6l=None):
        self.at, self.gat, self.s4, self.s5, self.s6, self.s5l, self.s6l = at, gat, s4, s5, s6, s5l, s6l

    def first(self, q, ab, arriving):
        at = self.at
        y0 = (1 - at.y) if arriving else at.y
        x1 = (1 - at.x) if arriving else at.x
        b = self.gat.at[q, 0, at.c, y0, at.x] if ab == 0 else self.gat.at[q, 1, at.c, at.y, x1]
        return remote(b, b, self.s4[0].at[ab, q], self.s4[1].at[ab, q], at.y_nb if ab == 0 else at.x_nb)

    def second(self, q, ab, arriving, n=None):
        at = self.at
        x0 = (1 - at.x) if arriving else at.x
        y1 = (1 - at.y) if arriving else at.y
        b = self.gat.at[q, 0, at.c, :, x0] if ab == 0 else self.gat.at[q, 1, at.c, y1]
        dev = at.x_nb if ab == 0 else at.y_nb
        if n is None:
            return remote(b, b, self.s5[0].at[ab, q], self.s5[1].at[ab, q], dev)
        b = b.at[:, :, :, sub(n)]
        return remote(b, b, self.s5l[0].at[ab, n], self.s5l[1].at[ab, n], dev)

    def third(self, q, arriving, n=None):
        at = self.at
        b = self.gat.at[q, :, (1 - at.c) if arriving else at.c]
        if n is None:
            return remote(b, b, self.s6[0].at[q], self.s6[1].at[q], at.core_nb)
        b = b.at[:, :, :, :, :, sub(n)]
        return remote(b, b, self.s6l[0].at[n], self.s6l[1].at[n], at.core_nb)


def first_kernel(x_hbm, gy_hbm, wg_hbm, wu_hbm, wd_hbm,
                 xs_ref, gat, acc, rows, sx, sy, kx, ky, r2n,
                 wg, wu, wd, rd, r2, st, xin, part, r3,
                 in_sem, w_sem, x_send, x_recv, d_send, d_recv, d0_send, d0_recv, s2_send, s2_recv, s20_send, s20_recv,
                 s3_send, s3_recv, s4_send, s4_recv, s5_send, s5_recv, s6_send, s6_recv):
    at = Place()
    c, mx, my = at.c, at.x, at.y
    net = Gather(at, gat, (s4_send, s4_recv), (s5_send, s5_recv), (s6_send, s6_recv))

    def w_copies(p):
        cols = pl.ds(pl.multiple_of(p * 2 * FC, 2 * FC), 2 * FC)
        return (pltpu.make_async_copy(wg_hbm.at[:, cols], wg.at[p], w_sem.at[0, p]),
                pltpu.make_async_copy(wu_hbm.at[:, cols], wu.at[p], w_sem.at[1, p]),
                pltpu.make_async_copy(wd_hbm.at[cols, :], wd.at[p], w_sem.at[2, p]))

    in_copies = [pltpu.make_async_copy(r, rows.at[j], in_sem.at[j]) for j, r in enumerate((x_hbm, gy_hbm))]
    for cp in in_copies:
        cp.start()
    barrier = at.greet()

    @pl.loop(0, NP)
    def _(p):
        for cp in w_copies(p):
            cp.start()

    acc[...] = jnp.zeros_like(acc)
    for j in range(2):
        in_copies[j].wait()
        for dd in range(8):
            st[dd, j] = rows[j, :, dd * DL:(dd + 1) * DL]
    pl.semaphore_wait(barrier, 15)

    def x_copy(k, b):
        ot, od = at.other(k)
        return remote(st.at[od], xin.at[b], x_send.at[k], x_recv.at[b], (ot, od))

    @pl.loop(1, 16)
    def _(k):
        x_copy(k, at.mine).start()

    xin[at.mine] = st[at.dp]

    @pl.loop(1, 16)
    def _(k):
        x_copy(k, blk(*at.other(k))).wait_recv()

    for j in range(2):
        xs_ref[j] = xin[:, j].astype(F32).reshape(128, DL).astype(BF)

    def d_copy(p, ab, n=None):
        s = lax.rem(p, 2)
        if n is None:
            return remote(part.at[s, 1 - c, ab], rd.at[p, ab], d_send.at[ab, p], d_recv.at[ab, p], at.core_nb)
        return remote(part.at[s, 1 - c, ab, :, :, :, :, sub(n)], rd.at[p, ab, :, :, :, :, sub(n)],
                      d0_send.at[ab, n], d0_recv.at[ab, n], at.core_nb)

    def s2_copy(p, ab, n=None):
        src = rd.at[p, 0, :, :, 1 - mx] if ab == 0 else rd.at[p, 1, :, 1 - my]
        dst = r2n.at[ab] if p is N1 else r2.at[p, ab]
        dev = at.x_nb if ab == 0 else at.y_nb
        if n is None:
            return remote(src, dst, s2_send.at[ab, p], s2_recv.at[ab, p], dev)
        return remote(src.at[:, :, :, sub(n)], dst.at[:, :, :, sub(n)], s20_send.at[ab, n], s20_recv.at[ab, n], dev)

    def s3_copy(p, ab):
        src = r2.at[p, 0, :, 1 - my] if ab == 0 else r2.at[p, 1, :, 1 - mx]
        return remote(src, r3.at[p, ab], s3_send.at[ab, p], s3_recv.at[ab, p], at.y_nb if ab == 0 else at.x_nb)

    def product(p, ab, n):
        s = lax.rem(p, 2)
        cols = pl.ds(ab * FC + n * SUB, SUB)
        vals = (_dot(xs_ref[0], wg[p, :, cols], 1, 0),
                _dot(xs_ref[0], wu[p, :, cols], 1, 0),
                _dot(xs_ref[1], wd[p, cols, :], 1, 1))
        for t in range(3):
            v = vals[t].reshape(2, 2, 2, 16, SUB)
            for cc in range(2):
                part[s, cc, ab, t, :, :, :, sub(n)] = v[cc]

    def products(p):
        for cp in w_copies(p):
            cp.wait()
        for ab in range(2):
            @pl.when(p >= 3)
            def _():
                d_copy(p - 2, ab).wait_send()

            @pl.when(p == 2)
            def _():
                for n in range(NS):
                    d_copy(0, ab, n).wait_send()
            for n in range(NS):
                product(p, ab, n)
            d_copy(p, ab).start()

    def stage2(p):
        s = lax.rem(p, 2)
        for ab in range(2):
            d_copy(p, ab).wait_recv()
            for t in range(3):
                rd[p, ab, t] = rd[p, ab, t] + part[s, c, ab, t]

            @pl.when(p < N1)
            def _():
                s2_copy(p, ab).start()

        @pl.when(p >= N1)
        def _():
            for t in range(3):
                kx[p - N1, t] = rd[p, 0, t, :, mx]
                ky[p - N1, t] = rd[p, 1, t, my]

        @pl.when(p > N1)
        def _():
            for t in range(3):
                sx[p - N1 - 1, t] = rd[p, 0, t, :, 1 - mx]
                sy[p - N1 - 1, t] = rd[p, 1, t, 1 - my]

    def stage3(p):
        for ab in range(2):
            @pl.when(p == 0)
            def _():
                for n in range(NS):
                    s2_copy(0, ab, n).wait_recv()

            @pl.when(p > 0)
            def _():
                s2_copy(p, ab).wait_recv()
            for t in range(3):
                r2[p, ab, t] = r2[p, ab, t] + (rd[p, 0, t, :, mx] if ab == 0 else rd[p, 1, t, my])
            s3_copy(p, ab).start()

    def stage4(p):
        for ab in range(2):
            s3_copy(p, ab).wait_recv()
            keep = my if ab == 0 else mx
            vals = silu_parts(*(r3[p, ab, t] + r2[p, ab, t, keep] for t in range(3)))
            for t in range(3):
                gat[p, ab, c, my, mx, t] = vals[t]
            net.first(p, ab, False).start()

    def stage5(p):
        for ab in range(2):
            net.first(p, ab, True).wait_recv()
            net.second(p, ab, False).start()

        @pl.when(p == N1 - 1)
        def _():
            for ab in range(2):
                s2_copy(N1, ab).start()

    def stage6(p):
        for ab in range(2):
            net.second(p, ab, True).wait_recv()
        net.third(p, False).start()

    def stage7(p):
        net.third(p, True).wait_recv()
        y_part(acc, gat, lambda q, lo, w: wd[q, lo:lo + w, :], p, 0, FC)
        dx_part(acc, gat, *(lambda q, lo, w, r=r: r[q, :, lo:lo + w] for r in (wg, wu)), p, 0, FC)

    for cp in w_copies(0):
        cp.wait()
    for n in range(NS):
        for ab in range(2):
            product(0, ab, n)
            d_copy(0, ab, n).start()
    for n in range(NS):
        for ab in range(2):
            d_copy(0, ab, n).wait_recv()
            rd[0, ab, :, :, :, :, sub(n)] = rd[0, ab, :, :, :, :, sub(n)] + part[0, c, ab, :, :, :, :, sub(n)]
            s2_copy(0, ab, n).start()

    @pl.loop(0, N1 + 5)
    def _(i):
        pl.when((i >= 1) & (i < NP))(lambda: stage2(i))
        pl.when((i >= 1) & (i < N1 + 1))(lambda: stage3(i - 1))
        pl.when((i >= 2) & (i < N1 + 2))(lambda: stage4(i - 2))
        pl.when((i >= 3) & (i < N1 + 3))(lambda: stage5(i - 3))
        pl.when((i >= 4) & (i < N1 + 4))(lambda: stage6(i - 4))
        pl.when(i < NP - 1)(lambda: products(i + 1))
        pl.when(i >= 5)(lambda: stage7(i - 5))

    @pl.loop(0, N1)
    def _(p):
        for ab in range(2):
            s3_copy(p, ab).wait_send()
            net.first(p, ab, False).wait_send()
            net.second(p, ab, False).wait_send()
        net.third(p, False).wait_send()

    @pl.loop(1, N1)
    def _(p):
        for ab in range(2):
            s2_copy(p, ab).wait_send()
    for n in range(NS):
        for ab in range(2):
            s2_copy(0, ab, n).wait_send()
    for p in (NP - 2, NP - 1):
        for ab in range(2):
            d_copy(p, ab).wait_send()

    @pl.loop(1, 16)
    def _(k):
        x_copy(k, at.mine).wait_send()
    for ab in range(2):
        s2_copy(N1, ab).wait_send()
        s2_copy(N1, ab).wait_recv()


def second_kernel(wg_hbm, wu_hbm, wd_hbm, acc_in, rows, rx, ry, kx, ky, r2n,
                  y_ref, gx_ref, gat,
                  wg, wu, wd, r2b, r3, acc, fin,
                  w_sem, s3_send, s3_recv, s4_send, s4_recv, s5_send, s5_recv, s5l_send, s5l_recv,
                  s6_send, s6_recv, s6l_send, s6l_recv, o_send, o_recv):
    at = Place()
    c, mx, my = at.c, at.x, at.y
    net = Gather(at, gat, (s4_send, s4_recv), (s5_send, s5_recv), (s6_send, s6_recv),
                 (s5l_send, s5l_recv), (s6l_send, s6l_recv))
    barrier = at.greet()
    cols = pl.ds(N1 * 2 * FC, NB * 2 * FC)
    w_copies = (pltpu.make_async_copy(wg_hbm.at[:, cols], wg, w_sem.at[0]),
                pltpu.make_async_copy(wu_hbm.at[:, cols], wu, w_sem.at[1]),
                pltpu.make_async_copy(wd_hbm.at[cols, :], wd, w_sem.at[2]))
    for cp in w_copies:
        cp.start()

    def s3_copy(q, ab):
        src = r2b.at[q, 0, :, 1 - my] if ab == 0 else r2b.at[q, 1, :, 1 - mx]
        return remote(src, r3.at[q, ab], s3_send.at[ab, q], s3_recv.at[ab, q], at.y_nb if ab == 0 else at.x_nb)

    for q in range(NB):
        for ab in range(2):
            for t in range(3):
                got = r2n[ab, t] if q == 0 else (rx, ry)[ab][q - 1, t]
                r2b[q, ab, t] = got + (kx, ky)[ab][q, t]
    pl.semaphore_wait(barrier, 15)
    for q in range(NB):
        for ab in range(2):
            s3_copy(q, ab).start()
    acc[...] = acc_in[...]

    for q in range(NB):
        for ab in range(2):
            s3_copy(q, ab).wait_recv()
            keep = my if ab == 0 else mx
            vals = silu_parts(*(r3[q, ab, t] + r2b[q, ab, t, keep] for t in range(3)))
            for t in range(3):
                gat[q, ab, c, my, mx, t] = vals[t]
            net.first(q, ab, False).start()

    for q in range(NB):
        for ab in range(2):
            net.first(q, ab, True).wait_recv()
            if q < NB - 1:
                net.second(q, ab, False).start()
            else:
                for n in range(NS):
                    net.second(q, ab, False, n).start()

    for q in range(NB - 1):
        for ab in range(2):
            net.second(q, ab, True).wait_recv()
        net.third(q, False).start()

    def down(q, lo, w):
        return wd[q * 2 * FC + lo:q * 2 * FC + lo + w, :]

    def gate(q, lo, w):
        return wg[:, q * 2 * FC + lo:q * 2 * FC + lo + w]

    def up(q, lo, w):
        return wu[:, q * 2 * FC + lo:q * 2 * FC + lo + w]

    for cp in w_copies:
        cp.wait()
    for q in range(NB - 1):
        net.third(q, True).wait_recv()
        y_part(acc, gat, down, q, 0, FC)
        dx_part(acc, gat, gate, up, q, 0, FC)

    def o_copy(j, k, slot):
        ot, od = at.other(k)
        return remote(acc.at[j, blk(ot, od)], fin.at[j, slot], o_send.at[j, k], o_recv.at[j, slot], (ot, od))

    def send_out(j):
        @pl.loop(1, 16)
        def _(k):
            o_copy(j, k, at.me).start()
        fin[j, at.me] = acc[j, at.mine]

    q = NB - 1
    for n in range(NS):
        for ab in range(2):
            net.second(q, ab, True, n).wait_recv()
        net.third(q, False, n).start()
    for n in range(NS):
        net.third(q, True, n).wait_recv()
        y_part(acc, gat, down, q, n * SUB, SUB)
        if n == NS - 1:
            send_out(0)
        dx_part(acc, gat, gate, up, q, n * SUB, SUB)
    send_out(1)

    for q in range(NB):
        for ab in range(2):
            s3_copy(q, ab).wait_send()
            net.first(q, ab, False).wait_send()
            if q < NB - 1:
                net.second(q, ab, False).wait_send()
            else:
                for n in range(NS):
                    net.second(q, ab, False, n).wait_send()
        if q < NB - 1:
            net.third(q, False).wait_send()
        else:
            for n in range(NS):
                net.third(q, False, n).wait_send()

    for j, out in enumerate((y_ref, gx_ref)):
        @pl.loop(1, 16)
        def _(k):
            ot, od = at.other(k)
            o_copy(j, k, ot * 8 + od).wait_recv()
        for dd in range(8):
            cols = slice(dd * DL, (dd + 1) * DL)
            out[:, cols] = (rows[j, :, cols].astype(F32) + (fin[j, dd] + fin[j, 8 + dd])).astype(BF)

    @pl.loop(1, 16)
    def _(k):
        for j in range(2):
            o_copy(j, k, at.me).wait_send()


def grads(xs_ref, g_ref, dwg_ref, dwu_ref, dwd_ref):
    q, ab = pl.program_id(0) // 2, lax.rem(pl.program_id(0), 2)
    h = g_ref[q, ab, :, :, :, 0].reshape(128, FC)
    da = g_ref[q, ab, :, :, :, 1].reshape(128, FC)
    db = g_ref[q, ab, :, :, :, 2].reshape(128, FC)
    dwg_ref[...] = _dot(xs_ref[0], da, 0, 0)
    dwu_ref[...] = _dot(xs_ref[0], db, 0, 0)
    dwd_ref[...] = _dot(h, xs_ref[1], 0, 0)


def early_grads(xs_ref, g_ref, dwg_ref, dwu_ref, dwd_ref):
    grads(xs_ref, g_ref, dwg_ref, dwu_ref, dwd_ref)


def late_grads(xs_ref, g_ref, y_ref, gx_ref, a_ref, b_ref, c_ref, yo_ref, gxo_ref, dwg_ref, dwu_ref, dwd_ref):
    @pl.when(pl.program_id(0) == 0)
    def _():
        yo_ref[...] = y_ref[...]
        gxo_ref[...] = gx_ref[...]
    grads(xs_ref, g_ref, dwg_ref, dwu_ref, dwd_ref)


def local_step(x_loc, wg_loc, wu_loc, wd_loc, gy_loc):
    vm = pl.BlockSpec(memory_space=pltpu.VMEM)
    hb = pl.BlockSpec(memory_space=pl.ANY)
    hbm = pl.BlockSpec(memory_space=pltpu.HBM)
    dma = pltpu.SemaphoreType.DMA
    row = jax.ShapeDtypeStruct((8, D), BF)
    kib = 1024
    half = (3, 2, 16, FC)
    xs, gat1, acc, rows, sx, sy, kx, ky, r2n = pl.pallas_call(
        first_kernel,
        out_shape=(pltpu.VMEM((2, 128, DL), BF), pltpu.VMEM((N1, 2, 2, 2, 2, 3, 16, FC), BF),
                   pltpu.VMEM((2, 16, 8, DL), F32), pltpu.VMEM((2, 8, D), BF),
                   pltpu.VMEM((NB - 1,) + half, F32), pltpu.VMEM((NB - 1,) + half, F32),
                   pltpu.VMEM((NB,) + half, F32), pltpu.VMEM((NB,) + half, F32), pltpu.VMEM((2,) + half, F32)),
        in_specs=[hbm] * 5,
        out_specs=(vm,) * 9,
        scratch_shapes=[
            pltpu.VMEM((NP, DL, 2 * FC), BF),
            pltpu.VMEM((NP, DL, 2 * FC), BF),
            pltpu.VMEM((NP, 2 * FC, DL), BF),
            pltpu.VMEM((NP, 2, 3, 2, 2, 16, FC), F32),
            pltpu.VMEM((N1, 2) + half, F32),
            pltpu.VMEM((8, 2, 8, DL), BF),
            pltpu.VMEM((16, 2, 8, DL), BF),
            pltpu.VMEM((2, 2, 2, 3, 2, 2, 16, FC), F32),
            pltpu.VMEM((N1, 2, 3, 16, FC), F32),
            dma((2,)), dma((3, NP)), dma((16,)), dma((16,)),
            dma((2, NP)), dma((2, NP)), dma((2, NS)), dma((2, NS)),
            dma((2, NP)), dma((2, NP)), dma((2, NS)), dma((2, NS)),
            dma((2, N1)), dma((2, N1)), dma((2, N1)), dma((2, N1)),
            dma((2, N1)), dma((2, N1)), dma((N1,)), dma((N1,)),
        ],
        compiler_params=pltpu.CompilerParams(
            collective_id=0, has_side_effects=True, vmem_limit_bytes=49000 * kib),
        name="mlp_first",
    )(x_loc, gy_loc, wg_loc, wu_loc, wd_loc)

    rx = lax.ppermute(sx, "dp", [(i, i + 2 if i % 4 < 2 else i - 2) for i in range(8)])
    ry = lax.ppermute(sy, "dp", [(i, (i + 4) % 8) for i in range(8)])

    full = (jax.ShapeDtypeStruct((DL, FF_LOC), F32), jax.ShapeDtypeStruct((DL, FF_LOC), F32),
            jax.ShapeDtypeStruct((FF_LOC, DL), F32))

    def grad_specs(first):
        return (pl.BlockSpec((DL, FC), lambda k: (0, k + first)), pl.BlockSpec((DL, FC), lambda k: (0, k + first)),
                pl.BlockSpec((FC, DL), lambda k: (k + first, 0)))

    def cost(n):
        return pl.CostEstimate(flops=12 * n * 128 * DL * FC, bytes_accessed=24 * n * DL * FC, transcendentals=0)

    dwg, dwu, dwd = pl.pallas_call(
        early_grads,
        grid=(2 * N1,),
        out_shape=full,
        in_specs=[vm, vm],
        out_specs=grad_specs(0),
        cost_estimate=cost(N1),
        compiler_params=pltpu.CompilerParams(dimension_semantics=("arbitrary",), vmem_limit_bytes=9000 * kib),
        name="mlp_early_grads",
    )(xs, gat1)

    y_rows, gx_rows, gat2 = pl.pallas_call(
        second_kernel,
        out_shape=(pltpu.VMEM((8, D), BF), pltpu.VMEM((8, D), BF), pltpu.VMEM((NB, 2, 2, 2, 2, 3, 16, FC), BF)),
        in_specs=[hbm] * 3 + [vm] * 7,
        out_specs=(vm,) * 3,
        scratch_shapes=[
            pltpu.VMEM((DL, NB * 2 * FC), BF),
            pltpu.VMEM((DL, NB * 2 * FC), BF),
            pltpu.VMEM((NB * 2 * FC, DL), BF),
            pltpu.VMEM((NB, 2) + half, F32),
            pltpu.VMEM((NB, 2, 3, 16, FC), F32),
            pltpu.VMEM((2, 16, 8, DL), F32),
            pltpu.VMEM((2, 16, 8, DL), F32),
            dma((3,)), dma((2, NB)), dma((2, NB)), dma((2, NB)), dma((2, NB)),
            dma((2, NB)), dma((2, NB)), dma((2, NS)), dma((2, NS)),
            dma((NB,)), dma((NB,)), dma((NS,)), dma((NS,)),
            dma((2, 16)), dma((2, 16)),
        ],
        compiler_params=pltpu.CompilerParams(
            collective_id=1, has_side_effects=True, vmem_limit_bytes=48000 * kib),
        name="mlp_second",
    )(wg_loc, wu_loc, wd_loc, acc, rows, rx, ry, kx, ky, r2n)

    rows_spec = pl.BlockSpec((8, D), lambda k: (0, 0))
    return pl.pallas_call(
        late_grads,
        grid=(2 * NB,),
        out_shape=(row, row) + full,
        in_specs=[vm, vm, vm, vm, hbm, hbm, hbm],
        out_specs=(rows_spec, rows_spec) + grad_specs(2 * N1),
        input_output_aliases={4: 2, 5: 3, 6: 4},
        cost_estimate=cost(NB),
        compiler_params=pltpu.CompilerParams(dimension_semantics=("arbitrary",), vmem_limit_bytes=50000 * kib),
        name="mlp_late_grads",
    )(xs, gat2, y_rows, gx_rows, dwg, dwu, dwd)


def solution(mesh):
    row_spec = P(("dp", "tp"), None)
    up_spec = P("dp", "tp")
    down_spec = P("tp", "dp")
    return jax.shard_map(local_step, mesh=mesh,
                         in_specs=(row_spec, up_spec, up_spec, down_spec, row_spec),
                         out_specs=(row_spec, row_spec, up_spec, up_spec, down_spec),
                         check_vma=False)
```

```python
import functools

import jax
import jax.numpy as jnp
from jax import lax
from jax.experimental import pallas as pl
from jax.experimental.pallas import tpu as pltpu
from jax.sharding import PartitionSpec as P

MESH = pl.DeviceIdType.MESH
BF = jnp.bfloat16
F32 = jnp.float32

D = 3072
FF_LOC = 12288
DL = 384
NP = 8
N1 = 5
NB = NP - N1
FC = FF_LOC // (2 * NP)
NS = 3
SUB = FC // NS


def _dot(a, b, ca, cb):
    return lax.dot_general(a, b, (((ca,), (cb,)), ((), ())), preferred_element_type=F32)


def remote(src, dst, send, recv, dev):
    return pltpu.make_async_remote_copy(src_ref=src, dst_ref=dst, send_sem=send, recv_sem=recv,
                                        device_id=dev, device_id_type=MESH)


def sub(n):
    return pl.ds(n * SUB, SUB)


def blk(tt, dd):
    return (lax.rem(dd, 2) * 4 + (dd // 4) * 2 + lax.rem(dd // 2, 2)) * 2 + tt


class Place:
    def __init__(self):
        tp, dp = lax.axis_index("tp"), lax.axis_index("dp")
        c, x, y = lax.rem(dp, 2), lax.rem(dp // 2, 2), dp // 4
        self.tp, self.dp, self.c, self.x, self.y = tp, dp, c, x, y
        self.me = tp * 8 + dp
        self.core_nb = (tp, y * 4 + x * 2 + (1 - c))
        self.x_nb = (tp, y * 4 + (1 - x) * 2 + c)
        self.y_nb = (tp, (1 - y) * 4 + x * 2 + c)
        self.mine = blk(tp, dp)

    def other(self, k):
        o = lax.rem(self.me + k, 16)
        return o // 8, lax.rem(o, 8)

    def greet(self):
        barrier = pltpu.get_barrier_semaphore()

        @pl.loop(1, 16)
        def _(k):
            pl.semaphore_signal(barrier, inc=1, device_id=self.other(k), device_id_type=MESH)
        return barrier


def silu_parts(a, b, g):
    s = jax.nn.sigmoid(a)
    silu = a * s
    return ((silu * b).astype(BF), (g * b * (s * (1.0 + a * (1.0 - s)))).astype(BF), (g * silu).astype(BF))


def accumulate(acc, j, v):
    acc[j] = acc[j] + v.reshape(16, 8, DL)


def y_part(acc, gat, wd, q, lo, w):
    v = None
    for ab in range(2):
        h = gat[q, ab, :, :, :, 0, :, lo:lo + w].reshape(128, w)
        d = _dot(h, wd(q, ab * FC + lo, w), 1, 0)
        v = d if v is None else v + d
    accumulate(acc, 0, v)


def dx_part(acc, gat, wg, wu, q, lo, w):
    v = None
    for ab in range(2):
        for t, wt in ((1, wg), (2, wu)):
            z = gat[q, ab, :, :, :, t, :, lo:lo + w].reshape(128, w)
            d = _dot(z, wt(q, ab * FC + lo, w), 1, 1)
            v = d if v is None else v + d
    accumulate(acc, 1, v)


class Gather:
    def __init__(self, at, gat, s4, s5, s6, s5l=None, s6l=None):
        self.at, self.gat, self.s4, self.s5, self.s6, self.s5l, self.s6l = at, gat, s4, s5, s6, s5l, s6l

    def first(self, q, ab, arriving):
        at = self.at
        y0 = (1 - at.y) if arriving else at.y
        x1 = (1 - at.x) if arriving else at.x
        b = self.gat.at[q, 0, at.c, y0, at.x] if ab == 0 else self.gat.at[q, 1, at.c, at.y, x1]
        return remote(b, b, self.s4[0].at[ab, q], self.s4[1].at[ab, q], at.y_nb if ab == 0 else at.x_nb)

    def second(self, q, ab, arriving, n=None):
        at = self.at
        x0 = (1 - at.x) if arriving else at.x
        y1 = (1 - at.y) if arriving else at.y
        b = self.gat.at[q, 0, at.c, :, x0] if ab == 0 else self.gat.at[q, 1, at.c, y1]
        dev = at.x_nb if ab == 0 else at.y_nb
        if n is None:
            return remote(b, b, self.s5[0].at[ab, q], self.s5[1].at[ab, q], dev)
        b = b.at[:, :, :, sub(n)]
        return remote(b, b, self.s5l[0].at[ab, n], self.s5l[1].at[ab, n], dev)

    def third(self, q, arriving, n=None):
        at = self.at
        b = self.gat.at[q, :, (1 - at.c) if arriving else at.c]
        if n is None:
            return remote(b, b, self.s6[0].at[q], self.s6[1].at[q], at.core_nb)
        b = b.at[:, :, :, :, :, sub(n)]
        return remote(b, b, self.s6l[0].at[n], self.s6l[1].at[n], at.core_nb)


def first_kernel(x_hbm, gy_hbm, wg_hbm, wu_hbm, wd_hbm,
                 xs_ref, gat, acc, rows, sx, sy, kx, ky, r2n,
                 wg, wu, wd, rd, r2, st, xin, part, r3,
                 in_sem, w_sem, x_send, x_recv, d_send, d_recv, d0_send, d0_recv, s2_send, s2_recv, s20_send, s20_recv,
                 s3_send, s3_recv, s4_send, s4_recv, s5_send, s5_recv, s6_send, s6_recv):
    at = Place()
    c, mx, my = at.c, at.x, at.y
    net = Gather(at, gat, (s4_send, s4_recv), (s5_send, s5_recv), (s6_send, s6_recv))

    def w_copies(p):
        cols = pl.ds(pl.multiple_of(p * 2 * FC, 2 * FC), 2 * FC)
        return (pltpu.make_async_copy(wg_hbm.at[:, cols], wg.at[p], w_sem.at[0, p]),
                pltpu.make_async_copy(wu_hbm.at[:, cols], wu.at[p], w_sem.at[1, p]),
                pltpu.make_async_copy(wd_hbm.at[cols, :], wd.at[p], w_sem.at[2, p]))

    in_copies = [pltpu.make_async_copy(r, rows.at[j], in_sem.at[j]) for j, r in enumerate((x_hbm, gy_hbm))]
    for cp in in_copies:
        cp.start()
    barrier = at.greet()

    @pl.loop(0, NP)
    def _(p):
        for cp in w_copies(p):
            cp.start()

    acc[...] = jnp.zeros_like(acc)
    for j in range(2):
        in_copies[j].wait()
        for dd in range(8):
            st[dd, j] = rows[j, :, dd * DL:(dd + 1) * DL]
    pl.semaphore_wait(barrier, 15)

    def x_copy(k, b):
        ot, od = at.other(k)
        return remote(st.at[od], xin.at[b], x_send.at[k], x_recv.at[b], (ot, od))

    @pl.loop(1, 16)
    def _(k):
        x_copy(k, at.mine).start()

    xin[at.mine] = st[at.dp]

    @pl.loop(1, 16)
    def _(k):
        x_copy(k, blk(*at.other(k))).wait_recv()

    for j in range(2):
        xs_ref[j] = xin[:, j].astype(F32).reshape(128, DL).astype(BF)

    def d_copy(p, ab, n=None):
        s = lax.rem(p, 2)
        if n is None:
            return remote(part.at[s, 1 - c, ab], rd.at[p, ab], d_send.at[ab, p], d_recv.at[ab, p], at.core_nb)
        return remote(part.at[s, 1 - c, ab, :, :, :, :, sub(n)], rd.at[p, ab, :, :, :, :, sub(n)],
                      d0_send.at[ab, n], d0_recv.at[ab, n], at.core_nb)

    def s2_copy(p, ab, n=None):
        src = rd.at[p, 0, :, :, 1 - mx] if ab == 0 else rd.at[p, 1, :, 1 - my]
        dst = r2n.at[ab] if p is N1 else r2.at[p, ab]
        dev = at.x_nb if ab == 0 else at.y_nb
        if n is None:
            return remote(src, dst, s2_send.at[ab, p], s2_recv.at[ab, p], dev)
        return remote(src.at[:, :, :, sub(n)], dst.at[:, :, :, sub(n)], s20_send.at[ab, n], s20_recv.at[ab, n], dev)

    def s3_copy(p, ab):
        src = r2.at[p, 0, :, 1 - my] if ab == 0 else r2.at[p, 1, :, 1 - mx]
        return remote(src, r3.at[p, ab], s3_send.at[ab, p], s3_recv.at[ab, p], at.y_nb if ab == 0 else at.x_nb)

    def product(p, ab, n):
        s = lax.rem(p, 2)
        cols = pl.ds(ab * FC + n * SUB, SUB)
        vals = (_dot(xs_ref[0], wg[p, :, cols], 1, 0),
                _dot(xs_ref[0], wu[p, :, cols], 1, 0),
                _dot(xs_ref[1], wd[p, cols, :], 1, 1))
        for t in range(3):
            v = vals[t].reshape(2, 2, 2, 16, SUB)
            for cc in range(2):
                part[s, cc, ab, t, :, :, :, sub(n)] = v[cc]

    def products(p):
        for cp in w_copies(p):
            cp.wait()
        for ab in range(2):
            @pl.when(p >= 3)
            def _():
                d_copy(p - 2, ab).wait_send()

            @pl.when(p == 2)
            def _():
                for n in range(NS):
                    d_copy(0, ab, n).wait_send()
            for n in range(NS):
                product(p, ab, n)
            d_copy(p, ab).start()

    def stage2(p):
        s = lax.rem(p, 2)
        for ab in range(2):
            d_copy(p, ab).wait_recv()
            for t in range(3):
                rd[p, ab, t] = rd[p, ab, t] + part[s, c, ab, t]

            @pl.when(p < N1)
            def _():
                s2_copy(p, ab).start()

        @pl.when(p >= N1)
        def _():
            for t in range(3):
                kx[p - N1, t] = rd[p, 0, t, :, mx]
                ky[p - N1, t] = rd[p, 1, t, my]

        @pl.when(p > N1)
        def _():
            for t in range(3):
                sx[p - N1 - 1, t] = rd[p, 0, t, :, 1 - mx]
                sy[p - N1 - 1, t] = rd[p, 1, t, 1 - my]

    def stage3(p):
        for ab in range(2):
            @pl.when(p == 0)
            def _():
                for n in range(NS):
                    s2_copy(0, ab, n).wait_recv()

            @pl.when(p > 0)
            def _():
                s2_copy(p, ab).wait_recv()
            for t in range(3):
                r2[p, ab, t] = r2[p, ab, t] + (rd[p, 0, t, :, mx] if ab == 0 else rd[p, 1, t, my])
            s3_copy(p, ab).start()

    def stage4(p):
        for ab in range(2):
            s3_copy(p, ab).wait_recv()
            keep = my if ab == 0 else mx
            vals = silu_parts(*(r3[p, ab, t] + r2[p, ab, t, keep] for t in range(3)))
            for t in range(3):
                gat[p, ab, c, my, mx, t] = vals[t]
            net.first(p, ab, False).start()

    def stage5(p):
        for ab in range(2):
            net.first(p, ab, True).wait_recv()
            net.second(p, ab, False).start()

        @pl.when(p == N1 - 1)
        def _():
            for ab in range(2):
                s2_copy(N1, ab).start()

    def stage6(p):
        for ab in range(2):
            net.second(p, ab, True).wait_recv()
        net.third(p, False).start()

    def stage7(p):
        net.third(p, True).wait_recv()
        y_part(acc, gat, lambda q, lo, w: wd[q, lo:lo + w, :], p, 0, FC)
        dx_part(acc, gat, *(lambda q, lo, w, r=r: r[q, :, lo:lo + w] for r in (wg, wu)), p, 0, FC)

    for cp in w_copies(0):
        cp.wait()
    for n in range(NS):
        for ab in range(2):
            product(0, ab, n)
            d_copy(0, ab, n).start()
    for n in range(NS):
        for ab in range(2):
            d_copy(0, ab, n).wait_recv()
            rd[0, ab, :, :, :, :, sub(n)] = rd[0, ab, :, :, :, :, sub(n)] + part[0, c, ab, :, :, :, :, sub(n)]
            s2_copy(0, ab, n).start()

    @pl.loop(0, N1 + 5)
    def _(i):
        pl.when((i >= 1) & (i < NP))(lambda: stage2(i))
        pl.when((i >= 1) & (i < N1 + 1))(lambda: stage3(i - 1))
        pl.when((i >= 2) & (i < N1 + 2))(lambda: stage4(i - 2))
        pl.when((i >= 3) & (i < N1 + 3))(lambda: stage5(i - 3))
        pl.when((i >= 4) & (i < N1 + 4))(lambda: stage6(i - 4))
        pl.when(i < NP - 1)(lambda: products(i + 1))
        pl.when(i >= 5)(lambda: stage7(i - 5))

    @pl.loop(0, N1)
    def _(p):
        for ab in range(2):
            s3_copy(p, ab).wait_send()
            net.first(p, ab, False).wait_send()
            net.second(p, ab, False).wait_send()
        net.third(p, False).wait_send()

    @pl.loop(1, N1)
    def _(p):
        for ab in range(2):
            s2_copy(p, ab).wait_send()
    for n in range(NS):
        for ab in range(2):
            s2_copy(0, ab, n).wait_send()
    for p in (NP - 2, NP - 1):
        for ab in range(2):
            d_copy(p, ab).wait_send()

    @pl.loop(1, 16)
    def _(k):
        x_copy(k, at.mine).wait_send()
    for ab in range(2):
        s2_copy(N1, ab).wait_send()
        s2_copy(N1, ab).wait_recv()


def second_kernel(wg_hbm, wu_hbm, wd_hbm, xs_ref, acc_in, rows, rx, ry, kx, ky, r2n,
                  y_ref, gx_ref, lwg, lwu, lwd,
                  gat, wg, wu, wd, r2b, r3, acc, fin,
                  w_sem, s3_send, s3_recv, s4_send, s4_recv, s5_send, s5_recv, s5l_send, s5l_recv,
                  s6_send, s6_recv, s6l_send, s6l_recv, o_send, o_recv):
    at = Place()
    c, mx, my = at.c, at.x, at.y
    net = Gather(at, gat, (s4_send, s4_recv), (s5_send, s5_recv), (s6_send, s6_recv),
                 (s5l_send, s5l_recv), (s6l_send, s6l_recv))
    barrier = at.greet()
    cols = pl.ds(N1 * 2 * FC, NB * 2 * FC)
    w_copies = (pltpu.make_async_copy(wg_hbm.at[:, cols], wg, w_sem.at[0]),
                pltpu.make_async_copy(wu_hbm.at[:, cols], wu, w_sem.at[1]),
                pltpu.make_async_copy(wd_hbm.at[cols, :], wd, w_sem.at[2]))
    for cp in w_copies:
        cp.start()

    def s3_copy(q, ab):
        src = r2b.at[q, 0, :, 1 - my] if ab == 0 else r2b.at[q, 1, :, 1 - mx]
        return remote(src, r3.at[q, ab], s3_send.at[ab, q], s3_recv.at[ab, q], at.y_nb if ab == 0 else at.x_nb)

    def halves(q):
        for ab in range(2):
            for t in range(3):
                got = r2n[ab, t] if q == 0 else (rx, ry)[ab][q - 1, t]
                r2b[q, ab, t] = got + (kx, ky)[ab][q, t]

    def send_quarters(q):
        for ab in range(2):
            s3_copy(q, ab).start()

    def activate(q):
        for ab in range(2):
            s3_copy(q, ab).wait_recv()
            keep = my if ab == 0 else mx
            vals = silu_parts(*(r3[q, ab, t] + r2b[q, ab, t, keep] for t in range(3)))
            for t in range(3):
                gat[q, ab, c, my, mx, t] = vals[t]
            net.first(q, ab, False).start()

    def spread(q):
        for ab in range(2):
            net.first(q, ab, True).wait_recv()
            if q < NB - 1:
                net.second(q, ab, False).start()
            else:
                for n in range(NS):
                    net.second(q, ab, False, n).start()

    def cross(q):
        for ab in range(2):
            net.second(q, ab, True).wait_recv()
        net.third(q, False).start()

    def down(q, lo, w):
        return wd[q * 2 * FC + lo:q * 2 * FC + lo + w, :]

    def gate(q, lo, w):
        return wg[:, q * 2 * FC + lo:q * 2 * FC + lo + w]

    def up(q, lo, w):
        return wu[:, q * 2 * FC + lo:q * 2 * FC + lo + w]

    halves(0)
    pl.semaphore_wait(barrier, 15)
    send_quarters(0)
    for q in range(1, NB):
        halves(q)
        if q < NB - 1:
            send_quarters(q)
    acc[...] = acc_in[...]
    for q in range(NB):
        activate(q)
        if q == 0:
            send_quarters(NB - 1)
        else:
            spread(q - 1)
    spread(NB - 1)
    for cp in w_copies:
        cp.wait()
    cross(0)
    for q in range(1, NB - 1):
        net.third(q - 1, True).wait_recv()
        y_part(acc, gat, down, q - 1, 0, FC)
        cross(q)
        dx_part(acc, gat, gate, up, q - 1, 0, FC)
    q = NB - 1
    for n in range(NS):
        for ab in range(2):
            net.second(q, ab, True, n).wait_recv()
        net.third(q, False, n).start()
    net.third(q - 1, True).wait_recv()
    y_part(acc, gat, down, q - 1, 0, FC)
    dx_part(acc, gat, gate, up, q - 1, 0, FC)

    def o_copy(j, k, slot):
        ot, od = at.other(k)
        return remote(acc.at[j, blk(ot, od)], fin.at[j, slot], o_send.at[j, k], o_recv.at[j, slot], (ot, od))

    def send_out(j):
        @pl.loop(1, 16)
        def _(k):
            o_copy(j, k, at.me).start()
        fin[j, at.me] = acc[j, at.mine]

    for n in range(NS):
        net.third(q, True, n).wait_recv()
        y_part(acc, gat, down, q, n * SUB, SUB)
        if n == NS - 1:
            send_out(0)
        dx_part(acc, gat, gate, up, q, n * SUB, SUB)
    send_out(1)

    @pl.loop(0, 2 * NB)
    def _(k):
        lo = pl.ds(pl.multiple_of(k * FC, FC), FC)
        h, da, db = (gat[k // 2, lax.rem(k, 2), :, :, :, t].reshape(128, FC) for t in range(3))
        lwg[:, lo] = _dot(xs_ref[0], da, 0, 0)
        lwu[:, lo] = _dot(xs_ref[0], db, 0, 0)
        lwd[lo, :] = _dot(h, xs_ref[1], 0, 0)

    for q in range(NB):
        for ab in range(2):
            s3_copy(q, ab).wait_send()
            net.first(q, ab, False).wait_send()
            if q < NB - 1:
                net.second(q, ab, False).wait_send()
            else:
                for n in range(NS):
                    net.second(q, ab, False, n).wait_send()
        if q < NB - 1:
            net.third(q, False).wait_send()
        else:
            for n in range(NS):
                net.third(q, False, n).wait_send()

    for j, out in enumerate((y_ref, gx_ref)):
        @pl.loop(1, 16)
        def _(k):
            ot, od = at.other(k)
            o_copy(j, k, ot * 8 + od).wait_recv()
        for dd in range(8):
            cols = slice(dd * DL, (dd + 1) * DL)
            out[:, cols] = (rows[j, :, cols].astype(F32) + (fin[j, dd] + fin[j, 8 + dd])).astype(BF)

    @pl.loop(1, 16)
    def _(k):
        for j in range(2):
            o_copy(j, k, at.me).wait_send()


def early_grads(xs_ref, g_ref, dwg_ref, dwu_ref, dwd_ref):
    q, ab = pl.program_id(0) // 2, lax.rem(pl.program_id(0), 2)
    h, da, db = (g_ref[q, ab, :, :, :, t].reshape(128, FC) for t in range(3))
    dwg_ref[...] = _dot(xs_ref[0], da, 0, 0)
    dwu_ref[...] = _dot(xs_ref[0], db, 0, 0)
    dwd_ref[...] = _dot(h, xs_ref[1], 0, 0)


def late_grads(y_ref, gx_ref, lwg, lwu, lwd, a_ref, b_ref, c_ref, yo_ref, gxo_ref, dwg_ref, dwu_ref, dwd_ref, sem):
    copies = []
    for k in range(NB):
        src = pl.ds(k * 2 * FC, 2 * FC)
        dst = pl.ds((N1 + k) * 2 * FC, 2 * FC)
        copies += [pltpu.make_async_copy(lwg.at[:, src], dwg_ref.at[:, dst], sem.at[0, k]),
                   pltpu.make_async_copy(lwu.at[:, src], dwu_ref.at[:, dst], sem.at[1, k]),
                   pltpu.make_async_copy(lwd.at[src, :], dwd_ref.at[dst, :], sem.at[2, k])]
    for cp in copies:
        cp.start()
    yo_ref[...] = y_ref[...]
    gxo_ref[...] = gx_ref[...]
    for cp in copies:
        cp.wait()


def local_step(x_loc, wg_loc, wu_loc, wd_loc, gy_loc):
    vm = pl.BlockSpec(memory_space=pltpu.VMEM)
    hb = pl.BlockSpec(memory_space=pl.ANY)
    hbm = pl.BlockSpec(memory_space=pltpu.HBM)
    dma = pltpu.SemaphoreType.DMA
    row = jax.ShapeDtypeStruct((8, D), BF)
    kib = 1024
    half = (3, 2, 16, FC)
    xs, gat1, acc, rows, sx, sy, kx, ky, r2n = pl.pallas_call(
        first_kernel,
        out_shape=(pltpu.VMEM((2, 128, DL), BF), pltpu.VMEM((N1, 2, 2, 2, 2, 3, 16, FC), BF),
                   pltpu.VMEM((2, 16, 8, DL), F32), pltpu.VMEM((2, 8, D), BF),
                   pltpu.VMEM((NB - 1,) + half, F32), pltpu.VMEM((NB - 1,) + half, F32),
                   pltpu.VMEM((NB,) + half, F32), pltpu.VMEM((NB,) + half, F32), pltpu.VMEM((2,) + half, F32)),
        in_specs=[hbm] * 5,
        out_specs=(vm,) * 9,
        scratch_shapes=[
            pltpu.VMEM((NP, DL, 2 * FC), BF),
            pltpu.VMEM((NP, DL, 2 * FC), BF),
            pltpu.VMEM((NP, 2 * FC, DL), BF),
            pltpu.VMEM((NP, 2, 3, 2, 2, 16, FC), F32),
            pltpu.VMEM((N1, 2) + half, F32),
            pltpu.VMEM((8, 2, 8, DL), BF),
            pltpu.VMEM((16, 2, 8, DL), BF),
            pltpu.VMEM((2, 2, 2, 3, 2, 2, 16, FC), F32),
            pltpu.VMEM((N1, 2, 3, 16, FC), F32),
            dma((2,)), dma((3, NP)), dma((16,)), dma((16,)),
            dma((2, NP)), dma((2, NP)), dma((2, NS)), dma((2, NS)),
            dma((2, NP)), dma((2, NP)), dma((2, NS)), dma((2, NS)),
            dma((2, N1)), dma((2, N1)), dma((2, N1)), dma((2, N1)),
            dma((2, N1)), dma((2, N1)), dma((N1,)), dma((N1,)),
        ],
        compiler_params=pltpu.CompilerParams(
            collective_id=0, has_side_effects=True, vmem_limit_bytes=49000 * kib),
        name="mlp_first",
    )(x_loc, gy_loc, wg_loc, wu_loc, wd_loc)

    rx = lax.ppermute(sx, "dp", [(i, i + 2 if i % 4 < 2 else i - 2) for i in range(8)])
    ry = lax.ppermute(sy, "dp", [(i, (i + 4) % 8) for i in range(8)])

    full = (jax.ShapeDtypeStruct((DL, FF_LOC), F32), jax.ShapeDtypeStruct((DL, FF_LOC), F32),
            jax.ShapeDtypeStruct((FF_LOC, DL), F32))

    dwg, dwu, dwd = pl.pallas_call(
        early_grads,
        grid=(2 * N1,),
        out_shape=full,
        in_specs=[vm, vm],
        out_specs=(pl.BlockSpec((DL, FC), lambda k: (0, k)), pl.BlockSpec((DL, FC), lambda k: (0, k)),
                   pl.BlockSpec((FC, DL), lambda k: (k, 0))),
        cost_estimate=pl.CostEstimate(flops=12 * N1 * 128 * DL * FC, bytes_accessed=24 * N1 * DL * FC,
                                      transcendentals=0),
        compiler_params=pltpu.CompilerParams(dimension_semantics=("arbitrary",), vmem_limit_bytes=9000 * kib),
        name="mlp_early_grads",
    )(xs, gat1)

    y_rows, gx_rows, lwg, lwu, lwd = pl.pallas_call(
        second_kernel,
        out_shape=(pltpu.VMEM((8, D), BF), pltpu.VMEM((8, D), BF), pltpu.VMEM((DL, NB * 2 * FC), F32),
                   pltpu.VMEM((DL, NB * 2 * FC), F32), pltpu.VMEM((NB * 2 * FC, DL), F32)),
        in_specs=[hbm] * 3 + [vm] * 8,
        out_specs=(vm,) * 5,
        scratch_shapes=[
            pltpu.VMEM((NB, 2, 2, 2, 2, 3, 16, FC), BF),
            pltpu.VMEM((DL, NB * 2 * FC), BF),
            pltpu.VMEM((DL, NB * 2 * FC), BF),
            pltpu.VMEM((NB * 2 * FC, DL), BF),
            pltpu.VMEM((NB, 2) + half, F32),
            pltpu.VMEM((NB, 2, 3, 16, FC), F32),
            pltpu.VMEM((2, 16, 8, DL), F32),
            pltpu.VMEM((2, 16, 8, DL), F32),
            dma((3,)), dma((2, NB)), dma((2, NB)), dma((2, NB)), dma((2, NB)),
            dma((2, NB)), dma((2, NB)), dma((2, NS)), dma((2, NS)),
            dma((NB,)), dma((NB,)), dma((NS,)), dma((NS,)),
            dma((2, 16)), dma((2, 16)),
        ],
        compiler_params=pltpu.CompilerParams(
            collective_id=1, has_side_effects=True, vmem_limit_bytes=30000 * kib),
        name="mlp_second",
    )(wg_loc, wu_loc, wd_loc, xs, acc, rows, rx, ry, kx, ky, r2n)

    return pl.pallas_call(
        late_grads,
        out_shape=(row, row) + full,
        in_specs=[vm] * 5 + [hbm] * 3,
        out_specs=(vm, vm, hbm, hbm, hbm),
        input_output_aliases={5: 2, 6: 3, 7: 4},
        scratch_shapes=[dma((3, NB))],
        compiler_params=pltpu.CompilerParams(vmem_limit_bytes=30000 * kib),
        name="mlp_late_grads",
    )(y_rows, gx_rows, lwg, lwu, lwd, dwg, dwu, dwd)


def solution(mesh):
    row_spec = P(("dp", "tp"), None)
    up_spec = P("dp", "tp")
    down_spec = P("tp", "dp")
    return jax.shard_map(local_step, mesh=mesh,
                         in_specs=(row_spec, up_spec, up_spec, down_spec, row_spec),
                         out_specs=(row_spec, row_spec, up_spec, up_spec, down_spec),
                         check_vma=False)
```

```python
import functools

import jax
import jax.numpy as jnp
from jax import lax
from jax.experimental import pallas as pl
from jax.experimental.pallas import tpu as pltpu
from jax.sharding import PartitionSpec as P

MESH = pl.DeviceIdType.MESH
BF = jnp.bfloat16
F32 = jnp.float32

D = 3072
FF_LOC = 12288
DL = 384
NP = 8
N1 = 5
NB = NP - N1
FC = FF_LOC // (2 * NP)
NS = 3
SUB = FC // NS


def _dot(a, b, ca, cb):
    return lax.dot_general(a, b, (((ca,), (cb,)), ((), ())), preferred_element_type=F32)


def remote(src, dst, send, recv, dev):
    return pltpu.make_async_remote_copy(src_ref=src, dst_ref=dst, send_sem=send, recv_sem=recv,
                                        device_id=dev, device_id_type=MESH)


def sub(n):
    return pl.ds(n * SUB, SUB)


def blk(tt, dd):
    return (lax.rem(dd, 2) * 4 + (dd // 4) * 2 + lax.rem(dd // 2, 2)) * 2 + tt


class Place:
    def __init__(self):
        tp, dp = lax.axis_index("tp"), lax.axis_index("dp")
        c, x, y = lax.rem(dp, 2), lax.rem(dp // 2, 2), dp // 4
        self.tp, self.dp, self.c, self.x, self.y = tp, dp, c, x, y
        self.me = tp * 8 + dp
        self.core_nb = (tp, y * 4 + x * 2 + (1 - c))
        self.x_nb = (tp, y * 4 + (1 - x) * 2 + c)
        self.y_nb = (tp, (1 - y) * 4 + x * 2 + c)
        self.mine = blk(tp, dp)

    def other(self, k):
        o = lax.rem(self.me + k, 16)
        return o // 8, lax.rem(o, 8)

    def greet(self):
        barrier = pltpu.get_barrier_semaphore()

        @pl.loop(1, 16)
        def _(k):
            pl.semaphore_signal(barrier, inc=1, device_id=self.other(k), device_id_type=MESH)
        return barrier


def silu_parts(a, b, g):
    s = jax.nn.sigmoid(a)
    silu = a * s
    return ((silu * b).astype(BF), (g * b * (s * (1.0 + a * (1.0 - s)))).astype(BF), (g * silu).astype(BF))


def accumulate(acc, j, v):
    acc[j] = acc[j] + v.reshape(16, 8, DL)


def y_part(acc, gat, wd, q, lo, w):
    v = None
    for ab in range(2):
        h = gat[q, ab, :, :, :, 0, :, lo:lo + w].reshape(128, w)
        d = _dot(h, wd(q, ab * FC + lo, w), 1, 0)
        v = d if v is None else v + d
    accumulate(acc, 0, v)


def dx_part(acc, gat, wg, wu, q, lo, w, ts=(1, 2)):
    v = None
    for ab in range(2):
        for t, wt in ((t, (wg, wu)[t - 1]) for t in ts):
            z = gat[q, ab, :, :, :, t, :, lo:lo + w].reshape(128, w)
            d = _dot(z, wt(q, ab * FC + lo, w), 1, 1)
            v = d if v is None else v + d
    accumulate(acc, 1, v)


class Gather:
    def __init__(self, at, gat, s4, s5, s6, s5l=None, s6l=None):
        self.at, self.gat, self.s4, self.s5, self.s6, self.s5l, self.s6l = at, gat, s4, s5, s6, s5l, s6l

    def first(self, q, ab, arriving):
        at = self.at
        y0 = (1 - at.y) if arriving else at.y
        x1 = (1 - at.x) if arriving else at.x
        b = self.gat.at[q, 0, at.c, y0, at.x] if ab == 0 else self.gat.at[q, 1, at.c, at.y, x1]
        return remote(b, b, self.s4[0].at[ab, q], self.s4[1].at[ab, q], at.y_nb if ab == 0 else at.x_nb)

    def second(self, q, ab, arriving, n=None):
        at = self.at
        x0 = (1 - at.x) if arriving else at.x
        y1 = (1 - at.y) if arriving else at.y
        b = self.gat.at[q, 0, at.c, :, x0] if ab == 0 else self.gat.at[q, 1, at.c, y1]
        dev = at.x_nb if ab == 0 else at.y_nb
        if n is None:
            return remote(b, b, self.s5[0].at[ab, q], self.s5[1].at[ab, q], dev)
        b = b.at[:, n]
        return remote(b, b, self.s5l[0].at[ab, n], self.s5l[1].at[ab, n], dev)

    def third(self, q, arriving, n=None):
        at = self.at
        b = self.gat.at[q, :, (1 - at.c) if arriving else at.c]
        if n is None:
            return remote(b, b, self.s6[0].at[q], self.s6[1].at[q], at.core_nb)
        b = b.at[:, :, :, n]
        return remote(b, b, self.s6l[0].at[n], self.s6l[1].at[n], at.core_nb)


def first_kernel(x_hbm, gy_hbm, wg_hbm, wu_hbm, wd_hbm,
                 xs_ref, gat, acc, rows, sx, sy, kx, ky, r2n,
                 wg, wu, wd, rd, r2, st, xin, part, r3,
                 in_sem, w_sem, x_send, x_recv, d_send, d_recv, d0_send, d0_recv, s2_send, s2_recv, s20_send, s20_recv,
                 s3_send, s3_recv, s4_send, s4_recv, s5_send, s5_recv, s6_send, s6_recv):
    at = Place()
    c, mx, my = at.c, at.x, at.y
    net = Gather(at, gat, (s4_send, s4_recv), (s5_send, s5_recv), (s6_send, s6_recv))

    def w_copies(p):
        cols = pl.ds(pl.multiple_of(p * 2 * FC, 2 * FC), 2 * FC)
        return (pltpu.make_async_copy(wg_hbm.at[:, cols], wg.at[p], w_sem.at[0, p]),
                pltpu.make_async_copy(wu_hbm.at[:, cols], wu.at[p], w_sem.at[1, p]),
                pltpu.make_async_copy(wd_hbm.at[cols, :], wd.at[p], w_sem.at[2, p]))

    in_copies = [pltpu.make_async_copy(r, rows.at[j], in_sem.at[j]) for j, r in enumerate((x_hbm, gy_hbm))]
    for cp in in_copies:
        cp.start()
    barrier = at.greet()

    @pl.loop(0, NP)
    def _(p):
        for cp in w_copies(p):
            cp.start()

    acc[...] = jnp.zeros_like(acc)
    for j in range(2):
        in_copies[j].wait()
        for dd in range(8):
            st[dd, j] = rows[j, :, dd * DL:(dd + 1) * DL]
    pl.semaphore_wait(barrier, 15)

    def x_copy(k, b):
        ot, od = at.other(k)
        return remote(st.at[od], xin.at[b], x_send.at[k], x_recv.at[b], (ot, od))

    @pl.loop(1, 16)
    def _(k):
        x_copy(k, at.mine).start()

    xin[at.mine] = st[at.dp]

    @pl.loop(1, 16)
    def _(k):
        x_copy(k, blk(*at.other(k))).wait_recv()

    for j in range(2):
        xs_ref[j] = xin[:, j].astype(F32).reshape(128, DL).astype(BF)

    def d_copy(p, ab, n=None):
        s = lax.rem(p, 2)
        if n is None:
            return remote(part.at[s, 1 - c, ab], rd.at[p, ab], d_send.at[ab, p], d_recv.at[ab, p], at.core_nb)
        return remote(part.at[s, 1 - c, ab, :, :, :, :, sub(n)], rd.at[p, ab, :, :, :, :, sub(n)],
                      d0_send.at[ab, n], d0_recv.at[ab, n], at.core_nb)

    def s2_copy(p, ab, n=None):
        src = rd.at[p, 0, :, :, 1 - mx] if ab == 0 else rd.at[p, 1, :, 1 - my]
        dst = r2n.at[ab] if p is N1 else r2.at[p, ab]
        dev = at.x_nb if ab == 0 else at.y_nb
        if n is None:
            return remote(src, dst, s2_send.at[ab, p], s2_recv.at[ab, p], dev)
        return remote(src.at[:, :, :, sub(n)], dst.at[:, :, :, sub(n)], s20_send.at[ab, n], s20_recv.at[ab, n], dev)

    def s3_copy(p, ab):
        src = r2.at[p, 0, :, 1 - my] if ab == 0 else r2.at[p, 1, :, 1 - mx]
        return remote(src, r3.at[p, ab], s3_send.at[ab, p], s3_recv.at[ab, p], at.y_nb if ab == 0 else at.x_nb)

    def product(p, ab, n):
        s = lax.rem(p, 2)
        cols = pl.ds(ab * FC + n * SUB, SUB)
        vals = (_dot(xs_ref[0], wg[p, :, cols], 1, 0),
                _dot(xs_ref[0], wu[p, :, cols], 1, 0),
                _dot(xs_ref[1], wd[p, cols, :], 1, 1))
        for t in range(3):
            v = vals[t].reshape(2, 2, 2, 16, SUB)
            for cc in range(2):
                part[s, cc, ab, t, :, :, :, sub(n)] = v[cc]

    def products(p):
        for cp in w_copies(p):
            cp.wait()
        for ab in range(2):
            @pl.when(p >= 3)
            def _():
                d_copy(p - 2, ab).wait_send()

            @pl.when(p == 2)
            def _():
                for n in range(NS):
                    d_copy(0, ab, n).wait_send()
            for n in range(NS):
                product(p, ab, n)
            d_copy(p, ab).start()

    def stage2(p):
        s = lax.rem(p, 2)
        for ab in range(2):
            d_copy(p, ab).wait_recv()
            for t in range(3):
                rd[p, ab, t] = rd[p, ab, t] + part[s, c, ab, t]

            @pl.when(p < N1)
            def _():
                s2_copy(p, ab).start()

        @pl.when(p >= N1)
        def _():
            for t in range(3):
                kx[p - N1, t] = rd[p, 0, t, :, mx]
                ky[p - N1, t] = rd[p, 1, t, my]

        @pl.when(p > N1)
        def _():
            for t in range(3):
                sx[p - N1 - 1, t] = rd[p, 0, t, :, 1 - mx]
                sy[p - N1 - 1, t] = rd[p, 1, t, 1 - my]

    def stage3(p):
        for ab in range(2):
            @pl.when(p == 0)
            def _():
                for n in range(NS):
                    s2_copy(0, ab, n).wait_recv()

            @pl.when(p > 0)
            def _():
                s2_copy(p, ab).wait_recv()
            for t in range(3):
                r2[p, ab, t] = r2[p, ab, t] + (rd[p, 0, t, :, mx] if ab == 0 else rd[p, 1, t, my])
            s3_copy(p, ab).start()

    def stage4(p):
        for ab in range(2):
            s3_copy(p, ab).wait_recv()
            keep = my if ab == 0 else mx
            vals = silu_parts(*(r3[p, ab, t] + r2[p, ab, t, keep] for t in range(3)))
            for t in range(3):
                gat[p, ab, c, my, mx, t] = vals[t]
            net.first(p, ab, False).start()

    def stage5(p):
        for ab in range(2):
            net.first(p, ab, True).wait_recv()
            net.second(p, ab, False).start()

        @pl.when(p == N1 - 1)
        def _():
            for ab in range(2):
                s2_copy(N1, ab).start()

    def stage6(p):
        for ab in range(2):
            net.second(p, ab, True).wait_recv()
        net.third(p, False).start()

    def stage7(p):
        net.third(p, True).wait_recv()
        y_part(acc, gat, lambda q, lo, w: wd[q, lo:lo + w, :], p, 0, FC)
        dx_part(acc, gat, *(lambda q, lo, w, r=r: r[q, :, lo:lo + w] for r in (wg, wu)), p, 0, FC)

    for cp in w_copies(0):
        cp.wait()
    for n in range(NS):
        for ab in range(2):
            product(0, ab, n)
            d_copy(0, ab, n).start()
    for n in range(NS):
        for ab in range(2):
            d_copy(0, ab, n).wait_recv()
            rd[0, ab, :, :, :, :, sub(n)] = rd[0, ab, :, :, :, :, sub(n)] + part[0, c, ab, :, :, :, :, sub(n)]
            s2_copy(0, ab, n).start()

    @pl.loop(0, N1 + 5)
    def _(i):
        pl.when((i >= 1) & (i < NP))(lambda: stage2(i))
        pl.when((i >= 1) & (i < N1 + 1))(lambda: stage3(i - 1))
        pl.when((i >= 2) & (i < N1 + 2))(lambda: stage4(i - 2))
        pl.when((i >= 3) & (i < N1 + 3))(lambda: stage5(i - 3))
        pl.when((i >= 4) & (i < N1 + 4))(lambda: stage6(i - 4))
        pl.when(i < NP - 1)(lambda: products(i + 1))
        pl.when(i >= 5)(lambda: stage7(i - 5))

    @pl.loop(0, N1)
    def _(p):
        for ab in range(2):
            s3_copy(p, ab).wait_send()
            net.first(p, ab, False).wait_send()
            net.second(p, ab, False).wait_send()
        net.third(p, False).wait_send()

    @pl.loop(1, N1)
    def _(p):
        for ab in range(2):
            s2_copy(p, ab).wait_send()
    for n in range(NS):
        for ab in range(2):
            s2_copy(0, ab, n).wait_send()
    for p in (NP - 2, NP - 1):
        for ab in range(2):
            d_copy(p, ab).wait_send()

    @pl.loop(1, 16)
    def _(k):
        x_copy(k, at.mine).wait_send()
    for ab in range(2):
        s2_copy(N1, ab).wait_send()
        s2_copy(N1, ab).wait_recv()


def second_kernel(wg_hbm, wu_hbm, wd_hbm, xs_ref, acc_in, rows, rx, ry, kx, ky, r2n,
                  y_ref, gx_ref, lwg, lwu, lwd,
                  gat, wg, wu, wd, r2b, r3, acc, fin,
                  w_sem, s3_send, s3_recv, s4_send, s4_recv, s5_send, s5_recv, s5l_send, s5l_recv,
                  s6_send, s6_recv, s6l_send, s6l_recv, o_send, o_recv):
    at = Place()
    c, mx, my = at.c, at.x, at.y
    net = Gather(at, gat, (s4_send, s4_recv), (s5_send, s5_recv), (s6_send, s6_recv),
                 (s5l_send, s5l_recv), (s6l_send, s6l_recv))
    barrier = pltpu.get_barrier_semaphore()
    for nb in (at.x_nb, at.y_nb, at.core_nb, (1 - at.tp, at.dp)):
        pl.semaphore_signal(barrier, inc=1, device_id=nb, device_id_type=MESH)
    cols = pl.ds(N1 * 2 * FC, NB * 2 * FC)
    w_copies = (pltpu.make_async_copy(wg_hbm.at[:, cols], wg, w_sem.at[0]),
                pltpu.make_async_copy(wu_hbm.at[:, cols], wu, w_sem.at[1]),
                pltpu.make_async_copy(wd_hbm.at[cols, :], wd, w_sem.at[2]))
    for cp in w_copies:
        cp.start()

    def s3_copy(q, ab):
        src = r2b.at[q, 0, :, 1 - my] if ab == 0 else r2b.at[q, 1, :, 1 - mx]
        return remote(src, r3.at[q, ab], s3_send.at[ab, q], s3_recv.at[ab, q], at.y_nb if ab == 0 else at.x_nb)

    def halves(q):
        for ab in range(2):
            for t in range(3):
                got = r2n[ab, t] if q == 0 else (rx, ry)[ab][q - 1, t]
                r2b[q, ab, t] = got + (kx, ky)[ab][q, t]

    def send_quarters(q):
        for ab in range(2):
            s3_copy(q, ab).start()

    def activate(q):
        for ab in range(2):
            s3_copy(q, ab).wait_recv()
            keep = my if ab == 0 else mx
            vals = silu_parts(*(r3[q, ab, t] + r2b[q, ab, t, keep] for t in range(3)))
            for t in range(3):
                gat[q, ab, c, my, mx, t] = vals[t]
            net.first(q, ab, False).start()

    def spread(q):
        for ab in range(2):
            net.first(q, ab, True).wait_recv()
            if q < NB - 1:
                net.second(q, ab, False).start()
            else:
                for n in range(3):
                    net.second(q, ab, False, n).start()

    def cross(q):
        for ab in range(2):
            net.second(q, ab, True).wait_recv()
        net.third(q, False).start()

    def down(q, lo, w):
        return wd[q * 2 * FC + lo:q * 2 * FC + lo + w, :]

    def gate(q, lo, w):
        return wg[:, q * 2 * FC + lo:q * 2 * FC + lo + w]

    def up(q, lo, w):
        return wu[:, q * 2 * FC + lo:q * 2 * FC + lo + w]

    halves(0)
    pl.semaphore_wait(barrier, 4)
    send_quarters(0)
    for q in range(1, NB):
        halves(q)
        if q < NB - 1:
            send_quarters(q)
    acc[...] = acc_in[...]
    for q in range(NB):
        activate(q)
        if q == 0:
            send_quarters(NB - 1)
        else:
            spread(q - 1)
    spread(NB - 1)
    for cp in w_copies:
        cp.wait()
    cross(0)
    for q in range(1, NB - 1):
        net.third(q - 1, True).wait_recv()
        y_part(acc, gat, down, q - 1, 0, FC)
        cross(q)
        dx_part(acc, gat, gate, up, q - 1, 0, FC)
    q = NB - 1
    net.third(q - 1, True).wait_recv()
    y_part(acc, gat, down, q - 1, 0, FC)
    dx_part(acc, gat, gate, up, q - 1, 0, FC)

    def o_copy(j, k, slot):
        ot, od = at.other(k)
        return remote(acc.at[j, blk(ot, od)], fin.at[j, slot], o_send.at[j, k], o_recv.at[j, slot], (ot, od))

    def send_out(j):
        @pl.loop(1, 16)
        def _(k):
            o_copy(j, k, at.me).start()
        fin[j, at.me] = acc[j, at.mine]

    def finish(n):
        net.third(q, True, n).wait_recv()
        if n == 0:
            y_part(acc, gat, down, q, 0, FC)
            send_out(0)
        else:
            dx_part(acc, gat, gate, up, q, 0, FC, (n,))
        if n == 2:
            send_out(1)

    for n in range(3):
        for ab in range(2):
            net.second(q, ab, True, n).wait_recv()
        net.third(q, False, n).start()
        if n > 0:
            finish(n - 1)
    finish(2)

    @pl.loop(0, 2 * NB)
    def _(k):
        lo = pl.ds(pl.multiple_of(k * FC, FC), FC)
        h, da, db = (gat[k // 2, lax.rem(k, 2), :, :, :, t].reshape(128, FC) for t in range(3))
        lwg[:, lo] = _dot(xs_ref[0], da, 0, 0)
        lwu[:, lo] = _dot(xs_ref[0], db, 0, 0)
        lwd[lo, :] = _dot(h, xs_ref[1], 0, 0)

    for q in range(NB):
        for ab in range(2):
            s3_copy(q, ab).wait_send()
            net.first(q, ab, False).wait_send()
            if q < NB - 1:
                net.second(q, ab, False).wait_send()
            else:
                for n in range(3):
                    net.second(q, ab, False, n).wait_send()
        if q < NB - 1:
            net.third(q, False).wait_send()
        else:
            for n in range(3):
                net.third(q, False, n).wait_send()

    for j, out in enumerate((y_ref, gx_ref)):
        @pl.loop(1, 16)
        def _(k):
            ot, od = at.other(k)
            o_copy(j, k, ot * 8 + od).wait_recv()
        for dd in range(8):
            cols = slice(dd * DL, (dd + 1) * DL)
            out[:, cols] = (rows[j, :, cols].astype(F32) + (fin[j, dd] + fin[j, 8 + dd])).astype(BF)

    @pl.loop(1, 16)
    def _(k):
        for j in range(2):
            o_copy(j, k, at.me).wait_send()


def early_grads(xs_ref, g_ref, dwg_ref, dwu_ref, dwd_ref):
    q, ab = pl.program_id(0) // 2, lax.rem(pl.program_id(0), 2)
    h, da, db = (g_ref[q, ab, :, :, :, t].reshape(128, FC) for t in range(3))
    dwg_ref[...] = _dot(xs_ref[0], da, 0, 0)
    dwu_ref[...] = _dot(xs_ref[0], db, 0, 0)
    dwd_ref[...] = _dot(h, xs_ref[1], 0, 0)


def late_grads(y_ref, gx_ref, lwg, lwu, lwd, a_ref, b_ref, c_ref, yo_ref, gxo_ref, dwg_ref, dwu_ref, dwd_ref, sem, row_sem):
    copies = [pltpu.make_async_copy(y_ref, yo_ref, row_sem.at[0]), pltpu.make_async_copy(gx_ref, gxo_ref, row_sem.at[1])]
    for k in range(NB):
        src = pl.ds(k * 2 * FC, 2 * FC)
        dst = pl.ds((N1 + k) * 2 * FC, 2 * FC)
        copies += [pltpu.make_async_copy(lwg.at[:, src], dwg_ref.at[:, dst], sem.at[0, k]),
                   pltpu.make_async_copy(lwu.at[:, src], dwu_ref.at[:, dst], sem.at[1, k]),
                   pltpu.make_async_copy(lwd.at[src, :], dwd_ref.at[dst, :], sem.at[2, k])]
    for cp in copies:
        cp.start()
    for cp in copies:
        cp.wait()


def local_step(x_loc, wg_loc, wu_loc, wd_loc, gy_loc):
    vm = pl.BlockSpec(memory_space=pltpu.VMEM)
    hb = pl.BlockSpec(memory_space=pl.ANY)
    hbm = pl.BlockSpec(memory_space=pltpu.HBM)
    dma = pltpu.SemaphoreType.DMA
    row = jax.ShapeDtypeStruct((8, D), BF)
    kib = 1024
    half = (3, 2, 16, FC)
    xs, gat1, acc, rows, sx, sy, kx, ky, r2n = pl.pallas_call(
        first_kernel,
        out_shape=(pltpu.VMEM((2, 128, DL), BF), pltpu.VMEM((N1, 2, 2, 2, 2, 3, 16, FC), BF),
                   pltpu.VMEM((2, 16, 8, DL), F32), pltpu.VMEM((2, 8, D), BF),
                   pltpu.VMEM((NB - 1,) + half, F32), pltpu.VMEM((NB - 1,) + half, F32),
                   pltpu.VMEM((NB,) + half, F32), pltpu.VMEM((NB,) + half, F32), pltpu.VMEM((2,) + half, F32)),
        in_specs=[hbm] * 5,
        out_specs=(vm,) * 9,
        scratch_shapes=[
            pltpu.VMEM((NP, DL, 2 * FC), BF),
            pltpu.VMEM((NP, DL, 2 * FC), BF),
            pltpu.VMEM((NP, 2 * FC, DL), BF),
            pltpu.VMEM((NP, 2, 3, 2, 2, 16, FC), F32),
            pltpu.VMEM((N1, 2) + half, F32),
            pltpu.VMEM((8, 2, 8, DL), BF),
            pltpu.VMEM((16, 2, 8, DL), BF),
            pltpu.VMEM((2, 2, 2, 3, 2, 2, 16, FC), F32),
            pltpu.VMEM((N1, 2, 3, 16, FC), F32),
            dma((2,)), dma((3, NP)), dma((16,)), dma((16,)),
            dma((2, NP)), dma((2, NP)), dma((2, NS)), dma((2, NS)),
            dma((2, NP)), dma((2, NP)), dma((2, NS)), dma((2, NS)),
            dma((2, N1)), dma((2, N1)), dma((2, N1)), dma((2, N1)),
            dma((2, N1)), dma((2, N1)), dma((N1,)), dma((N1,)),
        ],
        compiler_params=pltpu.CompilerParams(
            collective_id=0, has_side_effects=True, vmem_limit_bytes=49000 * kib),
        name="mlp_first",
    )(x_loc, gy_loc, wg_loc, wu_loc, wd_loc)

    rx = lax.ppermute(sx, "dp", [(i, i + 2 if i % 4 < 2 else i - 2) for i in range(8)])
    ry = lax.ppermute(sy, "dp", [(i, (i + 4) % 8) for i in range(8)])

    full = (jax.ShapeDtypeStruct((DL, FF_LOC), F32), jax.ShapeDtypeStruct((DL, FF_LOC), F32),
            jax.ShapeDtypeStruct((FF_LOC, DL), F32))

    dwg, dwu, dwd = pl.pallas_call(
        early_grads,
        grid=(2 * N1,),
        out_shape=full,
        in_specs=[vm, vm],
        out_specs=(pl.BlockSpec((DL, FC), lambda k: (0, k)), pl.BlockSpec((DL, FC), lambda k: (0, k)),
                   pl.BlockSpec((FC, DL), lambda k: (k, 0))),
        cost_estimate=pl.CostEstimate(flops=12 * N1 * 128 * DL * FC, bytes_accessed=24 * N1 * DL * FC,
                                      transcendentals=0),
        compiler_params=pltpu.CompilerParams(dimension_semantics=("arbitrary",), vmem_limit_bytes=9000 * kib),
        name="mlp_early_grads",
    )(xs, gat1)

    y_rows, gx_rows, lwg, lwu, lwd = pl.pallas_call(
        second_kernel,
        out_shape=(pltpu.VMEM((8, D), BF), pltpu.VMEM((8, D), BF), pltpu.VMEM((DL, NB * 2 * FC), F32),
                   pltpu.VMEM((DL, NB * 2 * FC), F32), pltpu.VMEM((NB * 2 * FC, DL), F32)),
        in_specs=[hbm] * 3 + [vm] * 8,
        out_specs=(vm,) * 5,
        scratch_shapes=[
            pltpu.VMEM((NB, 2, 2, 2, 2, 3, 16, FC), BF),
            pltpu.VMEM((DL, NB * 2 * FC), BF),
            pltpu.VMEM((DL, NB * 2 * FC), BF),
            pltpu.VMEM((NB * 2 * FC, DL), BF),
            pltpu.VMEM((NB, 2) + half, F32),
            pltpu.VMEM((NB, 2, 3, 16, FC), F32),
            pltpu.VMEM((2, 16, 8, DL), F32),
            pltpu.VMEM((2, 16, 8, DL), F32),
            dma((3,)), dma((2, NB)), dma((2, NB)), dma((2, NB)), dma((2, NB)),
            dma((2, NB)), dma((2, NB)), dma((2, 3)), dma((2, 3)),
            dma((NB,)), dma((NB,)), dma((3,)), dma((3,)),
            dma((2, 16)), dma((2, 16)),
        ],
        compiler_params=pltpu.CompilerParams(
            collective_id=1, has_side_effects=True, vmem_limit_bytes=30000 * kib),
        name="mlp_second",
    )(wg_loc, wu_loc, wd_loc, xs, acc, rows, rx, ry, kx, ky, r2n)

    return pl.pallas_call(
        late_grads,
        out_shape=(row, row) + full,
        in_specs=[vm] * 5 + [hbm] * 3,
        out_specs=(hbm,) * 5,
        input_output_aliases={5: 2, 6: 3, 7: 4},
        scratch_shapes=[dma((3, NB)), dma((2,))],
        compiler_params=pltpu.CompilerParams(vmem_limit_bytes=30000 * kib),
        name="mlp_late_grads",
    )(y_rows, gx_rows, lwg, lwu, lwd, dwg, dwu, dwd)


def solution(mesh):
    row_spec = P(("dp", "tp"), None)
    up_spec = P("dp", "tp")
    down_spec = P("tp", "dp")
    return jax.shard_map(local_step, mesh=mesh,
                         in_specs=(row_spec, up_spec, up_spec, down_spec, row_spec),
                         out_specs=(row_spec, row_spec, up_spec, up_spec, down_spec),
                         check_vma=False)
```

```python
import functools

import jax
import jax.numpy as jnp
from jax import lax
from jax.experimental import pallas as pl
from jax.experimental.pallas import tpu as pltpu
from jax.sharding import PartitionSpec as P

MESH = pl.DeviceIdType.MESH
BF = jnp.bfloat16
F32 = jnp.float32

BOTH = range(2)
TENSORS = range(3)
D = 3072
FF_LOC = 12288
DL = 384
NP = 8
N1 = 5
NB = NP - N1
FC = FF_LOC // (2 * NP)
NS = 3
SUB = FC // NS


def _dot(a, b, ca, cb):
    return lax.dot_general(a, b, (((ca,), (cb,)), ((), ())), preferred_element_type=F32)


def remote(src, dst, send, recv, dev):
    return pltpu.make_async_remote_copy(src_ref=src, dst_ref=dst, send_sem=send, recv_sem=recv,
                                        device_id=dev, device_id_type=MESH)


def sub(n):
    return pl.ds(n * SUB, SUB)


def blk(tt, dd):
    return (lax.rem(dd, 2) * 4 + (dd // 4) * 2 + lax.rem(dd // 2, 2)) * 2 + tt


class Place:
    def __init__(self):
        tp, dp = lax.axis_index("tp"), lax.axis_index("dp")
        c, x, y = lax.rem(dp, 2), lax.rem(dp // 2, 2), dp // 4
        self.tp, self.dp, self.c, self.x, self.y = tp, dp, c, x, y
        self.me = tp * 8 + dp
        self.core_nb = (tp, y * 4 + x * 2 + (1 - c))
        self.x_nb = (tp, y * 4 + (1 - x) * 2 + c)
        self.y_nb = (tp, (1 - y) * 4 + x * 2 + c)
        self.mine = blk(tp, dp)

    def other(self, k):
        o = lax.rem(self.me + k, 16)
        return o // 8, lax.rem(o, 8)

    def greet(self):
        barrier = pltpu.get_barrier_semaphore()

        @pl.loop(1, 16)
        def _(k):
            pl.semaphore_signal(barrier, inc=1, device_id=self.other(k), device_id_type=MESH)
        return barrier


def silu_parts(a, b, g):
    s = jax.nn.sigmoid(a)
    silu = a * s
    return ((silu * b).astype(BF), (g * b * (s * (1.0 + a * (1.0 - s)))).astype(BF), (g * silu).astype(BF))


def accumulate(acc, j, v):
    acc[j] = acc[j] + v.reshape(16, 8, DL)


def y_part(acc, gat, wd, q, lo, w):
    v = None
    for ab in BOTH:
        h = gat[q, ab, :, :, :, 0, :, lo:lo + w].reshape(128, w)
        d = _dot(h, wd(q, ab * FC + lo, w), 1, 0)
        v = d if v is None else v + d
    accumulate(acc, 0, v)


def dx_part(acc, gat, wg, wu, q, lo, w, ts=(1, 2)):
    v = None
    for ab in BOTH:
        for t, wt in ((t, (wg, wu)[t - 1]) for t in ts):
            z = gat[q, ab, :, :, :, t, :, lo:lo + w].reshape(128, w)
            d = _dot(z, wt(q, ab * FC + lo, w), 1, 1)
            v = d if v is None else v + d
    accumulate(acc, 1, v)


class Gather:
    def __init__(self, at, gat, s4, s5, s6, s5l=None, s6l=None):
        self.at, self.gat, self.s4, self.s5, self.s6, self.s5l, self.s6l = at, gat, s4, s5, s6, s5l, s6l

    def first(self, q, ab, arriving):
        at = self.at
        y0 = (1 - at.y) if arriving else at.y
        x1 = (1 - at.x) if arriving else at.x
        b = self.gat.at[q, 0, at.c, y0, at.x] if ab == 0 else self.gat.at[q, 1, at.c, at.y, x1]
        return remote(b, b, self.s4[0].at[ab, q], self.s4[1].at[ab, q], at.y_nb if ab == 0 else at.x_nb)

    def second(self, q, ab, arriving, n=None):
        at = self.at
        x0 = (1 - at.x) if arriving else at.x
        y1 = (1 - at.y) if arriving else at.y
        b = self.gat.at[q, 0, at.c, :, x0] if ab == 0 else self.gat.at[q, 1, at.c, y1]
        dev = at.x_nb if ab == 0 else at.y_nb
        if n is None:
            return remote(b, b, self.s5[0].at[ab, q], self.s5[1].at[ab, q], dev)
        b = b.at[:, n]
        return remote(b, b, self.s5l[0].at[ab, n], self.s5l[1].at[ab, n], dev)

    def third(self, q, arriving, n=None):
        at = self.at
        b = self.gat.at[q, :, (1 - at.c) if arriving else at.c]
        if n is None:
            return remote(b, b, self.s6[0].at[q], self.s6[1].at[q], at.core_nb)
        b = b.at[:, :, :, n]
        return remote(b, b, self.s6l[0].at[n], self.s6l[1].at[n], at.core_nb)


def first_kernel(x_hbm, gy_hbm, wg_hbm, wu_hbm, wd_hbm,
                 xs_ref, gat, acc, rows, sx, sy, kx, ky, r2n,
                 wg, wu, wd, rd, r2, st, xin, part, r3,
                 in_sem, w_sem, x_send, x_recv, d_send, d_recv, d0_send, d0_recv, s2_send, s2_recv, s20_send, s20_recv,
                 s3_send, s3_recv, s4_send, s4_recv, s5_send, s5_recv, s6_send, s6_recv):
    at = Place()
    c, mx, my = at.c, at.x, at.y
    net = Gather(at, gat, (s4_send, s4_recv), (s5_send, s5_recv), (s6_send, s6_recv))

    def w_copies(p):
        cols = pl.ds(pl.multiple_of(p * 2 * FC, 2 * FC), 2 * FC)
        return (pltpu.make_async_copy(wg_hbm.at[:, cols], wg.at[p], w_sem.at[0, p]),
                pltpu.make_async_copy(wu_hbm.at[:, cols], wu.at[p], w_sem.at[1, p]),
                pltpu.make_async_copy(wd_hbm.at[cols, :], wd.at[p], w_sem.at[2, p]))

    in_copies = [pltpu.make_async_copy(r, rows.at[j], in_sem.at[j]) for j, r in enumerate((x_hbm, gy_hbm))]
    for cp in in_copies:
        cp.start()
    barrier = at.greet()

    @pl.loop(0, NP)
    def _(p):
        for cp in w_copies(p):
            cp.start()

    acc[...] = jnp.zeros_like(acc)
    for j in BOTH:
        in_copies[j].wait()
        for dd in range(8):
            st[dd, j] = rows[j, :, dd * DL:(dd + 1) * DL]
    pl.semaphore_wait(barrier, 15)

    def x_copy(k, b):
        ot, od = at.other(k)
        return remote(st.at[od], xin.at[b], x_send.at[k], x_recv.at[b], (ot, od))

    @pl.loop(1, 16)
    def _(k):
        x_copy(k, at.mine).start()

    xin[at.mine] = st[at.dp]

    @pl.loop(1, 16)
    def _(k):
        x_copy(k, blk(*at.other(k))).wait_recv()

    for j in BOTH:
        xs_ref[j] = xin[:, j].astype(F32).reshape(128, DL).astype(BF)

    def d_copy(p, ab, n=None):
        s = lax.rem(p, 2)
        if n is None:
            return remote(part.at[s, 1 - c, ab], rd.at[p, ab], d_send.at[ab, p], d_recv.at[ab, p], at.core_nb)
        return remote(part.at[s, 1 - c, ab, :, :, :, :, sub(n)], rd.at[p, ab, :, :, :, :, sub(n)],
                      d0_send.at[ab, n], d0_recv.at[ab, n], at.core_nb)

    def s2_copy(p, ab, n=None):
        src = rd.at[p, 0, :, :, 1 - mx] if ab == 0 else rd.at[p, 1, :, 1 - my]
        dst = r2n.at[ab] if p is N1 else r2.at[p, ab]
        dev = at.x_nb if ab == 0 else at.y_nb
        if n is None:
            return remote(src, dst, s2_send.at[ab, p], s2_recv.at[ab, p], dev)
        return remote(src.at[:, :, :, sub(n)], dst.at[:, :, :, sub(n)], s20_send.at[ab, n], s20_recv.at[ab, n], dev)

    def s3_copy(p, ab):
        src = r2.at[p, 0, :, 1 - my] if ab == 0 else r2.at[p, 1, :, 1 - mx]
        return remote(src, r3.at[p, ab], s3_send.at[ab, p], s3_recv.at[ab, p], at.y_nb if ab == 0 else at.x_nb)

    def product(p, ab, n):
        s = lax.rem(p, 2)
        cols = pl.ds(ab * FC + n * SUB, SUB)
        vals = (_dot(xs_ref[0], wg[p, :, cols], 1, 0),
                _dot(xs_ref[0], wu[p, :, cols], 1, 0),
                _dot(xs_ref[1], wd[p, cols, :], 1, 1))
        for t in TENSORS:
            v = vals[t].reshape(2, 2, 2, 16, SUB)
            for cc in BOTH:
                part[s, cc, ab, t, :, :, :, sub(n)] = v[cc]

    def products(p):
        for cp in w_copies(p):
            cp.wait()
        for ab in BOTH:
            @pl.when(p >= 3)
            def _():
                d_copy(p - 2, ab).wait_send()

            @pl.when(p == 2)
            def _():
                for n in range(NS):
                    d_copy(0, ab, n).wait_send()
            for n in range(NS):
                product(p, ab, n)
            d_copy(p, ab).start()

    def stage2(p):
        s = lax.rem(p, 2)
        for ab in BOTH:
            d_copy(p, ab).wait_recv()
            for t in TENSORS:
                rd[p, ab, t] = rd[p, ab, t] + part[s, c, ab, t]

            @pl.when(p < N1)
            def _():
                s2_copy(p, ab).start()

        @pl.when(p >= N1)
        def _():
            for t in TENSORS:
                kx[p - N1, t] = rd[p, 0, t, :, mx]
                ky[p - N1, t] = rd[p, 1, t, my]

        @pl.when(p > N1)
        def _():
            for t in TENSORS:
                sx[p - N1 - 1, t] = rd[p, 0, t, :, 1 - mx]
                sy[p - N1 - 1, t] = rd[p, 1, t, 1 - my]

    def stage3(p):
        for ab in BOTH:
            @pl.when(p == 0)
            def _():
                for n in range(NS):
                    s2_copy(0, ab, n).wait_recv()

            @pl.when(p > 0)
            def _():
                s2_copy(p, ab).wait_recv()
            for t in TENSORS:
                r2[p, ab, t] = r2[p, ab, t] + (rd[p, 0, t, :, mx] if ab == 0 else rd[p, 1, t, my])
            s3_copy(p, ab).start()

    def stage4(p):
        for ab in BOTH:
            s3_copy(p, ab).wait_recv()
            keep = my if ab == 0 else mx
            vals = silu_parts(*(r3[p, ab, t] + r2[p, ab, t, keep] for t in TENSORS))
            for t in TENSORS:
                gat[p, ab, c, my, mx, t] = vals[t]
            net.first(p, ab, False).start()

    def stage5(p):
        for ab in BOTH:
            net.first(p, ab, True).wait_recv()
            net.second(p, ab, False).start()

        @pl.when(p == N1 - 1)
        def _():
            for ab in BOTH:
                s2_copy(N1, ab).start()

    def stage6(p):
        for ab in BOTH:
            net.second(p, ab, True).wait_recv()
        net.third(p, False).start()

    def stage7(p):
        net.third(p, True).wait_recv()
        y_part(acc, gat, lambda q, lo, w: wd[q, lo:lo + w, :], p, 0, FC)
        dx_part(acc, gat, *(lambda q, lo, w, r=r: r[q, :, lo:lo + w] for r in (wg, wu)), p, 0, FC)

    for cp in w_copies(0):
        cp.wait()
    for n in range(NS):
        for ab in BOTH:
            product(0, ab, n)
            d_copy(0, ab, n).start()
    for n in range(NS):
        for ab in BOTH:
            d_copy(0, ab, n).wait_recv()
            rd[0, ab, :, :, :, :, sub(n)] = rd[0, ab, :, :, :, :, sub(n)] + part[0, c, ab, :, :, :, :, sub(n)]
            s2_copy(0, ab, n).start()

    @pl.loop(0, N1 + 5)
    def _(i):
        pl.when((i >= 1) & (i < NP))(lambda: stage2(i))
        pl.when((i >= 1) & (i < N1 + 1))(lambda: stage3(i - 1))
        pl.when((i >= 2) & (i < N1 + 2))(lambda: stage4(i - 2))
        pl.when((i >= 3) & (i < N1 + 3))(lambda: stage5(i - 3))
        pl.when((i >= 4) & (i < N1 + 4))(lambda: stage6(i - 4))
        pl.when(i < NP - 1)(lambda: products(i + 1))
        pl.when(i >= 5)(lambda: stage7(i - 5))

    @pl.loop(0, N1)
    def _(p):
        for ab in BOTH:
            s3_copy(p, ab).wait_send()
            net.first(p, ab, False).wait_send()
            net.second(p, ab, False).wait_send()
        net.third(p, False).wait_send()

    @pl.loop(1, N1)
    def _(p):
        for ab in BOTH:
            s2_copy(p, ab).wait_send()
    for n in range(NS):
        for ab in BOTH:
            s2_copy(0, ab, n).wait_send()
    for p in (NP - 2, NP - 1):
        for ab in BOTH:
            d_copy(p, ab).wait_send()

    @pl.loop(1, 16)
    def _(k):
        x_copy(k, at.mine).wait_send()
    for ab in BOTH:
        s2_copy(N1, ab).wait_send()
        s2_copy(N1, ab).wait_recv()


def second_kernel(wg_hbm, wu_hbm, wd_hbm, xs_ref, acc_in, rows, rx, ry, kx, ky, r2n,
                  y_ref, gx_ref, lwg, lwu, lwd,
                  gat, wg, wu, wd, r2b, r3, acc, fin,
                  w_sem, s3_send, s3_recv, s4_send, s4_recv, s5_send, s5_recv, s5l_send, s5l_recv,
                  s6_send, s6_recv, s6l_send, s6l_recv, o_send, o_recv):
    at = Place()
    c, mx, my = at.c, at.x, at.y
    net = Gather(at, gat, (s4_send, s4_recv), (s5_send, s5_recv), (s6_send, s6_recv),
                 (s5l_send, s5l_recv), (s6l_send, s6l_recv))
    barrier = pltpu.get_barrier_semaphore()
    for nb in (at.x_nb, at.y_nb, at.core_nb, (1 - at.tp, at.dp)):
        pl.semaphore_signal(barrier, inc=1, device_id=nb, device_id_type=MESH)
    cols = pl.ds(N1 * 2 * FC, NB * 2 * FC)
    w_copies = (pltpu.make_async_copy(wg_hbm.at[:, cols], wg, w_sem.at[0]),
                pltpu.make_async_copy(wu_hbm.at[:, cols], wu, w_sem.at[1]),
                pltpu.make_async_copy(wd_hbm.at[cols, :], wd, w_sem.at[2]))
    for cp in w_copies:
        cp.start()

    def s3_copy(q, ab):
        src = r2b.at[q, 0, :, 1 - my] if ab == 0 else r2b.at[q, 1, :, 1 - mx]
        return remote(src, r3.at[q, ab], s3_send.at[ab, q], s3_recv.at[ab, q], at.y_nb if ab == 0 else at.x_nb)

    def halves(q):
        for ab in BOTH:
            for t in TENSORS:
                got = r2n[ab, t] if q == 0 else (rx, ry)[ab][q - 1, t]
                r2b[q, ab, t] = got + (kx, ky)[ab][q, t]

    def send_quarters(q):
        for ab in BOTH:
            s3_copy(q, ab).start()

    def activate(q):
        for ab in BOTH:
            s3_copy(q, ab).wait_recv()
            keep = my if ab == 0 else mx
            vals = silu_parts(*(r3[q, ab, t] + r2b[q, ab, t, keep] for t in TENSORS))
            for t in TENSORS:
                gat[q, ab, c, my, mx, t] = vals[t]
            net.first(q, ab, False).start()

    def spread(q):
        for ab in BOTH:
            net.first(q, ab, True).wait_recv()
            if q < NB - 1:
                net.second(q, ab, False).start()
            else:
                for n in TENSORS:
                    net.second(q, ab, False, n).start()

    def cross(q):
        for ab in BOTH:
            net.second(q, ab, True).wait_recv()
        net.third(q, False).start()

    def down(q, lo, w):
        return wd[q * 2 * FC + lo:q * 2 * FC + lo + w, :]

    def gate(q, lo, w):
        return wg[:, q * 2 * FC + lo:q * 2 * FC + lo + w]

    def up(q, lo, w):
        return wu[:, q * 2 * FC + lo:q * 2 * FC + lo + w]

    halves(0)
    pl.semaphore_wait(barrier, 4)
    send_quarters(0)
    for q in range(1, NB):
        halves(q)
        if q < NB - 1:
            send_quarters(q)
    acc[...] = acc_in[...]
    for q in range(NB):
        activate(q)
        if q == 0:
            send_quarters(NB - 1)
        else:
            spread(q - 1)
    spread(NB - 1)
    for cp in w_copies:
        cp.wait()
    q = NB - 1

    def o_copy(j, k, slot):
        ot, od = at.other(k)
        return remote(acc.at[j, blk(ot, od)], fin.at[j, slot], o_send.at[j, k], o_recv.at[j, slot], (ot, od))

    def send_out(j):
        @pl.loop(1, 16)
        def _(k):
            o_copy(j, k, at.me).start()
        fin[j, at.me] = acc[j, at.mine]

    def finish(n):
        net.third(q, True, n).wait_recv()
        if n == 0:
            y_part(acc, gat, down, q, 0, FC)
            send_out(0)
        else:
            dx_part(acc, gat, gate, up, q, 0, FC, (n,))
        if n == 2:
            send_out(1)

    def late(k):
        lo = pl.ds(pl.multiple_of(k * FC, FC), FC)
        h, da, db = (gat[k // 2, k % 2, :, :, :, t].reshape(128, FC) for t in TENSORS)
        lwg[:, lo] = _dot(xs_ref[0], da, 0, 0)
        lwu[:, lo] = _dot(xs_ref[0], db, 0, 0)
        lwd[lo, :] = _dot(h, xs_ref[1], 0, 0)

    def cross_last(n):
        for ab in BOTH:
            net.second(q, ab, True, n).wait_recv()
        net.third(q, False, n).start()

    cross(0)
    for p in range(1, NB - 1):
        net.third(p - 1, True).wait_recv()
        y_part(acc, gat, down, p - 1, 0, FC)
        dx_part(acc, gat, gate, up, p - 1, 0, FC)
        cross(p)
    late(0)
    cross_last(0)
    late(1)
    cross_last(1)
    net.third(q - 1, True).wait_recv()
    y_part(acc, gat, down, q - 1, 0, FC)
    cross_last(2)
    finish(0)
    dx_part(acc, gat, gate, up, q - 1, 0, FC)
    finish(1)
    finish(2)

    pl.loop(2, 2 * NB)(late)

    for q in range(NB):
        for ab in BOTH:
            s3_copy(q, ab).wait_send()
            net.first(q, ab, False).wait_send()
            if q < NB - 1:
                net.second(q, ab, False).wait_send()
            else:
                for n in TENSORS:
                    net.second(q, ab, False, n).wait_send()
        if q < NB - 1:
            net.third(q, False).wait_send()
        else:
            for n in TENSORS:
                net.third(q, False, n).wait_send()

    for j, out in enumerate((y_ref, gx_ref)):
        @pl.loop(1, 16)
        def _(k):
            ot, od = at.other(k)
            o_copy(j, k, ot * 8 + od).wait_recv()
        for dd in range(8):
            cols = slice(dd * DL, (dd + 1) * DL)
            out[:, cols] = (rows[j, :, cols].astype(F32) + (fin[j, dd] + fin[j, 8 + dd])).astype(BF)

    @pl.loop(1, 16)
    def _(k):
        for j in BOTH:
            o_copy(j, k, at.me).wait_send()


def early_grads(xs_ref, g_ref, dwg_ref, dwu_ref, dwd_ref):
    q, ab = pl.program_id(0) // 2, lax.rem(pl.program_id(0), 2)
    h, da, db = (g_ref[q, ab, :, :, :, t].reshape(128, FC) for t in TENSORS)
    dwg_ref[...] = _dot(xs_ref[0], da, 0, 0)
    dwu_ref[...] = _dot(xs_ref[0], db, 0, 0)
    dwd_ref[...] = _dot(h, xs_ref[1], 0, 0)


def late_grads(y_ref, gx_ref, lwg, lwu, lwd, a_ref, b_ref, c_ref, yo_ref, gxo_ref, dwg_ref, dwu_ref, dwd_ref, sem, row_sem):
    copies = [pltpu.make_async_copy(y_ref, yo_ref, row_sem.at[0]), pltpu.make_async_copy(gx_ref, gxo_ref, row_sem.at[1])]
    for k in range(NB):
        src = pl.ds(k * 2 * FC, 2 * FC)
        dst = pl.ds((N1 + k) * 2 * FC, 2 * FC)
        copies += [pltpu.make_async_copy(lwg.at[:, src], dwg_ref.at[:, dst], sem.at[0, k]),
                   pltpu.make_async_copy(lwu.at[:, src], dwu_ref.at[:, dst], sem.at[1, k]),
                   pltpu.make_async_copy(lwd.at[src, :], dwd_ref.at[dst, :], sem.at[2, k])]
    for cp in copies:
        cp.start()
    for cp in copies:
        cp.wait()


def local_step(x_loc, wg_loc, wu_loc, wd_loc, gy_loc):
    vm = pl.BlockSpec(memory_space=pltpu.VMEM)
    hb = pl.BlockSpec(memory_space=pl.ANY)
    hbm = pl.BlockSpec(memory_space=pltpu.HBM)
    dma = pltpu.SemaphoreType.DMA
    row = jax.ShapeDtypeStruct((8, D), BF)
    kib = 1024
    half = (3, 2, 16, FC)
    xs, gat1, acc, rows, sx, sy, kx, ky, r2n = pl.pallas_call(
        first_kernel,
        out_shape=(pltpu.VMEM((2, 128, DL), BF), pltpu.VMEM((N1, 2, 2, 2, 2, 3, 16, FC), BF),
                   pltpu.VMEM((2, 16, 8, DL), F32), pltpu.VMEM((2, 8, D), BF),
                   pltpu.VMEM((NB - 1,) + half, F32), pltpu.VMEM((NB - 1,) + half, F32),
                   pltpu.VMEM((NB,) + half, F32), pltpu.VMEM((NB,) + half, F32), pltpu.VMEM((2,) + half, F32)),
        in_specs=[hbm] * 5,
        out_specs=(vm,) * 9,
        scratch_shapes=[
            pltpu.VMEM((NP, DL, 2 * FC), BF),
            pltpu.VMEM((NP, DL, 2 * FC), BF),
            pltpu.VMEM((NP, 2 * FC, DL), BF),
            pltpu.VMEM((NP, 2, 3, 2, 2, 16, FC), F32),
            pltpu.VMEM((N1, 2) + half, F32),
            pltpu.VMEM((8, 2, 8, DL), BF),
            pltpu.VMEM((16, 2, 8, DL), BF),
            pltpu.VMEM((2, 2, 2, 3, 2, 2, 16, FC), F32),
            pltpu.VMEM((N1, 2, 3, 16, FC), F32),
            dma((2,)), dma((3, NP)), dma((16,)), dma((16,)),
            dma((2, NP)), dma((2, NP)), dma((2, NS)), dma((2, NS)),
            dma((2, NP)), dma((2, NP)), dma((2, NS)), dma((2, NS)),
            dma((2, N1)), dma((2, N1)), dma((2, N1)), dma((2, N1)),
            dma((2, N1)), dma((2, N1)), dma((N1,)), dma((N1,)),
        ],
        compiler_params=pltpu.CompilerParams(
            collective_id=0, has_side_effects=True, vmem_limit_bytes=49000 * kib),
        name="mlp_first",
    )(x_loc, gy_loc, wg_loc, wu_loc, wd_loc)

    rx = lax.ppermute(sx, "dp", [(i, i + 2 if i % 4 < 2 else i - 2) for i in range(8)])
    ry = lax.ppermute(sy, "dp", [(i, (i + 4) % 8) for i in range(8)])

    full = (jax.ShapeDtypeStruct((DL, FF_LOC), F32), jax.ShapeDtypeStruct((DL, FF_LOC), F32),
            jax.ShapeDtypeStruct((FF_LOC, DL), F32))

    dwg, dwu, dwd = pl.pallas_call(
        early_grads,
        grid=(2 * N1,),
        out_shape=full,
        in_specs=[vm, vm],
        out_specs=(pl.BlockSpec((DL, FC), lambda k: (0, k)), pl.BlockSpec((DL, FC), lambda k: (0, k)),
                   pl.BlockSpec((FC, DL), lambda k: (k, 0))),
        cost_estimate=pl.CostEstimate(flops=12 * N1 * 128 * DL * FC, bytes_accessed=24 * N1 * DL * FC,
                                      transcendentals=0),
        compiler_params=pltpu.CompilerParams(dimension_semantics=("arbitrary",), vmem_limit_bytes=9000 * kib),
        name="mlp_early_grads",
    )(xs, gat1)

    y_rows, gx_rows, lwg, lwu, lwd = pl.pallas_call(
        second_kernel,
        out_shape=(pltpu.VMEM((8, D), BF), pltpu.VMEM((8, D), BF), pltpu.VMEM((DL, NB * 2 * FC), F32),
                   pltpu.VMEM((DL, NB * 2 * FC), F32), pltpu.VMEM((NB * 2 * FC, DL), F32)),
        in_specs=[hbm] * 3 + [vm] * 8,
        out_specs=(vm,) * 5,
        scratch_shapes=[
            pltpu.VMEM((NB, 2, 2, 2, 2, 3, 16, FC), BF),
            pltpu.VMEM((DL, NB * 2 * FC), BF),
            pltpu.VMEM((DL, NB * 2 * FC), BF),
            pltpu.VMEM((NB * 2 * FC, DL), BF),
            pltpu.VMEM((NB, 2) + half, F32),
            pltpu.VMEM((NB, 2, 3, 16, FC), F32),
            pltpu.VMEM((2, 16, 8, DL), F32),
            pltpu.VMEM((2, 16, 8, DL), F32),
            dma((3,)), dma((2, NB)), dma((2, NB)), dma((2, NB)), dma((2, NB)),
            dma((2, NB)), dma((2, NB)), dma((2, 3)), dma((2, 3)),
            dma((NB,)), dma((NB,)), dma((3,)), dma((3,)),
            dma((2, 16)), dma((2, 16)),
        ],
        compiler_params=pltpu.CompilerParams(
            collective_id=1, has_side_effects=True, vmem_limit_bytes=30000 * kib),
        name="mlp_second",
    )(wg_loc, wu_loc, wd_loc, xs, acc, rows, rx, ry, kx, ky, r2n)

    return pl.pallas_call(
        late_grads,
        out_shape=(row, row) + full,
        in_specs=[vm] * 5 + [hbm] * 3,
        out_specs=(hbm,) * 5,
        input_output_aliases={5: 2, 6: 3, 7: 4},
        scratch_shapes=[dma((3, NB)), dma((2,))],
        compiler_params=pltpu.CompilerParams(vmem_limit_bytes=30000 * kib),
        name="mlp_late_grads",
    )(y_rows, gx_rows, lwg, lwu, lwd, dwg, dwu, dwd)


def solution(mesh):
    row_spec = P(("dp", "tp"), None)
    up_spec = P("dp", "tp")
    down_spec = P("tp", "dp")
    return jax.shard_map(local_step, mesh=mesh,
                         in_specs=(row_spec, up_spec, up_spec, down_spec, row_spec),
                         out_specs=(row_spec, row_spec, up_spec, up_spec, down_spec),
                         check_vma=False)
```

```python
import itertools

import jax
import jax.numpy as jnp
from jax import lax
from jax.experimental import pallas as pl
from jax.experimental.pallas import tpu as pltpu
from jax.sharding import PartitionSpec as P

MESH = pl.DeviceIdType.MESH
BF = jnp.bfloat16
F32 = jnp.float32

BOTH = range(2)
TENSORS = range(3)
D = 3072
FF_LOC = 12288
DL = 384
NP = 8
N1 = 5
NB = NP - N1
FC = FF_LOC // (2 * NP)
NS = 3
SUB = FC // NS


def _dot(a, b, ca, cb):
    return lax.dot_general(a, b, (((ca,), (cb,)), ((), ())), preferred_element_type=F32)


def remote(src, dst, send, recv, dev):
    return pltpu.make_async_remote_copy(src_ref=src, dst_ref=dst, send_sem=send, recv_sem=recv,
                                        device_id=dev, device_id_type=MESH)


def sub(n):
    return pl.ds(n * SUB, SUB)


def block(tt, cc, yy, xx):
    return (cc * 4 + yy * 2 + xx) * 2 + tt


class Place:
    def __init__(self):
        tp, dp = lax.axis_index("tp"), lax.axis_index("dp")
        c, x, y = lax.rem(dp, 2), lax.rem(dp // 2, 2), dp // 4
        self.tp, self.dp, self.c, self.x, self.y = tp, dp, c, x, y
        self.me = tp * 8 + dp
        self.core_nb = (tp, y * 4 + x * 2 + (1 - c))
        self.x_nb = (tp, y * 4 + (1 - x) * 2 + c)
        self.y_nb = (tp, (1 - y) * 4 + x * 2 + c)
        self.mine = block(tp, c, y, x)
        flips = sorted(itertools.product(BOTH, repeat=4), key=sum, reverse=True)[:-1]
        self.others = []
        for ft, fy, fx, fc in flips:
            tt, yy, xx, cc = (1 - v if f else v for v, f in zip((tp, y, x, c), (ft, fy, fx, fc)))
            self.others.append((tt, yy * 4 + xx * 2 + cc, block(tt, cc, yy, xx)))

    def greet(self):
        barrier = pltpu.get_barrier_semaphore()
        for tt, dd, _ in self.others:
            pl.semaphore_signal(barrier, inc=1, device_id=(tt, dd), device_id_type=MESH)
        return barrier


def silu_parts(a, b, g):
    s = jax.nn.sigmoid(a)
    silu = a * s
    return ((silu * b).astype(BF), (g * b * (s * (1.0 + a * (1.0 - s)))).astype(BF), (g * silu).astype(BF))


def accumulate(acc, j, v):
    acc[j] = acc[j] + v.reshape(16, 8, DL)


def y_part(acc, gat, wd, q, lo, w):
    v = None
    for ab in BOTH:
        h = gat[q, ab, :, :, :, 0, :, lo:lo + w].reshape(128, w)
        d = _dot(h, wd(q, ab * FC + lo, w), 1, 0)
        v = d if v is None else v + d
    accumulate(acc, 0, v)


def dx_part(acc, gat, wg, wu, q, lo, w, ts=(1, 2)):
    v = None
    for ab in BOTH:
        for t, wt in ((t, (wg, wu)[t - 1]) for t in ts):
            z = gat[q, ab, :, :, :, t, :, lo:lo + w].reshape(128, w)
            d = _dot(z, wt(q, ab * FC + lo, w), 1, 1)
            v = d if v is None else v + d
    accumulate(acc, 1, v)


class Gather:
    def __init__(self, at, gat, s4, s5, s6, s5l=None, s6l=None):
        self.at, self.gat, self.s4, self.s5, self.s6, self.s5l, self.s6l = at, gat, s4, s5, s6, s5l, s6l

    def first(self, q, ab, arriving):
        at = self.at
        y0 = (1 - at.y) if arriving else at.y
        x1 = (1 - at.x) if arriving else at.x
        b = self.gat.at[q, 0, at.c, y0, at.x] if ab == 0 else self.gat.at[q, 1, at.c, at.y, x1]
        return remote(b, b, self.s4[0].at[ab, q], self.s4[1].at[ab, q], at.y_nb if ab == 0 else at.x_nb)

    def second(self, q, ab, arriving, n=None):
        at = self.at
        x0 = (1 - at.x) if arriving else at.x
        y1 = (1 - at.y) if arriving else at.y
        b = self.gat.at[q, 0, at.c, :, x0] if ab == 0 else self.gat.at[q, 1, at.c, y1]
        dev = at.x_nb if ab == 0 else at.y_nb
        if n is None:
            return remote(b, b, self.s5[0].at[ab, q], self.s5[1].at[ab, q], dev)
        b = b.at[:, n]
        return remote(b, b, self.s5l[0].at[ab, n], self.s5l[1].at[ab, n], dev)

    def third(self, q, arriving, n=None):
        at = self.at
        b = self.gat.at[q, :, (1 - at.c) if arriving else at.c]
        if n is None:
            return remote(b, b, self.s6[0].at[q], self.s6[1].at[q], at.core_nb)
        b = b.at[:, :, :, n]
        return remote(b, b, self.s6l[0].at[n], self.s6l[1].at[n], at.core_nb)


def first_kernel(x_hbm, gy_hbm, wg_hbm, wu_hbm, wd_hbm,
                 xs_ref, gat, acc, rows, sx, sy, kx, ky, r2n,
                 wg, wu, wd, rd, r2, st, xin, part, r3,
                 in_sem, w_sem, x_send, x_recv, d_send, d_recv, d0_send, d0_recv, s2_send, s2_recv, s20_send, s20_recv,
                 s3_send, s3_recv, s4_send, s4_recv, s5_send, s5_recv, s6_send, s6_recv):
    at = Place()
    c, mx, my = at.c, at.x, at.y
    net = Gather(at, gat, (s4_send, s4_recv), (s5_send, s5_recv), (s6_send, s6_recv))

    def w_copies(p):
        cols = pl.ds(pl.multiple_of(p * 2 * FC, 2 * FC), 2 * FC)
        return (pltpu.make_async_copy(wg_hbm.at[:, cols], wg.at[p], w_sem.at[0, p]),
                pltpu.make_async_copy(wu_hbm.at[:, cols], wu.at[p], w_sem.at[1, p]),
                pltpu.make_async_copy(wd_hbm.at[cols, :], wd.at[p], w_sem.at[2, p]))

    in_copies = [pltpu.make_async_copy(r, rows.at[j], in_sem.at[j]) for j, r in enumerate((x_hbm, gy_hbm))]
    for cp in in_copies:
        cp.start()
    barrier = at.greet()

    @pl.loop(0, NP)
    def _(p):
        for cp in w_copies(p):
            cp.start()

    acc[...] = jnp.zeros_like(acc)
    for j in BOTH:
        in_copies[j].wait()
        for dd in range(8):
            st[dd, j] = rows[j, :, dd * DL:(dd + 1) * DL]
    pl.semaphore_wait(barrier, 15)

    def x_copy(k, b):
        tt, dd, _ = at.others[k]
        return remote(st.at[dd], xin.at[b], x_send.at[k], x_recv.at[k], (tt, dd))

    everyone = range(len(at.others))
    for k in everyone:
        x_copy(k, at.mine).start()
    xin[at.mine] = st[at.dp]
    for k in everyone:
        x_copy(k, at.others[k][2]).wait_recv()

    for j in BOTH:
        xs_ref[j] = xin[:, j].astype(F32).reshape(128, DL).astype(BF)

    def d_copy(p, ab, n=None):
        s = lax.rem(p, 2)
        if n is None:
            return remote(part.at[s, 1 - c, ab], rd.at[p, ab], d_send.at[ab, p], d_recv.at[ab, p], at.core_nb)
        return remote(part.at[s, 1 - c, ab, :, :, :, :, sub(n)], rd.at[p, ab, :, :, :, :, sub(n)],
                      d0_send.at[ab, n], d0_recv.at[ab, n], at.core_nb)

    def s2_copy(p, ab, n=None):
        src = rd.at[p, 0, :, :, 1 - mx] if ab == 0 else rd.at[p, 1, :, 1 - my]
        dst = r2n.at[ab] if p is N1 else r2.at[p, ab]
        dev = at.x_nb if ab == 0 else at.y_nb
        if n is None:
            return remote(src, dst, s2_send.at[ab, p], s2_recv.at[ab, p], dev)
        return remote(src.at[:, :, :, sub(n)], dst.at[:, :, :, sub(n)], s20_send.at[ab, n], s20_recv.at[ab, n], dev)

    def s3_copy(p, ab):
        src = r2.at[p, 0, :, 1 - my] if ab == 0 else r2.at[p, 1, :, 1 - mx]
        return remote(src, r3.at[p, ab], s3_send.at[ab, p], s3_recv.at[ab, p], at.y_nb if ab == 0 else at.x_nb)

    def product(p, ab, n):
        s = lax.rem(p, 2)
        cols = pl.ds(ab * FC + n * SUB, SUB)
        vals = (_dot(xs_ref[0], wg[p, :, cols], 1, 0),
                _dot(xs_ref[0], wu[p, :, cols], 1, 0),
                _dot(xs_ref[1], wd[p, cols, :], 1, 1))
        for t in TENSORS:
            v = vals[t].reshape(2, 2, 2, 16, SUB)
            for cc in BOTH:
                part[s, cc, ab, t, :, :, :, sub(n)] = v[cc]

    def products(p):
        for cp in w_copies(p):
            cp.wait()
        for ab in BOTH:
            @pl.when(p >= 3)
            def _():
                d_copy(p - 2, ab).wait_send()

            @pl.when(p == 2)
            def _():
                for n in range(NS):
                    d_copy(0, ab, n).wait_send()
            for n in range(NS):
                product(p, ab, n)
            d_copy(p, ab).start()

    def stage2(p):
        s = lax.rem(p, 2)
        for ab in BOTH:
            d_copy(p, ab).wait_recv()
            for t in TENSORS:
                rd[p, ab, t] = rd[p, ab, t] + part[s, c, ab, t]

            @pl.when(p < N1)
            def _():
                s2_copy(p, ab).start()

        @pl.when(p >= N1)
        def _():
            for t in TENSORS:
                kx[p - N1, t] = rd[p, 0, t, :, mx]
                ky[p - N1, t] = rd[p, 1, t, my]

        @pl.when(p > N1)
        def _():
            for t in TENSORS:
                sx[p - N1 - 1, t] = rd[p, 0, t, :, 1 - mx]
                sy[p - N1 - 1, t] = rd[p, 1, t, 1 - my]

    def stage3(p):
        for ab in BOTH:
            @pl.when(p == 0)
            def _():
                for n in range(NS):
                    s2_copy(0, ab, n).wait_recv()

            @pl.when(p > 0)
            def _():
                s2_copy(p, ab).wait_recv()
            for t in TENSORS:
                r2[p, ab, t] = r2[p, ab, t] + (rd[p, 0, t, :, mx] if ab == 0 else rd[p, 1, t, my])
            s3_copy(p, ab).start()

    def stage4(p):
        for ab in BOTH:
            s3_copy(p, ab).wait_recv()
            keep = my if ab == 0 else mx
            vals = silu_parts(*(r3[p, ab, t] + r2[p, ab, t, keep] for t in TENSORS))
            for t in TENSORS:
                gat[p, ab, c, my, mx, t] = vals[t]
            net.first(p, ab, False).start()

    def stage5(p):
        for ab in BOTH:
            net.first(p, ab, True).wait_recv()
            net.second(p, ab, False).start()

        @pl.when(p == N1 - 1)
        def _():
            for ab in BOTH:
                s2_copy(N1, ab).start()

    def stage6(p):
        for ab in BOTH:
            net.second(p, ab, True).wait_recv()
        net.third(p, False).start()

    def stage7(p):
        net.third(p, True).wait_recv()
        y_part(acc, gat, lambda q, lo, w: wd[q, lo:lo + w, :], p, 0, FC)
        dx_part(acc, gat, *(lambda q, lo, w, r=r: r[q, :, lo:lo + w] for r in (wg, wu)), p, 0, FC)

    for cp in w_copies(0):
        cp.wait()
    for n in range(NS):
        for ab in BOTH:
            product(0, ab, n)
            d_copy(0, ab, n).start()
    for n in range(NS):
        for ab in BOTH:
            d_copy(0, ab, n).wait_recv()
            rd[0, ab, :, :, :, :, sub(n)] = rd[0, ab, :, :, :, :, sub(n)] + part[0, c, ab, :, :, :, :, sub(n)]
            s2_copy(0, ab, n).start()

    @pl.loop(0, N1 + 5)
    def _(i):
        pl.when((i >= 1) & (i < NP))(lambda: stage2(i))
        pl.when((i >= 1) & (i < N1 + 1))(lambda: stage3(i - 1))
        pl.when((i >= 2) & (i < N1 + 2))(lambda: stage4(i - 2))
        pl.when((i >= 3) & (i < N1 + 3))(lambda: stage5(i - 3))
        pl.when((i >= 4) & (i < N1 + 4))(lambda: stage6(i - 4))
        pl.when(i < NP - 1)(lambda: products(i + 1))
        pl.when(i >= 5)(lambda: stage7(i - 5))

    @pl.loop(0, N1)
    def _(p):
        for ab in BOTH:
            s3_copy(p, ab).wait_send()
            net.first(p, ab, False).wait_send()
            net.second(p, ab, False).wait_send()
        net.third(p, False).wait_send()

    @pl.loop(1, N1)
    def _(p):
        for ab in BOTH:
            s2_copy(p, ab).wait_send()
    for n in range(NS):
        for ab in BOTH:
            s2_copy(0, ab, n).wait_send()
    for p in (NP - 2, NP - 1):
        for ab in BOTH:
            d_copy(p, ab).wait_send()

    for k in everyone:
        x_copy(k, at.mine).wait_send()
    for ab in BOTH:
        s2_copy(N1, ab).wait_send()
        s2_copy(N1, ab).wait_recv()


def second_kernel(wg_hbm, wu_hbm, wd_hbm, xs_ref, acc_in, rows, rx, ry, kx, ky, r2n,
                  y_ref, gx_ref, lwg, lwu, lwd,
                  gat, wg, wu, wd, r2b, r3, acc, fin,
                  w_sem, s3_send, s3_recv, s4_send, s4_recv, s5_send, s5_recv, s5l_send, s5l_recv,
                  s6_send, s6_recv, s6l_send, s6l_recv, o_send, o_recv):
    at = Place()
    c, mx, my = at.c, at.x, at.y
    net = Gather(at, gat, (s4_send, s4_recv), (s5_send, s5_recv), (s6_send, s6_recv),
                 (s5l_send, s5l_recv), (s6l_send, s6l_recv))
    barrier = pltpu.get_barrier_semaphore()
    for nb in (at.x_nb, at.y_nb, at.core_nb, (1 - at.tp, at.dp)):
        pl.semaphore_signal(barrier, inc=1, device_id=nb, device_id_type=MESH)
    cols = pl.ds(N1 * 2 * FC, NB * 2 * FC)
    w_copies = (pltpu.make_async_copy(wg_hbm.at[:, cols], wg, w_sem.at[0]),
                pltpu.make_async_copy(wu_hbm.at[:, cols], wu, w_sem.at[1]),
                pltpu.make_async_copy(wd_hbm.at[cols, :], wd, w_sem.at[2]))
    for cp in w_copies:
        cp.start()

    def s3_copy(q, ab):
        src = r2b.at[q, 0, :, 1 - my] if ab == 0 else r2b.at[q, 1, :, 1 - mx]
        return remote(src, r3.at[q, ab], s3_send.at[ab, q], s3_recv.at[ab, q], at.y_nb if ab == 0 else at.x_nb)

    def halves(q):
        for ab in BOTH:
            for t in TENSORS:
                got = r2n[ab, t] if q == 0 else (rx, ry)[ab][q - 1, t]
                r2b[q, ab, t] = got + (kx, ky)[ab][q, t]

    def send_quarters(q):
        for ab in BOTH:
            s3_copy(q, ab).start()

    def activate(q):
        for ab in BOTH:
            s3_copy(q, ab).wait_recv()
            keep = my if ab == 0 else mx
            vals = silu_parts(*(r3[q, ab, t] + r2b[q, ab, t, keep] for t in TENSORS))
            for t in TENSORS:
                gat[q, ab, c, my, mx, t] = vals[t]
            net.first(q, ab, False).start()

    def spread(q):
        for ab in BOTH:
            net.first(q, ab, True).wait_recv()
            if q < NB - 1:
                net.second(q, ab, False).start()
            else:
                for n in TENSORS:
                    net.second(q, ab, False, n).start()

    def cross(q):
        for ab in BOTH:
            net.second(q, ab, True).wait_recv()
        net.third(q, False).start()

    def down(q, lo, w):
        return wd[q * 2 * FC + lo:q * 2 * FC + lo + w, :]

    def gate(q, lo, w):
        return wg[:, q * 2 * FC + lo:q * 2 * FC + lo + w]

    def up(q, lo, w):
        return wu[:, q * 2 * FC + lo:q * 2 * FC + lo + w]

    halves(0)
    pl.semaphore_wait(barrier, 4)
    send_quarters(0)
    for q in range(1, NB):
        halves(q)
        if q < NB - 1:
            send_quarters(q)
    acc[...] = acc_in[...]
    for q in range(NB):
        activate(q)
        if q == 0:
            send_quarters(NB - 1)
        else:
            spread(q - 1)
    spread(NB - 1)
    for cp in w_copies:
        cp.wait()
    q = NB - 1

    everyone = range(len(at.others))

    def o_copy(j, k, slot):
        tt, dd, b = at.others[k]
        return remote(acc.at[j, b], fin.at[j, slot], o_send.at[j, k], o_recv.at[j, k], (tt, dd))

    def send_out(j):
        for k in everyone:
            o_copy(j, k, at.me).start()
        fin[j, at.me] = acc[j, at.mine]

    def finish(n):
        net.third(q, True, n).wait_recv()
        if n == 0:
            y_part(acc, gat, down, q, 0, FC)
            send_out(0)
        else:
            dx_part(acc, gat, gate, up, q, 0, FC, (n,))
        if n == 2:
            send_out(1)

    def late(k):
        lo = pl.ds(pl.multiple_of(k * FC, FC), FC)
        h, da, db = (gat[k // 2, k % 2, :, :, :, t].reshape(128, FC) for t in TENSORS)
        lwg[:, lo] = _dot(xs_ref[0], da, 0, 0)
        lwu[:, lo] = _dot(xs_ref[0], db, 0, 0)
        lwd[lo, :] = _dot(h, xs_ref[1], 0, 0)

    def cross_last(n):
        for ab in BOTH:
            net.second(q, ab, True, n).wait_recv()
        net.third(q, False, n).start()

    cross(0)
    for p in range(1, NB - 1):
        net.third(p - 1, True).wait_recv()
        y_part(acc, gat, down, p - 1, 0, FC)
        dx_part(acc, gat, gate, up, p - 1, 0, FC)
        cross(p)
    late(0)
    cross_last(0)
    late(1)
    cross_last(1)
    net.third(q - 1, True).wait_recv()
    y_part(acc, gat, down, q - 1, 0, FC)
    cross_last(2)
    finish(0)
    dx_part(acc, gat, gate, up, q - 1, 0, FC)
    finish(1)
    finish(2)

    pl.loop(2, 2 * NB)(late)

    for q in range(NB):
        for ab in BOTH:
            s3_copy(q, ab).wait_send()
            net.first(q, ab, False).wait_send()
            if q < NB - 1:
                net.second(q, ab, False).wait_send()
            else:
                for n in TENSORS:
                    net.second(q, ab, False, n).wait_send()
        if q < NB - 1:
            net.third(q, False).wait_send()
        else:
            for n in TENSORS:
                net.third(q, False, n).wait_send()

    for j, out in enumerate((y_ref, gx_ref)):
        for k in everyone:
            tt, dd, _ = at.others[k]
            o_copy(j, k, tt * 8 + dd).wait_recv()
        for dd in range(8):
            cols = slice(dd * DL, (dd + 1) * DL)
            out[:, cols] = (rows[j, :, cols].astype(F32) + (fin[j, dd] + fin[j, 8 + dd])).astype(BF)

    for k in everyone:
        for j in BOTH:
            o_copy(j, k, at.me).wait_send()


def early_grads(xs_ref, g_ref, dwg_ref, dwu_ref, dwd_ref):
    q, ab = pl.program_id(0) // 2, lax.rem(pl.program_id(0), 2)
    h, da, db = (g_ref[q, ab, :, :, :, t].reshape(128, FC) for t in TENSORS)
    dwg_ref[...] = _dot(xs_ref[0], da, 0, 0)
    dwu_ref[...] = _dot(xs_ref[0], db, 0, 0)
    dwd_ref[...] = _dot(h, xs_ref[1], 0, 0)


def late_grads(y_ref, gx_ref, lwg, lwu, lwd, a_ref, b_ref, c_ref, yo_ref, gxo_ref, dwg_ref, dwu_ref, dwd_ref, sem, row_sem):
    copies = [pltpu.make_async_copy(y_ref, yo_ref, row_sem.at[0]), pltpu.make_async_copy(gx_ref, gxo_ref, row_sem.at[1])]
    for k in range(NB):
        src = pl.ds(k * 2 * FC, 2 * FC)
        dst = pl.ds((N1 + k) * 2 * FC, 2 * FC)
        copies += [pltpu.make_async_copy(lwg.at[:, src], dwg_ref.at[:, dst], sem.at[0, k]),
                   pltpu.make_async_copy(lwu.at[:, src], dwu_ref.at[:, dst], sem.at[1, k]),
                   pltpu.make_async_copy(lwd.at[src, :], dwd_ref.at[dst, :], sem.at[2, k])]
    for cp in copies:
        cp.start()
    for cp in copies:
        cp.wait()


def local_step(x_loc, wg_loc, wu_loc, wd_loc, gy_loc):
    vm = pl.BlockSpec(memory_space=pltpu.VMEM)
    hb = pl.BlockSpec(memory_space=pl.ANY)
    hbm = pl.BlockSpec(memory_space=pltpu.HBM)
    dma = pltpu.SemaphoreType.DMA
    row = jax.ShapeDtypeStruct((8, D), BF)
    kib = 1024
    half = (3, 2, 16, FC)
    xs, gat1, acc, rows, sx, sy, kx, ky, r2n = pl.pallas_call(
        first_kernel,
        out_shape=(pltpu.VMEM((2, 128, DL), BF), pltpu.VMEM((N1, 2, 2, 2, 2, 3, 16, FC), BF),
                   pltpu.VMEM((2, 16, 8, DL), F32), pltpu.VMEM((2, 8, D), BF),
                   pltpu.VMEM((NB - 1,) + half, F32), pltpu.VMEM((NB - 1,) + half, F32),
                   pltpu.VMEM((NB,) + half, F32), pltpu.VMEM((NB,) + half, F32), pltpu.VMEM((2,) + half, F32)),
        in_specs=[hbm] * 5,
        out_specs=(vm,) * 9,
        scratch_shapes=[
            pltpu.VMEM((NP, DL, 2 * FC), BF),
            pltpu.VMEM((NP, DL, 2 * FC), BF),
            pltpu.VMEM((NP, 2 * FC, DL), BF),
            pltpu.VMEM((NP, 2, 3, 2, 2, 16, FC), F32),
            pltpu.VMEM((N1, 2) + half, F32),
            pltpu.VMEM((8, 2, 8, DL), BF),
            pltpu.VMEM((16, 2, 8, DL), BF),
            pltpu.VMEM((2, 2, 2, 3, 2, 2, 16, FC), F32),
            pltpu.VMEM((N1, 2, 3, 16, FC), F32),
            dma((2,)), dma((3, NP)), dma((16,)), dma((16,)),
            dma((2, NP)), dma((2, NP)), dma((2, NS)), dma((2, NS)),
            dma((2, NP)), dma((2, NP)), dma((2, NS)), dma((2, NS)),
            dma((2, N1)), dma((2, N1)), dma((2, N1)), dma((2, N1)),
            dma((2, N1)), dma((2, N1)), dma((N1,)), dma((N1,)),
        ],
        compiler_params=pltpu.CompilerParams(
            collective_id=0, has_side_effects=True, vmem_limit_bytes=49000 * kib),
        name="mlp_first",
    )(x_loc, gy_loc, wg_loc, wu_loc, wd_loc)

    rx = lax.ppermute(sx, "dp", [(i, i + 2 if i % 4 < 2 else i - 2) for i in range(8)])
    ry = lax.ppermute(sy, "dp", [(i, (i + 4) % 8) for i in range(8)])

    full = (jax.ShapeDtypeStruct((DL, FF_LOC), F32), jax.ShapeDtypeStruct((DL, FF_LOC), F32),
            jax.ShapeDtypeStruct((FF_LOC, DL), F32))

    dwg, dwu, dwd = pl.pallas_call(
        early_grads,
        grid=(2 * N1,),
        out_shape=full,
        in_specs=[vm, vm],
        out_specs=(pl.BlockSpec((DL, FC), lambda k: (0, k)), pl.BlockSpec((DL, FC), lambda k: (0, k)),
                   pl.BlockSpec((FC, DL), lambda k: (k, 0))),
        cost_estimate=pl.CostEstimate(flops=12 * N1 * 128 * DL * FC, bytes_accessed=24 * N1 * DL * FC,
                                      transcendentals=0),
        compiler_params=pltpu.CompilerParams(dimension_semantics=("arbitrary",), vmem_limit_bytes=9000 * kib),
        name="mlp_early_grads",
    )(xs, gat1)

    y_rows, gx_rows, lwg, lwu, lwd = pl.pallas_call(
        second_kernel,
        out_shape=(pltpu.VMEM((8, D), BF), pltpu.VMEM((8, D), BF), pltpu.VMEM((DL, NB * 2 * FC), F32),
                   pltpu.VMEM((DL, NB * 2 * FC), F32), pltpu.VMEM((NB * 2 * FC, DL), F32)),
        in_specs=[hbm] * 3 + [vm] * 8,
        out_specs=(vm,) * 5,
        scratch_shapes=[
            pltpu.VMEM((NB, 2, 2, 2, 2, 3, 16, FC), BF),
            pltpu.VMEM((DL, NB * 2 * FC), BF),
            pltpu.VMEM((DL, NB * 2 * FC), BF),
            pltpu.VMEM((NB * 2 * FC, DL), BF),
            pltpu.VMEM((NB, 2) + half, F32),
            pltpu.VMEM((NB, 2, 3, 16, FC), F32),
            pltpu.VMEM((2, 16, 8, DL), F32),
            pltpu.VMEM((2, 16, 8, DL), F32),
            dma((3,)), dma((2, NB)), dma((2, NB)), dma((2, NB)), dma((2, NB)),
            dma((2, NB)), dma((2, NB)), dma((2, 3)), dma((2, 3)),
            dma((NB,)), dma((NB,)), dma((3,)), dma((3,)),
            dma((2, 16)), dma((2, 16)),
        ],
        compiler_params=pltpu.CompilerParams(
            collective_id=1, has_side_effects=True, vmem_limit_bytes=30000 * kib),
        name="mlp_second",
    )(wg_loc, wu_loc, wd_loc, xs, acc, rows, rx, ry, kx, ky, r2n)

    return pl.pallas_call(
        late_grads,
        out_shape=(row, row) + full,
        in_specs=[vm] * 5 + [hbm] * 3,
        out_specs=(hbm,) * 5,
        input_output_aliases={5: 2, 6: 3, 7: 4},
        scratch_shapes=[dma((3, NB)), dma((2,))],
        compiler_params=pltpu.CompilerParams(vmem_limit_bytes=30000 * kib),
        name="mlp_late_grads",
    )(y_rows, gx_rows, lwg, lwu, lwd, dwg, dwu, dwd)


def solution(mesh):
    row_spec = P(("dp", "tp"), None)
    up_spec = P("dp", "tp")
    down_spec = P("tp", "dp")
    return jax.shard_map(local_step, mesh=mesh,
                         in_specs=(row_spec, up_spec, up_spec, down_spec, row_spec),
                         out_specs=(row_spec, row_spec, up_spec, up_spec, down_spec),
                         check_vma=False)
```

```python
import itertools

import jax
import jax.numpy as jnp
from jax import lax
from jax.experimental import pallas as pl
from jax.experimental.pallas import tpu as pltpu
from jax.sharding import PartitionSpec as P

MESH = pl.DeviceIdType.MESH
BF = jnp.bfloat16
F32 = jnp.float32

BOTH = range(2)
TENSORS = range(3)
D = 3072
FF_LOC = 12288
DL = 384
NP = 8
N1 = 5
NB = NP - N1
FC = FF_LOC // (2 * NP)
SUB = 256


def _dot(a, b, ca, cb):
    return lax.dot_general(a, b, (((ca,), (cb,)), ((), ())), preferred_element_type=F32)


def remote(src, dst, send, recv, dev):
    return pltpu.make_async_remote_copy(src_ref=src, dst_ref=dst, send_sem=send, recv_sem=recv,
                                        device_id=dev, device_id_type=MESH)


def sub(n):
    return pl.ds(n * SUB, SUB)


def block(tt, cc, yy, xx):
    return (cc * 4 + yy * 2 + xx) * 2 + tt


class Place:
    def __init__(self):
        tp, dp = lax.axis_index("tp"), lax.axis_index("dp")
        c, x, y = lax.rem(dp, 2), lax.rem(dp // 2, 2), dp // 4
        self.tp, self.dp, self.c, self.x, self.y = tp, dp, c, x, y
        self.me = tp * 8 + dp
        self.core_nb = (tp, y * 4 + x * 2 + (1 - c))
        self.x_nb = (tp, y * 4 + (1 - x) * 2 + c)
        self.y_nb = (tp, (1 - y) * 4 + x * 2 + c)
        self.mine = block(tp, c, y, x)
        flips = sorted(itertools.product(BOTH, repeat=4), key=sum, reverse=True)[:-1]
        self.others = []
        for ft, fy, fx, fc in flips:
            tt, yy, xx, cc = (1 - v if f else v for v, f in zip((tp, y, x, c), (ft, fy, fx, fc)))
            self.others.append((tt, yy * 4 + xx * 2 + cc, block(tt, cc, yy, xx)))

    def greet(self):
        barrier = pltpu.get_barrier_semaphore()
        for tt, dd, _ in self.others:
            pl.semaphore_signal(barrier, inc=1, device_id=(tt, dd), device_id_type=MESH)
        return barrier


def silu_parts(a, b, g):
    s = jax.nn.sigmoid(a)
    silu = a * s
    return ((silu * b).astype(BF), (g * b * (s * (1.0 + a * (1.0 - s)))).astype(BF), (g * silu).astype(BF))


def accumulate(acc, j, v):
    acc[j] = acc[j] + v.reshape(16, 8, DL)


def y_part(acc, gat, wd, q, lo, w):
    v = None
    for ab in BOTH:
        h = gat[q, ab, :, :, :, 0, :, lo:lo + w].reshape(128, w)
        d = _dot(h, wd(q, ab * FC + lo, w), 1, 0)
        v = d if v is None else v + d
    accumulate(acc, 0, v)


def dx_part(acc, gat, wg, wu, q, lo, w, ts=(1, 2)):
    v = None
    for ab in BOTH:
        for t, wt in ((t, (wg, wu)[t - 1]) for t in ts):
            z = gat[q, ab, :, :, :, t, :, lo:lo + w].reshape(128, w)
            d = _dot(z, wt(q, ab * FC + lo, w), 1, 1)
            v = d if v is None else v + d
    accumulate(acc, 1, v)


class Gather:
    def __init__(self, at, gat, s4, s5, s6, s5l=None, s6l=None):
        self.at, self.gat, self.s4, self.s5, self.s6, self.s5l, self.s6l = at, gat, s4, s5, s6, s5l, s6l

    def first(self, q, ab, arriving):
        at = self.at
        y0 = (1 - at.y) if arriving else at.y
        x1 = (1 - at.x) if arriving else at.x
        b = self.gat.at[q, 0, at.c, y0, at.x] if ab == 0 else self.gat.at[q, 1, at.c, at.y, x1]
        return remote(b, b, self.s4[0].at[ab, q], self.s4[1].at[ab, q], at.y_nb if ab == 0 else at.x_nb)

    def second(self, q, ab, arriving, n=None):
        at = self.at
        x0 = (1 - at.x) if arriving else at.x
        y1 = (1 - at.y) if arriving else at.y
        b = self.gat.at[q, 0, at.c, :, x0] if ab == 0 else self.gat.at[q, 1, at.c, y1]
        dev = at.x_nb if ab == 0 else at.y_nb
        if n is None:
            return remote(b, b, self.s5[0].at[ab, q], self.s5[1].at[ab, q], dev)
        b = b.at[:, n]
        return remote(b, b, self.s5l[0].at[ab, n], self.s5l[1].at[ab, n], dev)

    def third(self, q, arriving, n=None):
        at = self.at
        b = self.gat.at[q, :, (1 - at.c) if arriving else at.c]
        if n is None:
            return remote(b, b, self.s6[0].at[q], self.s6[1].at[q], at.core_nb)
        b = b.at[:, :, :, n]
        return remote(b, b, self.s6l[0].at[n], self.s6l[1].at[n], at.core_nb)


def first_kernel(x_hbm, gy_hbm, wg_hbm, wu_hbm, wd_hbm,
                 xs_ref, gat, acc, rows, sx, sy, kx, ky, r2n,
                 wg, wu, wd, rd, r2, st, xin, part, r3,
                 in_sem, w_sem, x_send, x_recv, d_send, d_recv, d0_send, d0_recv, s2_send, s2_recv, s20_send, s20_recv,
                 s3_send, s3_recv, s4_send, s4_recv, s5_send, s5_recv, s6_send, s6_recv):
    at = Place()
    c, mx, my = at.c, at.x, at.y
    net = Gather(at, gat, (s4_send, s4_recv), (s5_send, s5_recv), (s6_send, s6_recv))

    def w_copies(p):
        cols = pl.ds(pl.multiple_of(p * 2 * FC, 2 * FC), 2 * FC)
        return (pltpu.make_async_copy(wg_hbm.at[:, cols], wg.at[p], w_sem.at[0, p]),
                pltpu.make_async_copy(wu_hbm.at[:, cols], wu.at[p], w_sem.at[1, p]),
                pltpu.make_async_copy(wd_hbm.at[cols, :], wd.at[p], w_sem.at[2, p]))

    in_copies = [pltpu.make_async_copy(r, rows.at[j], in_sem.at[j]) for j, r in enumerate((x_hbm, gy_hbm))]
    for cp in in_copies:
        cp.start()
    barrier = at.greet()

    @pl.loop(0, NP)
    def _(p):
        for cp in w_copies(p):
            cp.start()

    acc[...] = jnp.zeros_like(acc)
    for j in BOTH:
        in_copies[j].wait()
        for dd in range(8):
            st[dd, j] = rows[j, :, dd * DL:(dd + 1) * DL]
    pl.semaphore_wait(barrier, 15)

    def x_copy(j, k, b):
        tt, dd, _ = at.others[k]
        return remote(st.at[dd, j], xin.at[b, j], x_send.at[j, k], x_recv.at[j, k], (tt, dd))

    everyone = range(len(at.others))
    for j in BOTH:
        for k in everyone:
            x_copy(j, k, at.mine).start()
    xin[at.mine] = st[at.dp]

    def arrived(j):
        for k in everyone:
            x_copy(j, k, at.others[k][2]).wait_recv()
        xs_ref[j] = xin[:, j].astype(F32).reshape(128, DL).astype(BF)

    def d_copy(p, ab, n=None):
        s = lax.rem(p, 2)
        if n is None:
            return remote(part.at[s, 1 - c, ab], rd.at[p, ab], d_send.at[ab, p], d_recv.at[ab, p], at.core_nb)
        return remote(part.at[s, 1 - c, ab, n], rd.at[p, ab, n],
                      d0_send.at[ab, n], d0_recv.at[ab, n], at.core_nb)

    def s2_copy(p, ab, n=None):
        src = rd.at[p, 0, :, :, 1 - mx] if ab == 0 else rd.at[p, 1, :, 1 - my]
        dst = r2n.at[ab] if p is N1 else r2.at[p, ab]
        dev = at.x_nb if ab == 0 else at.y_nb
        if n is None:
            return remote(src, dst, s2_send.at[ab, p], s2_recv.at[ab, p], dev)
        return remote(src.at[n], dst.at[n], s20_send.at[ab, n], s20_recv.at[ab, n], dev)

    def s3_copy(p, ab):
        src = r2.at[p, 0, :, 1 - my] if ab == 0 else r2.at[p, 1, :, 1 - mx]
        return remote(src, r3.at[p, ab], s3_send.at[ab, p], s3_recv.at[ab, p], at.y_nb if ab == 0 else at.x_nb)

    def product(p, ab, ts):
        s = lax.rem(p, 2)
        for n in range(FC // SUB):
            cols = pl.ds(ab * FC + n * SUB, SUB)
            for t in ts:
                v = _dot(xs_ref[1], wd[p, cols, :], 1, 1) if t == 2 else _dot(xs_ref[0], (wg, wu)[t][p, :, cols], 1, 0)
                v = v.reshape(2, 2, 2, 16, SUB)
                for cc in BOTH:
                    part[s, cc, ab, t, :, :, :, sub(n)] = v[cc]

    def products(p):
        for cp in w_copies(p):
            cp.wait()
        for ab in BOTH:
            @pl.when(p >= 3)
            def _():
                d_copy(p - 2, ab).wait_send()

            @pl.when(p == 2)
            def _():
                for n in TENSORS:
                    d_copy(0, ab, n).wait_send()
            product(p, ab, TENSORS)
            d_copy(p, ab).start()

    def begin(n):
        for ab in BOTH:
            d_copy(0, ab, n).wait_recv()
            rd[0, ab, n] = rd[0, ab, n] + part[0, c, ab, n]
            s2_copy(0, ab, n).start()

    def stage2(p):
        s = lax.rem(p, 2)
        for ab in BOTH:
            d_copy(p, ab).wait_recv()
            for t in TENSORS:
                rd[p, ab, t] = rd[p, ab, t] + part[s, c, ab, t]

            @pl.when(p < N1)
            def _():
                s2_copy(p, ab).start()

        @pl.when(p >= N1)
        def _():
            for t in TENSORS:
                kx[p - N1, t] = rd[p, 0, t, :, mx]
                ky[p - N1, t] = rd[p, 1, t, my]

        @pl.when(p > N1)
        def _():
            for t in TENSORS:
                sx[p - N1 - 1, t] = rd[p, 0, t, :, 1 - mx]
                sy[p - N1 - 1, t] = rd[p, 1, t, 1 - my]

    def stage3(p):
        for ab in BOTH:
            @pl.when(p == 0)
            def _():
                for n in TENSORS:
                    s2_copy(0, ab, n).wait_recv()

            @pl.when(p > 0)
            def _():
                s2_copy(p, ab).wait_recv()
            for t in TENSORS:
                r2[p, ab, t] = r2[p, ab, t] + (rd[p, 0, t, :, mx] if ab == 0 else rd[p, 1, t, my])
            s3_copy(p, ab).start()

    def stage4(p):
        for ab in BOTH:
            s3_copy(p, ab).wait_recv()
            keep = my if ab == 0 else mx
            vals = silu_parts(*(r3[p, ab, t] + r2[p, ab, t, keep] for t in TENSORS))
            for t in TENSORS:
                gat[p, ab, c, my, mx, t] = vals[t]
            net.first(p, ab, False).start()

    def stage5(p):
        for ab in BOTH:
            net.first(p, ab, True).wait_recv()
            net.second(p, ab, False).start()

        @pl.when(p == N1 - 1)
        def _():
            for ab in BOTH:
                s2_copy(N1, ab).start()

    def stage6(p):
        for ab in BOTH:
            net.second(p, ab, True).wait_recv()
        net.third(p, False).start()

    def stage7(p):
        net.third(p, True).wait_recv()
        y_part(acc, gat, lambda q, lo, w: wd[q, lo:lo + w, :], p, 0, FC)
        dx_part(acc, gat, *(lambda q, lo, w, r=r: r[q, :, lo:lo + w] for r in (wg, wu)), p, 0, FC)

    arrived(0)
    for cp in w_copies(0):
        cp.wait()
    for n in TENSORS:
        if n == 2:
            arrived(1)
        for ab in BOTH:
            product(0, ab, (n,))
            d_copy(0, ab, n).start()
        if n > 0:
            begin(n - 1)
    begin(2)

    @pl.loop(0, N1 + 5)
    def _(i):
        pl.when((i >= 1) & (i < NP))(lambda: stage2(i))
        pl.when((i >= 1) & (i < N1 + 1))(lambda: stage3(i - 1))
        pl.when((i >= 2) & (i < N1 + 2))(lambda: stage4(i - 2))
        pl.when((i >= 3) & (i < N1 + 3))(lambda: stage5(i - 3))
        pl.when((i >= 4) & (i < N1 + 4))(lambda: stage6(i - 4))
        pl.when(i < NP - 1)(lambda: products(i + 1))
        pl.when(i >= 5)(lambda: stage7(i - 5))

    @pl.loop(0, N1)
    def _(p):
        for ab in BOTH:
            s3_copy(p, ab).wait_send()
            net.first(p, ab, False).wait_send()
            net.second(p, ab, False).wait_send()
        net.third(p, False).wait_send()

    @pl.loop(1, N1)
    def _(p):
        for ab in BOTH:
            s2_copy(p, ab).wait_send()
    for n in TENSORS:
        for ab in BOTH:
            s2_copy(0, ab, n).wait_send()
    for p in (NP - 2, NP - 1):
        for ab in BOTH:
            d_copy(p, ab).wait_send()

    for k in everyone:
        for j in BOTH:
            x_copy(j, k, at.mine).wait_send()
    for ab in BOTH:
        s2_copy(N1, ab).wait_send()
        s2_copy(N1, ab).wait_recv()


def second_kernel(wg_hbm, wu_hbm, wd_hbm, xs_ref, acc_in, rows, rx, ry, kx, ky, r2n,
                  y_ref, gx_ref, lwg, lwu, lwd,
                  gat, wg, wu, wd, r2b, r3, acc, fin,
                  w_sem, s3_send, s3_recv, s4_send, s4_recv, s5_send, s5_recv, s5l_send, s5l_recv,
                  s6_send, s6_recv, s6l_send, s6l_recv, o_send, o_recv):
    at = Place()
    c, mx, my = at.c, at.x, at.y
    net = Gather(at, gat, (s4_send, s4_recv), (s5_send, s5_recv), (s6_send, s6_recv),
                 (s5l_send, s5l_recv), (s6l_send, s6l_recv))
    barrier = pltpu.get_barrier_semaphore()
    for nb in (at.x_nb, at.y_nb, at.core_nb, (1 - at.tp, at.dp)):
        pl.semaphore_signal(barrier, inc=1, device_id=nb, device_id_type=MESH)
    cols = pl.ds(N1 * 2 * FC, NB * 2 * FC)
    w_copies = (pltpu.make_async_copy(wg_hbm.at[:, cols], wg, w_sem.at[0]),
                pltpu.make_async_copy(wu_hbm.at[:, cols], wu, w_sem.at[1]),
                pltpu.make_async_copy(wd_hbm.at[cols, :], wd, w_sem.at[2]))
    for cp in w_copies:
        cp.start()

    def s3_copy(q, ab):
        src = r2b.at[q, 0, :, 1 - my] if ab == 0 else r2b.at[q, 1, :, 1 - mx]
        return remote(src, r3.at[q, ab], s3_send.at[ab, q], s3_recv.at[ab, q], at.y_nb if ab == 0 else at.x_nb)

    def halves(q):
        for ab in BOTH:
            for t in TENSORS:
                got = r2n[ab, t] if q == 0 else (rx, ry)[ab][q - 1, t]
                r2b[q, ab, t] = got + (kx, ky)[ab][q, t]

    def send_quarters(q):
        for ab in BOTH:
            s3_copy(q, ab).start()

    def activate(q):
        for ab in BOTH:
            s3_copy(q, ab).wait_recv()
            keep = my if ab == 0 else mx
            vals = silu_parts(*(r3[q, ab, t] + r2b[q, ab, t, keep] for t in TENSORS))
            for t in TENSORS:
                gat[q, ab, c, my, mx, t] = vals[t]
            net.first(q, ab, False).start()

    def spread(q):
        for ab in BOTH:
            net.first(q, ab, True).wait_recv()
            if q < NB - 1:
                net.second(q, ab, False).start()
            else:
                for n in TENSORS:
                    net.second(q, ab, False, n).start()

    def cross(q):
        for ab in BOTH:
            net.second(q, ab, True).wait_recv()
        net.third(q, False).start()

    def down(q, lo, w):
        return wd[q * 2 * FC + lo:q * 2 * FC + lo + w, :]

    def gate(q, lo, w):
        return wg[:, q * 2 * FC + lo:q * 2 * FC + lo + w]

    def up(q, lo, w):
        return wu[:, q * 2 * FC + lo:q * 2 * FC + lo + w]

    halves(0)
    pl.semaphore_wait(barrier, 4)
    send_quarters(0)
    for q in range(1, NB):
        halves(q)
        if q < NB - 1:
            send_quarters(q)
    acc[...] = acc_in[...]
    for q in range(NB):
        activate(q)
        if q == 0:
            send_quarters(NB - 1)
        else:
            spread(q - 1)
    spread(NB - 1)
    for cp in w_copies:
        cp.wait()
    q = NB - 1

    everyone = range(len(at.others))

    def o_copy(j, k, slot):
        tt, dd, b = at.others[k]
        return remote(acc.at[j, b], fin.at[j, slot], o_send.at[j, k], o_recv.at[j, k], (tt, dd))

    def send_out(j):
        for k in everyone:
            o_copy(j, k, at.me).start()
        fin[j, at.me] = acc[j, at.mine]

    def finish(n):
        net.third(q, True, n).wait_recv()
        if n == 0:
            y_part(acc, gat, down, q, 0, FC)
            send_out(0)
        else:
            dx_part(acc, gat, gate, up, q, 0, FC, (n,))
        if n == 2:
            send_out(1)

    def late(k):
        lo = pl.ds(pl.multiple_of(k * FC, FC), FC)
        h, da, db = (gat[k // 2, k % 2, :, :, :, t].reshape(128, FC) for t in TENSORS)
        lwg[:, lo] = _dot(xs_ref[0], da, 0, 0)
        lwu[:, lo] = _dot(xs_ref[0], db, 0, 0)
        lwd[lo, :] = _dot(h, xs_ref[1], 0, 0)

    def cross_last(n):
        for ab in BOTH:
            net.second(q, ab, True, n).wait_recv()
        net.third(q, False, n).start()

    cross(0)
    for p in range(1, NB - 1):
        net.third(p - 1, True).wait_recv()
        y_part(acc, gat, down, p - 1, 0, FC)
        dx_part(acc, gat, gate, up, p - 1, 0, FC)
        cross(p)
    late(0)
    cross_last(0)
    late(1)
    cross_last(1)
    net.third(q - 1, True).wait_recv()
    y_part(acc, gat, down, q - 1, 0, FC)
    cross_last(2)
    finish(0)
    dx_part(acc, gat, gate, up, q - 1, 0, FC)
    finish(1)
    finish(2)

    pl.loop(2, 2 * NB)(late)

    for q in range(NB):
        for ab in BOTH:
            s3_copy(q, ab).wait_send()
            net.first(q, ab, False).wait_send()
            if q < NB - 1:
                net.second(q, ab, False).wait_send()
            else:
                for n in TENSORS:
                    net.second(q, ab, False, n).wait_send()
        if q < NB - 1:
            net.third(q, False).wait_send()
        else:
            for n in TENSORS:
                net.third(q, False, n).wait_send()

    for j, out in enumerate((y_ref, gx_ref)):
        for k in everyone:
            tt, dd, _ = at.others[k]
            o_copy(j, k, tt * 8 + dd).wait_recv()
        for dd in range(8):
            cols = slice(dd * DL, (dd + 1) * DL)
            out[:, cols] = (rows[j, :, cols].astype(F32) + (fin[j, dd] + fin[j, 8 + dd])).astype(BF)

    for k in everyone:
        for j in BOTH:
            o_copy(j, k, at.me).wait_send()


def early_grads(xs_ref, g_ref, dwg_ref, dwu_ref, dwd_ref):
    q, ab = pl.program_id(0) // 2, lax.rem(pl.program_id(0), 2)
    h, da, db = (g_ref[q, ab, :, :, :, t].reshape(128, FC) for t in TENSORS)
    dwg_ref[...] = _dot(xs_ref[0], da, 0, 0)
    dwu_ref[...] = _dot(xs_ref[0], db, 0, 0)
    dwd_ref[...] = _dot(h, xs_ref[1], 0, 0)


def late_grads(y_ref, gx_ref, lwg, lwu, lwd, a_ref, b_ref, c_ref, yo_ref, gxo_ref, dwg_ref, dwu_ref, dwd_ref, sem, row_sem):
    copies = [pltpu.make_async_copy(y_ref, yo_ref, row_sem.at[0]), pltpu.make_async_copy(gx_ref, gxo_ref, row_sem.at[1])]
    for k in range(NB):
        src = pl.ds(k * 2 * FC, 2 * FC)
        dst = pl.ds((N1 + k) * 2 * FC, 2 * FC)
        copies += [pltpu.make_async_copy(lwg.at[:, src], dwg_ref.at[:, dst], sem.at[0, k]),
                   pltpu.make_async_copy(lwu.at[:, src], dwu_ref.at[:, dst], sem.at[1, k]),
                   pltpu.make_async_copy(lwd.at[src, :], dwd_ref.at[dst, :], sem.at[2, k])]
    for cp in copies:
        cp.start()
    for cp in copies:
        cp.wait()


def local_step(x_loc, wg_loc, wu_loc, wd_loc, gy_loc):
    vm = pl.BlockSpec(memory_space=pltpu.VMEM)
    hb = pl.BlockSpec(memory_space=pl.ANY)
    hbm = pl.BlockSpec(memory_space=pltpu.HBM)
    dma = pltpu.SemaphoreType.DMA
    row = jax.ShapeDtypeStruct((8, D), BF)
    kib = 1024
    half = (3, 2, 16, FC)
    xs, gat1, acc, rows, sx, sy, kx, ky, r2n = pl.pallas_call(
        first_kernel,
        out_shape=(pltpu.VMEM((2, 128, DL), BF), pltpu.VMEM((N1, 2, 2, 2, 2, 3, 16, FC), BF),
                   pltpu.VMEM((2, 16, 8, DL), F32), pltpu.VMEM((2, 8, D), BF),
                   pltpu.VMEM((NB - 1,) + half, F32), pltpu.VMEM((NB - 1,) + half, F32),
                   pltpu.VMEM((NB,) + half, F32), pltpu.VMEM((NB,) + half, F32), pltpu.VMEM((2,) + half, F32)),
        in_specs=[hbm] * 5,
        out_specs=(vm,) * 9,
        scratch_shapes=[
            pltpu.VMEM((NP, DL, 2 * FC), BF),
            pltpu.VMEM((NP, DL, 2 * FC), BF),
            pltpu.VMEM((NP, 2 * FC, DL), BF),
            pltpu.VMEM((NP, 2, 3, 2, 2, 16, FC), F32),
            pltpu.VMEM((N1, 2) + half, F32),
            pltpu.VMEM((8, 2, 8, DL), BF),
            pltpu.VMEM((16, 2, 8, DL), BF),
            pltpu.VMEM((2, 2, 2, 3, 2, 2, 16, FC), F32),
            pltpu.VMEM((N1, 2, 3, 16, FC), F32),
            dma((2,)), dma((3, NP)), dma((2, 16)), dma((2, 16)),
            dma((2, NP)), dma((2, NP)), dma((2, 3)), dma((2, 3)),
            dma((2, NP)), dma((2, NP)), dma((2, 3)), dma((2, 3)),
            dma((2, N1)), dma((2, N1)), dma((2, N1)), dma((2, N1)),
            dma((2, N1)), dma((2, N1)), dma((N1,)), dma((N1,)),
        ],
        compiler_params=pltpu.CompilerParams(
            collective_id=0, has_side_effects=True, vmem_limit_bytes=49000 * kib),
        name="mlp_first",
    )(x_loc, gy_loc, wg_loc, wu_loc, wd_loc)

    rx = lax.ppermute(sx, "dp", [(i, i + 2 if i % 4 < 2 else i - 2) for i in range(8)])
    ry = lax.ppermute(sy, "dp", [(i, (i + 4) % 8) for i in range(8)])

    full = (jax.ShapeDtypeStruct((DL, FF_LOC), F32), jax.ShapeDtypeStruct((DL, FF_LOC), F32),
            jax.ShapeDtypeStruct((FF_LOC, DL), F32))

    dwg, dwu, dwd = pl.pallas_call(
        early_grads,
        grid=(2 * N1,),
        out_shape=full,
        in_specs=[vm, vm],
        out_specs=(pl.BlockSpec((DL, FC), lambda k: (0, k)), pl.BlockSpec((DL, FC), lambda k: (0, k)),
                   pl.BlockSpec((FC, DL), lambda k: (k, 0))),
        cost_estimate=pl.CostEstimate(flops=12 * N1 * 128 * DL * FC, bytes_accessed=24 * N1 * DL * FC,
                                      transcendentals=0),
        compiler_params=pltpu.CompilerParams(dimension_semantics=("arbitrary",), vmem_limit_bytes=9000 * kib),
        name="mlp_early_grads",
    )(xs, gat1)

    y_rows, gx_rows, lwg, lwu, lwd = pl.pallas_call(
        second_kernel,
        out_shape=(pltpu.VMEM((8, D), BF), pltpu.VMEM((8, D), BF), pltpu.VMEM((DL, NB * 2 * FC), F32),
                   pltpu.VMEM((DL, NB * 2 * FC), F32), pltpu.VMEM((NB * 2 * FC, DL), F32)),
        in_specs=[hbm] * 3 + [vm] * 8,
        out_specs=(vm,) * 5,
        scratch_shapes=[
            pltpu.VMEM((NB, 2, 2, 2, 2, 3, 16, FC), BF),
            pltpu.VMEM((DL, NB * 2 * FC), BF),
            pltpu.VMEM((DL, NB * 2 * FC), BF),
            pltpu.VMEM((NB * 2 * FC, DL), BF),
            pltpu.VMEM((NB, 2) + half, F32),
            pltpu.VMEM((NB, 2, 3, 16, FC), F32),
            pltpu.VMEM((2, 16, 8, DL), F32),
            pltpu.VMEM((2, 16, 8, DL), F32),
            dma((3,)), dma((2, NB)), dma((2, NB)), dma((2, NB)), dma((2, NB)),
            dma((2, NB)), dma((2, NB)), dma((2, 3)), dma((2, 3)),
            dma((NB,)), dma((NB,)), dma((3,)), dma((3,)),
            dma((2, 16)), dma((2, 16)),
        ],
        compiler_params=pltpu.CompilerParams(
            collective_id=1, has_side_effects=True, vmem_limit_bytes=30000 * kib),
        name="mlp_second",
    )(wg_loc, wu_loc, wd_loc, xs, acc, rows, rx, ry, kx, ky, r2n)

    return pl.pallas_call(
        late_grads,
        out_shape=(row, row) + full,
        in_specs=[vm] * 5 + [hbm] * 3,
        out_specs=(hbm,) * 5,
        input_output_aliases={5: 2, 6: 3, 7: 4},
        scratch_shapes=[dma((3, NB)), dma((2,))],
        compiler_params=pltpu.CompilerParams(vmem_limit_bytes=30000 * kib),
        name="mlp_late_grads",
    )(y_rows, gx_rows, lwg, lwu, lwd, dwg, dwu, dwd)


def solution(mesh):
    row_spec = P(("dp", "tp"), None)
    up_spec = P("dp", "tp")
    down_spec = P("tp", "dp")
    return jax.shard_map(local_step, mesh=mesh,
                         in_specs=(row_spec, up_spec, up_spec, down_spec, row_spec),
                         out_specs=(row_spec, row_spec, up_spec, up_spec, down_spec),
                         check_vma=False)
```

```python
import itertools

import jax
import jax.numpy as jnp
from jax import lax
from jax.experimental import pallas as pl
from jax.experimental.pallas import tpu as pltpu
from jax.sharding import PartitionSpec as P

MESH = pl.DeviceIdType.MESH
BF = jnp.bfloat16
F32 = jnp.float32

BOTH = range(2)
TENSORS = range(3)
D = 3072
FF_LOC = 12288
DL = 384
NP = 8
N1 = 5
NB = NP - N1
FC = FF_LOC // (2 * NP)
NS = 3
SUB = FC // NS


def _dot(a, b, ca, cb):
    return lax.dot_general(a, b, (((ca,), (cb,)), ((), ())), preferred_element_type=F32)


def remote(src, dst, send, recv, dev):
    return pltpu.make_async_remote_copy(src_ref=src, dst_ref=dst, send_sem=send, recv_sem=recv,
                                        device_id=dev, device_id_type=MESH)


def sub(n):
    return pl.ds(n * SUB, SUB)


def block(tt, cc, yy, xx):
    return (cc * 4 + yy * 2 + xx) * 2 + tt


class Place:
    def __init__(self):
        tp, dp = lax.axis_index("tp"), lax.axis_index("dp")
        c, x, y = lax.rem(dp, 2), lax.rem(dp // 2, 2), dp // 4
        self.tp, self.dp, self.c, self.x, self.y = tp, dp, c, x, y
        self.me = tp * 8 + dp
        self.core_nb = (tp, y * 4 + x * 2 + (1 - c))
        self.x_nb = (tp, y * 4 + (1 - x) * 2 + c)
        self.y_nb = (tp, (1 - y) * 4 + x * 2 + c)
        self.z_nb = (1 - tp, dp)
        self.mine = block(tp, c, y, x)
        flips = sorted(itertools.product(BOTH, repeat=4), key=sum, reverse=True)[:-1]
        self.others = []
        for ft, fy, fx, fc in flips:
            tt, yy, xx, cc = (1 - v if f else v for v, f in zip((tp, y, x, c), (ft, fy, fx, fc)))
            self.others.append((tt, yy * 4 + xx * 2 + cc, block(tt, cc, yy, xx)))
        self.plane = [k for k, f in enumerate(flips) if not f[0]]

    def greet(self):
        barrier = pltpu.get_barrier_semaphore()
        for tt, dd, _ in self.others:
            pl.semaphore_signal(barrier, inc=1, device_id=(tt, dd), device_id_type=MESH)
        return barrier


def silu_parts(a, b, g):
    s = jax.nn.sigmoid(a)
    silu = a * s
    return ((silu * b).astype(BF), (g * b * (s * (1.0 + a * (1.0 - s)))).astype(BF), (g * silu).astype(BF))


def accumulate(acc, j, v):
    acc[j] = acc[j] + v.reshape(16, 8, DL)


def y_part(acc, gat, wd, q, lo, w):
    v = None
    for ab in BOTH:
        h = gat[q, ab, :, :, :, 0, :, lo:lo + w].reshape(128, w)
        d = _dot(h, wd(q, ab * FC + lo, w), 1, 0)
        v = d if v is None else v + d
    accumulate(acc, 0, v)


def dx_part(acc, gat, wg, wu, q, lo, w, ts=(1, 2)):
    v = None
    for ab in BOTH:
        for t, wt in ((t, (wg, wu)[t - 1]) for t in ts):
            z = gat[q, ab, :, :, :, t, :, lo:lo + w].reshape(128, w)
            d = _dot(z, wt(q, ab * FC + lo, w), 1, 1)
            v = d if v is None else v + d
    accumulate(acc, 1, v)


class Gather:
    def __init__(self, at, gat, s4, s5, s6, s5l=None, s6l=None):
        self.at, self.gat, self.s4, self.s5, self.s6, self.s5l, self.s6l = at, gat, s4, s5, s6, s5l, s6l

    def first(self, q, ab, arriving):
        at = self.at
        y0 = (1 - at.y) if arriving else at.y
        x1 = (1 - at.x) if arriving else at.x
        b = self.gat.at[q, 0, at.c, y0, at.x] if ab == 0 else self.gat.at[q, 1, at.c, at.y, x1]
        return remote(b, b, self.s4[0].at[ab, q], self.s4[1].at[ab, q], at.y_nb if ab == 0 else at.x_nb)

    def second(self, q, ab, arriving, n=None):
        at = self.at
        x0 = (1 - at.x) if arriving else at.x
        y1 = (1 - at.y) if arriving else at.y
        b = self.gat.at[q, 0, at.c, :, x0] if ab == 0 else self.gat.at[q, 1, at.c, y1]
        dev = at.x_nb if ab == 0 else at.y_nb
        if n is None:
            return remote(b, b, self.s5[0].at[ab, q], self.s5[1].at[ab, q], dev)
        b = b.at[:, n]
        return remote(b, b, self.s5l[0].at[ab, n], self.s5l[1].at[ab, n], dev)

    def third(self, q, arriving, n=None):
        at = self.at
        b = self.gat.at[q, :, (1 - at.c) if arriving else at.c]
        if n is None:
            return remote(b, b, self.s6[0].at[q], self.s6[1].at[q], at.core_nb)
        b = b.at[:, :, :, n]
        return remote(b, b, self.s6l[0].at[n], self.s6l[1].at[n], at.core_nb)


def first_kernel(x_hbm, gy_hbm, wg_hbm, wu_hbm, wd_hbm,
                 xs_ref, xin, gat, acc, rows, sx, sy, kx, ky, r2n,
                 wg, wu, wd, rd, r2, st, part, r3,
                 in_sem, w_sem, x_send, x_recv, d_send, d_recv, d0_send, d0_recv, s2_send, s2_recv, s20_send, s20_recv,
                 s3_send, s3_recv, s4_send, s4_recv, s5_send, s5_recv, s6_send, s6_recv):
    at = Place()
    c, mx, my = at.c, at.x, at.y
    net = Gather(at, gat, (s4_send, s4_recv), (s5_send, s5_recv), (s6_send, s6_recv))

    def w_copies(p):
        cols = pl.ds(pl.multiple_of(p * 2 * FC, 2 * FC), 2 * FC)
        return (pltpu.make_async_copy(wg_hbm.at[:, cols], wg.at[p], w_sem.at[0, p]),
                pltpu.make_async_copy(wu_hbm.at[:, cols], wu.at[p], w_sem.at[1, p]),
                pltpu.make_async_copy(wd_hbm.at[cols, :], wd.at[p], w_sem.at[2, p]))

    in_copies = [pltpu.make_async_copy(r, rows.at[j], in_sem.at[j]) for j, r in enumerate((x_hbm, gy_hbm))]
    for cp in in_copies:
        cp.start()
    barrier = at.greet()

    @pl.loop(0, NP)
    def _(p):
        for cp in w_copies(p):
            cp.start()

    acc[...] = jnp.zeros_like(acc)
    for j in BOTH:
        in_copies[j].wait()
        for dd in range(8):
            st[dd, j] = rows[j, :, dd * DL:(dd + 1) * DL]
    pl.semaphore_wait(barrier, 15)

    def x_copy(k, b):
        tt, dd, _ = at.others[k]
        return remote(st.at[dd], xin.at[b], x_send.at[k], x_recv.at[k], (tt, dd))

    everyone = range(len(at.others))
    for k in everyone:
        x_copy(k, at.mine).start()
    xin[at.mine] = st[at.dp]
    for k in everyone:
        x_copy(k, at.others[k][2]).wait_recv()

    for j in BOTH:
        xs_ref[j] = xin[:, j].astype(F32).reshape(128, DL).astype(BF)

    def d_copy(p, ab, n=None):
        s = lax.rem(p, 2)
        if n is None:
            return remote(part.at[s, 1 - c, ab], rd.at[p, ab], d_send.at[ab, p], d_recv.at[ab, p], at.core_nb)
        return remote(part.at[s, 1 - c, ab, :, :, :, :, sub(n)], rd.at[p, ab, :, :, :, :, sub(n)],
                      d0_send.at[ab, n], d0_recv.at[ab, n], at.core_nb)

    def s2_copy(p, ab, n=None):
        src = rd.at[p, 0, :, :, 1 - mx] if ab == 0 else rd.at[p, 1, :, 1 - my]
        dst = r2n.at[ab] if p is N1 else r2.at[p, ab]
        dev = at.x_nb if ab == 0 else at.y_nb
        if n is None:
            return remote(src, dst, s2_send.at[ab, p], s2_recv.at[ab, p], dev)
        return remote(src.at[:, :, :, sub(n)], dst.at[:, :, :, sub(n)], s20_send.at[ab, n], s20_recv.at[ab, n], dev)

    def s3_copy(p, ab):
        src = r2.at[p, 0, :, 1 - my] if ab == 0 else r2.at[p, 1, :, 1 - mx]
        return remote(src, r3.at[p, ab], s3_send.at[ab, p], s3_recv.at[ab, p], at.y_nb if ab == 0 else at.x_nb)

    def product(p, ab, n):
        s = lax.rem(p, 2)
        cols = pl.ds(ab * FC + n * SUB, SUB)
        vals = (_dot(xs_ref[0], wg[p, :, cols], 1, 0),
                _dot(xs_ref[0], wu[p, :, cols], 1, 0),
                _dot(xs_ref[1], wd[p, cols, :], 1, 1))
        for t in TENSORS:
            v = vals[t].reshape(2, 2, 2, 16, SUB)
            for cc in BOTH:
                part[s, cc, ab, t, :, :, :, sub(n)] = v[cc]

    def products(p):
        for cp in w_copies(p):
            cp.wait()
        for ab in BOTH:
            @pl.when(p >= 3)
            def _():
                d_copy(p - 2, ab).wait_send()

            @pl.when(p == 2)
            def _():
                for n in range(NS):
                    d_copy(0, ab, n).wait_send()
            for n in range(NS):
                product(p, ab, n)
            d_copy(p, ab).start()

    def stage2(p):
        s = lax.rem(p, 2)
        for ab in BOTH:
            d_copy(p, ab).wait_recv()
            for t in TENSORS:
                rd[p, ab, t] = rd[p, ab, t] + part[s, c, ab, t]

            @pl.when(p < N1)
            def _():
                s2_copy(p, ab).start()

        @pl.when(p >= N1)
        def _():
            for t in TENSORS:
                kx[p - N1, t] = rd[p, 0, t, :, mx]
                ky[p - N1, t] = rd[p, 1, t, my]

        @pl.when(p > N1)
        def _():
            for t in TENSORS:
                sx[p - N1 - 1, t] = rd[p, 0, t, :, 1 - mx]
                sy[p - N1 - 1, t] = rd[p, 1, t, 1 - my]

    def stage3(p):
        for ab in BOTH:
            @pl.when(p == 0)
            def _():
                for n in range(NS):
                    s2_copy(0, ab, n).wait_recv()

            @pl.when(p > 0)
            def _():
                s2_copy(p, ab).wait_recv()
            for t in TENSORS:
                r2[p, ab, t] = r2[p, ab, t] + (rd[p, 0, t, :, mx] if ab == 0 else rd[p, 1, t, my])
            s3_copy(p, ab).start()

    def stage4(p):
        for ab in BOTH:
            s3_copy(p, ab).wait_recv()
            keep = my if ab == 0 else mx
            vals = silu_parts(*(r3[p, ab, t] + r2[p, ab, t, keep] for t in TENSORS))
            for t in TENSORS:
                gat[p, ab, c, my, mx, t] = vals[t]
            net.first(p, ab, False).start()

    def stage5(p):
        for ab in BOTH:
            net.first(p, ab, True).wait_recv()
            net.second(p, ab, False).start()

        @pl.when(p == N1 - 1)
        def _():
            for ab in BOTH:
                s2_copy(N1, ab).start()

    def stage6(p):
        for ab in BOTH:
            net.second(p, ab, True).wait_recv()
        net.third(p, False).start()

    def stage7(p):
        net.third(p, True).wait_recv()
        y_part(acc, gat, lambda q, lo, w: wd[q, lo:lo + w, :], p, 0, FC)
        dx_part(acc, gat, *(lambda q, lo, w, r=r: r[q, :, lo:lo + w] for r in (wg, wu)), p, 0, FC)

    for cp in w_copies(0):
        cp.wait()
    for n in range(NS):
        for ab in BOTH:
            product(0, ab, n)
            d_copy(0, ab, n).start()
    for n in range(NS):
        for ab in BOTH:
            d_copy(0, ab, n).wait_recv()
            rd[0, ab, :, :, :, :, sub(n)] = rd[0, ab, :, :, :, :, sub(n)] + part[0, c, ab, :, :, :, :, sub(n)]
            s2_copy(0, ab, n).start()

    @pl.loop(0, N1 + 5)
    def _(i):
        pl.when((i >= 1) & (i < NP))(lambda: stage2(i))
        pl.when((i >= 1) & (i < N1 + 1))(lambda: stage3(i - 1))
        pl.when((i >= 2) & (i < N1 + 2))(lambda: stage4(i - 2))
        pl.when((i >= 3) & (i < N1 + 3))(lambda: stage5(i - 3))
        pl.when((i >= 4) & (i < N1 + 4))(lambda: stage6(i - 4))
        pl.when(i < NP - 1)(lambda: products(i + 1))
        pl.when(i >= 5)(lambda: stage7(i - 5))

    @pl.loop(0, N1)
    def _(p):
        for ab in BOTH:
            s3_copy(p, ab).wait_send()
            net.first(p, ab, False).wait_send()
            net.second(p, ab, False).wait_send()
        net.third(p, False).wait_send()

    @pl.loop(1, N1)
    def _(p):
        for ab in BOTH:
            s2_copy(p, ab).wait_send()
    for n in range(NS):
        for ab in BOTH:
            s2_copy(0, ab, n).wait_send()
    for p in (NP - 2, NP - 1):
        for ab in BOTH:
            d_copy(p, ab).wait_send()

    for k in everyone:
        x_copy(k, at.mine).wait_send()
    for ab in BOTH:
        s2_copy(N1, ab).wait_send()
        s2_copy(N1, ab).wait_recv()


def second_kernel(wg_hbm, wu_hbm, wd_hbm, xs_ref, xin, acc_in, rows, rx, ry, kx, ky, r2n,
                  y_ref, gx_ref, lwg, lwu, lwd,
                  gat, wg, wu, wd, r2b, r3, acc, fin, rz, ob, oy,
                  w_sem, s3_send, s3_recv, s4_send, s4_recv, s5_send, s5_recv, s5l_send, s5l_recv,
                  s6_send, s6_recv, s6l_send, s6l_recv, o_send, o_recv,
                  z_send, z_recv, p_send, p_recv):
    at = Place()
    c, mx, my = at.c, at.x, at.y
    net = Gather(at, gat, (s4_send, s4_recv), (s5_send, s5_recv), (s6_send, s6_recv),
                 (s5l_send, s5l_recv), (s6l_send, s6l_recv))
    barrier = pltpu.get_barrier_semaphore()
    for nb in (at.x_nb, at.y_nb, at.core_nb, at.z_nb):
        pl.semaphore_signal(barrier, inc=1, device_id=nb, device_id_type=MESH)
    cols = pl.ds(N1 * 2 * FC, NB * 2 * FC)
    w_copies = (pltpu.make_async_copy(wg_hbm.at[:, cols], wg, w_sem.at[0]),
                pltpu.make_async_copy(wu_hbm.at[:, cols], wu, w_sem.at[1]),
                pltpu.make_async_copy(wd_hbm.at[cols, :], wd, w_sem.at[2]))
    for cp in w_copies:
        cp.start()

    def s3_copy(q, ab):
        src = r2b.at[q, 0, :, 1 - my] if ab == 0 else r2b.at[q, 1, :, 1 - mx]
        return remote(src, r3.at[q, ab], s3_send.at[ab, q], s3_recv.at[ab, q], at.y_nb if ab == 0 else at.x_nb)

    def halves(q):
        for ab in BOTH:
            for t in TENSORS:
                got = r2n[ab, t] if q == 0 else (rx, ry)[ab][q - 1, t]
                r2b[q, ab, t] = got + (kx, ky)[ab][q, t]

    def send_quarters(q):
        for ab in BOTH:
            s3_copy(q, ab).start()

    def activate(q):
        for ab in BOTH:
            s3_copy(q, ab).wait_recv()
            keep = my if ab == 0 else mx
            vals = silu_parts(*(r3[q, ab, t] + r2b[q, ab, t, keep] for t in TENSORS))
            for t in TENSORS:
                gat[q, ab, c, my, mx, t] = vals[t]
            net.first(q, ab, False).start()

    def spread(q):
        for ab in BOTH:
            net.first(q, ab, True).wait_recv()
            if q < NB - 1:
                net.second(q, ab, False).start()
            else:
                for n in TENSORS:
                    net.second(q, ab, False, n).start()

    def cross(q):
        for ab in BOTH:
            net.second(q, ab, True).wait_recv()
        net.third(q, False).start()

    def down(q, lo, w):
        return wd[q * 2 * FC + lo:q * 2 * FC + lo + w, :]

    def gate(q, lo, w):
        return wg[:, q * 2 * FC + lo:q * 2 * FC + lo + w]

    def up(q, lo, w):
        return wu[:, q * 2 * FC + lo:q * 2 * FC + lo + w]

    halves(0)
    pl.semaphore_wait(barrier, 4)
    send_quarters(0)
    for q in range(1, NB):
        halves(q)
        if q < NB - 1:
            send_quarters(q)
    acc[...] = acc_in[...]
    for q in range(NB):
        activate(q)
        if q == 0:
            send_quarters(NB - 1)
        else:
            spread(q - 1)
    spread(NB - 1)
    for cp in w_copies:
        cp.wait()
    q = NB - 1

    everyone = range(len(at.others))

    def o_copy(k, slot):
        tt, dd, b = at.others[k]
        return remote(acc.at[1, b], fin.at[slot], o_send.at[k], o_recv.at[k], (tt, dd))

    halves_y = acc.reshape(2, 8, 2, 8, DL)
    z_copy = remote(halves_y.at[0, :, 1 - at.tp], rz, z_send, z_recv, at.z_nb)

    def p_copy(k, slot):
        tt, dd, b = at.others[k]
        return remote(ob.at[b // 2], oy.at[slot], p_send.at[k], p_recv.at[k], (tt, dd))

    def y_rows_out():
        z_copy.wait_recv()
        for b in range(8):
            ob[b] = (xin[2 * b + at.tp, 0].astype(F32) + (halves_y[0, b, at.tp] + rz[b])).astype(BF)
        for k in at.plane:
            p_copy(k, at.dp).start()
        oy[at.dp] = ob[at.mine // 2]

    def finish(n):
        net.third(q, True, n).wait_recv()
        if n == 0:
            y_part(acc, gat, down, q, 0, FC)
            z_copy.start()
        else:
            dx_part(acc, gat, gate, up, q, 0, FC, (n,))
        if n == 2:
            for k in everyone:
                o_copy(k, at.me).start()
            fin[at.me] = acc[1, at.mine]

    def late(k):
        lo = pl.ds(pl.multiple_of(k * FC, FC), FC)
        h, da, db = (gat[k // 2, k % 2, :, :, :, t].reshape(128, FC) for t in TENSORS)
        lwg[:, lo] = _dot(xs_ref[0], da, 0, 0)
        lwu[:, lo] = _dot(xs_ref[0], db, 0, 0)
        lwd[lo, :] = _dot(h, xs_ref[1], 0, 0)

    def cross_last(n):
        for ab in BOTH:
            net.second(q, ab, True, n).wait_recv()
        net.third(q, False, n).start()

    cross(0)
    for p in range(1, NB - 1):
        net.third(p - 1, True).wait_recv()
        y_part(acc, gat, down, p - 1, 0, FC)
        dx_part(acc, gat, gate, up, p - 1, 0, FC)
        cross(p)
    late(0)
    cross_last(0)
    late(1)
    cross_last(1)
    net.third(q - 1, True).wait_recv()
    y_part(acc, gat, down, q - 1, 0, FC)
    cross_last(2)
    finish(0)
    dx_part(acc, gat, gate, up, q - 1, 0, FC)
    finish(1)
    y_rows_out()
    finish(2)

    pl.loop(2, 2 * NB)(late)

    for q in range(NB):
        for ab in BOTH:
            s3_copy(q, ab).wait_send()
            net.first(q, ab, False).wait_send()
            if q < NB - 1:
                net.second(q, ab, False).wait_send()
            else:
                for n in TENSORS:
                    net.second(q, ab, False, n).wait_send()
        if q < NB - 1:
            net.third(q, False).wait_send()
        else:
            for n in TENSORS:
                net.third(q, False, n).wait_send()

    def arrival(k):
        tt, dd, _ = at.others[k]
        return o_copy(k, tt * 8 + dd), p_copy(k, dd)

    for k in at.plane:
        arrival(k)[1].wait_recv()
    for k in everyone:
        arrival(k)[0].wait_recv()
    for dd in range(8):
        cols = slice(dd * DL, (dd + 1) * DL)
        y_ref[:, cols] = oy[dd]
        gx_ref[:, cols] = (rows[1, :, cols].astype(F32) + (fin[dd] + fin[8 + dd])).astype(BF)
    z_copy.wait_send()
    for k in at.plane:
        p_copy(k, at.dp).wait_send()
    for k in everyone:
        o_copy(k, at.me).wait_send()


def early_grads(xs_ref, g_ref, dwg_ref, dwu_ref, dwd_ref):
    q, ab = pl.program_id(0) // 2, lax.rem(pl.program_id(0), 2)
    h, da, db = (g_ref[q, ab, :, :, :, t].reshape(128, FC) for t in TENSORS)
    dwg_ref[...] = _dot(xs_ref[0], da, 0, 0)
    dwu_ref[...] = _dot(xs_ref[0], db, 0, 0)
    dwd_ref[...] = _dot(h, xs_ref[1], 0, 0)


def late_grads(y_ref, gx_ref, lwg, lwu, lwd, a_ref, b_ref, c_ref, yo_ref, gxo_ref, dwg_ref, dwu_ref, dwd_ref, sem, row_sem):
    copies = [pltpu.make_async_copy(y_ref, yo_ref, row_sem.at[0]), pltpu.make_async_copy(gx_ref, gxo_ref, row_sem.at[1])]
    for k in range(NB):
        src = pl.ds(k * 2 * FC, 2 * FC)
        dst = pl.ds((N1 + k) * 2 * FC, 2 * FC)
        copies += [pltpu.make_async_copy(lwg.at[:, src], dwg_ref.at[:, dst], sem.at[0, k]),
                   pltpu.make_async_copy(lwu.at[:, src], dwu_ref.at[:, dst], sem.at[1, k]),
                   pltpu.make_async_copy(lwd.at[src, :], dwd_ref.at[dst, :], sem.at[2, k])]
    for cp in copies:
        cp.start()
    for cp in copies:
        cp.wait()


def local_step(x_loc, wg_loc, wu_loc, wd_loc, gy_loc):
    vm = pl.BlockSpec(memory_space=pltpu.VMEM)
    hb = pl.BlockSpec(memory_space=pl.ANY)
    hbm = pl.BlockSpec(memory_space=pltpu.HBM)
    dma = pltpu.SemaphoreType.DMA
    row = jax.ShapeDtypeStruct((8, D), BF)
    kib = 1024
    half = (3, 2, 16, FC)
    xs, xin, gat1, acc, rows, sx, sy, kx, ky, r2n = pl.pallas_call(
        first_kernel,
        out_shape=(pltpu.VMEM((2, 128, DL), BF), pltpu.VMEM((16, 2, 8, DL), BF), pltpu.VMEM((N1, 2, 2, 2, 2, 3, 16, FC), BF),
                   pltpu.VMEM((2, 16, 8, DL), F32), pltpu.VMEM((2, 8, D), BF),
                   pltpu.VMEM((NB - 1,) + half, F32), pltpu.VMEM((NB - 1,) + half, F32),
                   pltpu.VMEM((NB,) + half, F32), pltpu.VMEM((NB,) + half, F32), pltpu.VMEM((2,) + half, F32)),
        in_specs=[hbm] * 5,
        out_specs=(vm,) * 10,
        scratch_shapes=[
            pltpu.VMEM((NP, DL, 2 * FC), BF),
            pltpu.VMEM((NP, DL, 2 * FC), BF),
            pltpu.VMEM((NP, 2 * FC, DL), BF),
            pltpu.VMEM((NP, 2, 3, 2, 2, 16, FC), F32),
            pltpu.VMEM((N1, 2) + half, F32),
            pltpu.VMEM((8, 2, 8, DL), BF),
            pltpu.VMEM((2, 2, 2, 3, 2, 2, 16, FC), F32),
            pltpu.VMEM((N1, 2, 3, 16, FC), F32),
            dma((2,)), dma((3, NP)), dma((16,)), dma((16,)),
            dma((2, NP)), dma((2, NP)), dma((2, NS)), dma((2, NS)),
            dma((2, NP)), dma((2, NP)), dma((2, NS)), dma((2, NS)),
            dma((2, N1)), dma((2, N1)), dma((2, N1)), dma((2, N1)),
            dma((2, N1)), dma((2, N1)), dma((N1,)), dma((N1,)),
        ],
        compiler_params=pltpu.CompilerParams(
            collective_id=0, has_side_effects=True, vmem_limit_bytes=49000 * kib),
        name="mlp_first",
    )(x_loc, gy_loc, wg_loc, wu_loc, wd_loc)

    rx = lax.ppermute(sx, "dp", [(i, i + 2 if i % 4 < 2 else i - 2) for i in range(8)])
    ry = lax.ppermute(sy, "dp", [(i, (i + 4) % 8) for i in range(8)])

    full = (jax.ShapeDtypeStruct((DL, FF_LOC), F32), jax.ShapeDtypeStruct((DL, FF_LOC), F32),
            jax.ShapeDtypeStruct((FF_LOC, DL), F32))

    dwg, dwu, dwd = pl.pallas_call(
        early_grads,
        grid=(2 * N1,),
        out_shape=full,
        in_specs=[vm, vm],
        out_specs=(pl.BlockSpec((DL, FC), lambda k: (0, k)), pl.BlockSpec((DL, FC), lambda k: (0, k)),
                   pl.BlockSpec((FC, DL), lambda k: (k, 0))),
        cost_estimate=pl.CostEstimate(flops=12 * N1 * 128 * DL * FC, bytes_accessed=24 * N1 * DL * FC,
                                      transcendentals=0),
        compiler_params=pltpu.CompilerParams(dimension_semantics=("arbitrary",), vmem_limit_bytes=9000 * kib),
        name="mlp_early_grads",
    )(xs, gat1)

    y_rows, gx_rows, lwg, lwu, lwd = pl.pallas_call(
        second_kernel,
        out_shape=(pltpu.VMEM((8, D), BF), pltpu.VMEM((8, D), BF), pltpu.VMEM((DL, NB * 2 * FC), F32),
                   pltpu.VMEM((DL, NB * 2 * FC), F32), pltpu.VMEM((NB * 2 * FC, DL), F32)),
        in_specs=[hbm] * 3 + [vm] * 9,
        out_specs=(vm,) * 5,
        scratch_shapes=[
            pltpu.VMEM((NB, 2, 2, 2, 2, 3, 16, FC), BF),
            pltpu.VMEM((DL, NB * 2 * FC), BF),
            pltpu.VMEM((DL, NB * 2 * FC), BF),
            pltpu.VMEM((NB * 2 * FC, DL), BF),
            pltpu.VMEM((NB, 2) + half, F32),
            pltpu.VMEM((NB, 2, 3, 16, FC), F32),
            pltpu.VMEM((2, 16, 8, DL), F32),
            pltpu.VMEM((16, 8, DL), F32), pltpu.VMEM((8, 8, DL), F32),
            pltpu.VMEM((8, 8, DL), BF), pltpu.VMEM((8, 8, DL), BF),
            dma((3,)), dma((2, NB)), dma((2, NB)), dma((2, NB)), dma((2, NB)),
            dma((2, NB)), dma((2, NB)), dma((2, 3)), dma((2, 3)),
            dma((NB,)), dma((NB,)), dma((3,)), dma((3,)),
            dma((16,)), dma((16,)), dma(()), dma(()), dma((16,)), dma((16,)),
        ],
        compiler_params=pltpu.CompilerParams(
            collective_id=1, has_side_effects=True, vmem_limit_bytes=30000 * kib),
        name="mlp_second",
    )(wg_loc, wu_loc, wd_loc, xs, xin, acc, rows, rx, ry, kx, ky, r2n)

    return pl.pallas_call(
        late_grads,
        out_shape=(row, row) + full,
        in_specs=[vm] * 5 + [hbm] * 3,
        out_specs=(hbm,) * 5,
        input_output_aliases={5: 2, 6: 3, 7: 4},
        scratch_shapes=[dma((3, NB)), dma((2,))],
        compiler_params=pltpu.CompilerParams(vmem_limit_bytes=30000 * kib),
        name="mlp_late_grads",
    )(y_rows, gx_rows, lwg, lwu, lwd, dwg, dwu, dwd)


def solution(mesh):
    row_spec = P(("dp", "tp"), None)
    up_spec = P("dp", "tp")
    down_spec = P("tp", "dp")
    return jax.shard_map(local_step, mesh=mesh,
                         in_specs=(row_spec, up_spec, up_spec, down_spec, row_spec),
                         out_specs=(row_spec, row_spec, up_spec, up_spec, down_spec),
                         check_vma=False)
```

```python
import itertools

import jax
import jax.numpy as jnp
from jax import lax
from jax.experimental import pallas as pl
from jax.experimental.pallas import tpu as pltpu
from jax.sharding import PartitionSpec as P

MESH = pl.DeviceIdType.MESH
BF = jnp.bfloat16
F32 = jnp.float32

BOTH = range(2)
TENSORS = range(3)
D = 3072
FF_LOC = 12288
DL = 384
NP = 8
N1 = 5
NB = NP - N1
FC = FF_LOC // (2 * NP)
NS = 3
SUB = FC // NS


def _dot(a, b, ca, cb):
    return lax.dot_general(a, b, (((ca,), (cb,)), ((), ())), preferred_element_type=F32)


def remote(src, dst, send, recv, dev):
    return pltpu.make_async_remote_copy(src_ref=src, dst_ref=dst, send_sem=send, recv_sem=recv,
                                        device_id=dev, device_id_type=MESH)


def sub(n):
    return pl.ds(n * SUB, SUB)


def block(tt, cc, yy, xx):
    return (cc * 4 + yy * 2 + xx) * 2 + tt


class Place:
    def __init__(self):
        tp, dp = lax.axis_index("tp"), lax.axis_index("dp")
        c, x, y = lax.rem(dp, 2), lax.rem(dp // 2, 2), dp // 4
        self.tp, self.dp, self.c, self.x, self.y = tp, dp, c, x, y
        self.me = tp * 8 + dp
        self.core_nb = (tp, y * 4 + x * 2 + (1 - c))
        self.x_nb = (tp, y * 4 + (1 - x) * 2 + c)
        self.y_nb = (tp, (1 - y) * 4 + x * 2 + c)
        self.z_nb = (1 - tp, dp)
        self.mine = block(tp, c, y, x)
        flips = sorted(itertools.product(BOTH, repeat=4), key=sum, reverse=True)[:-1]
        self.others = []
        for ft, fy, fx, fc in flips:
            tt, yy, xx, cc = (1 - v if f else v for v, f in zip((tp, y, x, c), (ft, fy, fx, fc)))
            self.others.append((tt, yy * 4 + xx * 2 + cc, block(tt, cc, yy, xx)))
        self.plane = [k for k, f in enumerate(flips) if not f[0]]

    def greet(self):
        barrier = pltpu.get_barrier_semaphore()
        for tt, dd, _ in self.others:
            pl.semaphore_signal(barrier, inc=1, device_id=(tt, dd), device_id_type=MESH)
        return barrier


def silu_parts(a, b, g):
    s = jax.nn.sigmoid(a)
    silu = a * s
    return ((silu * b).astype(BF), (g * b * (s * (1.0 + a * (1.0 - s)))).astype(BF), (g * silu).astype(BF))


def accumulate(acc, j, v):
    acc[j] = acc[j] + v.reshape(16, 8, DL)


def y_part(acc, gat, wd, q, lo, w):
    v = None
    for ab in BOTH:
        h = gat[q, ab, :, :, :, 0, :, lo:lo + w].reshape(128, w)
        d = _dot(h, wd(q, ab * FC + lo, w), 1, 0)
        v = d if v is None else v + d
    accumulate(acc, 0, v)


def dx_part(acc, gat, wg, wu, q, lo, w, ts=(1, 2)):
    v = None
    for ab in BOTH:
        for t, wt in ((t, (wg, wu)[t - 1]) for t in ts):
            z = gat[q, ab, :, :, :, t, :, lo:lo + w].reshape(128, w)
            d = _dot(z, wt(q, ab * FC + lo, w), 1, 1)
            v = d if v is None else v + d
    accumulate(acc, 1, v)


class Gather:
    def __init__(self, at, gat, s4, s5, s6, s5l=None, s6l=None):
        self.at, self.gat, self.s4, self.s5, self.s6, self.s5l, self.s6l = at, gat, s4, s5, s6, s5l, s6l

    def first(self, q, ab, arriving):
        at = self.at
        y0 = (1 - at.y) if arriving else at.y
        x1 = (1 - at.x) if arriving else at.x
        b = self.gat.at[q, 0, at.c, y0, at.x] if ab == 0 else self.gat.at[q, 1, at.c, at.y, x1]
        return remote(b, b, self.s4[0].at[ab, q], self.s4[1].at[ab, q], at.y_nb if ab == 0 else at.x_nb)

    def second(self, q, ab, arriving, n=None):
        at = self.at
        x0 = (1 - at.x) if arriving else at.x
        y1 = (1 - at.y) if arriving else at.y
        b = self.gat.at[q, 0, at.c, :, x0] if ab == 0 else self.gat.at[q, 1, at.c, y1]
        dev = at.x_nb if ab == 0 else at.y_nb
        if n is None:
            return remote(b, b, self.s5[0].at[ab, q], self.s5[1].at[ab, q], dev)
        b = b.at[:, n]
        return remote(b, b, self.s5l[0].at[ab, n], self.s5l[1].at[ab, n], dev)

    def third(self, q, arriving, n=None):
        at = self.at
        b = self.gat.at[q, :, (1 - at.c) if arriving else at.c]
        if n is None:
            return remote(b, b, self.s6[0].at[q], self.s6[1].at[q], at.core_nb)
        b = b.at[:, :, :, n]
        return remote(b, b, self.s6l[0].at[n], self.s6l[1].at[n], at.core_nb)


def first_kernel(x_hbm, gy_hbm, wg_hbm, wu_hbm, wd_hbm,
                 xs_ref, xin, gat, acc, rows, sx, sy, kx, ky, r2n,
                 wg, wu, wd, rd, r2, st, part, r3,
                 in_sem, w_sem, x_send, x_recv, d_send, d_recv, d0_send, d0_recv, s2_send, s2_recv, s20_send, s20_recv,
                 s3_send, s3_recv, s4_send, s4_recv, s5_send, s5_recv, s6_send, s6_recv):
    at = Place()
    c, mx, my = at.c, at.x, at.y
    net = Gather(at, gat, (s4_send, s4_recv), (s5_send, s5_recv), (s6_send, s6_recv))

    def w_copies(p):
        cols = pl.ds(pl.multiple_of(p * 2 * FC, 2 * FC), 2 * FC)
        return (pltpu.make_async_copy(wg_hbm.at[:, cols], wg.at[p], w_sem.at[0, p]),
                pltpu.make_async_copy(wu_hbm.at[:, cols], wu.at[p], w_sem.at[1, p]),
                pltpu.make_async_copy(wd_hbm.at[cols, :], wd.at[p], w_sem.at[2, p]))

    in_copies = [pltpu.make_async_copy(r, rows.at[j], in_sem.at[j]) for j, r in enumerate((x_hbm, gy_hbm))]
    for cp in in_copies:
        cp.start()
    barrier = at.greet()

    @pl.loop(0, NP)
    def _(p):
        for cp in w_copies(p):
            cp.start()

    acc[...] = jnp.zeros_like(acc)
    for j in BOTH:
        in_copies[j].wait()
        for dd in range(8):
            st[dd, j] = rows[j, :, dd * DL:(dd + 1) * DL]
    pl.semaphore_wait(barrier, 15)

    def x_copy(k, b):
        tt, dd, _ = at.others[k]
        return remote(st.at[dd], xin.at[b], x_send.at[k], x_recv.at[k], (tt, dd))

    everyone = range(len(at.others))
    for k in everyone:
        x_copy(k, at.mine).start()
    xin[at.mine] = st[at.dp]
    for k in everyone:
        x_copy(k, at.others[k][2]).wait_recv()

    for j in BOTH:
        xs_ref[j] = xin[:, j].astype(F32).reshape(128, DL).astype(BF)

    def d_copy(p, ab, n=None):
        s = lax.rem(p, 2)
        if n is None:
            return remote(part.at[s, 1 - c, ab], rd.at[p, ab], d_send.at[ab, p], d_recv.at[ab, p], at.core_nb)
        return remote(part.at[s, 1 - c, ab, :, :, :, :, sub(n)], rd.at[p, ab, :, :, :, :, sub(n)],
                      d0_send.at[ab, n], d0_recv.at[ab, n], at.core_nb)

    def s2_copy(p, ab, n=None):
        src = rd.at[p, 0, :, :, 1 - mx] if ab == 0 else rd.at[p, 1, :, 1 - my]
        dst = r2n.at[ab] if p is N1 else r2.at[p, ab]
        dev = at.x_nb if ab == 0 else at.y_nb
        if n is None:
            return remote(src, dst, s2_send.at[ab, p], s2_recv.at[ab, p], dev)
        return remote(src.at[:, :, :, sub(n)], dst.at[:, :, :, sub(n)], s20_send.at[ab, n], s20_recv.at[ab, n], dev)

    def s3_copy(p, ab):
        src = r2.at[p, 0, :, 1 - my] if ab == 0 else r2.at[p, 1, :, 1 - mx]
        return remote(src, r3.at[p, ab], s3_send.at[ab, p], s3_recv.at[ab, p], at.y_nb if ab == 0 else at.x_nb)

    def product(p, ab, n):
        s = lax.rem(p, 2)
        cols = pl.ds(ab * FC + n * SUB, SUB)
        vals = (_dot(xs_ref[0], wg[p, :, cols], 1, 0),
                _dot(xs_ref[0], wu[p, :, cols], 1, 0),
                _dot(xs_ref[1], wd[p, cols, :], 1, 1))
        for t in TENSORS:
            v = vals[t].reshape(2, 2, 2, 16, SUB)
            for cc in BOTH:
                part[s, cc, ab, t, :, :, :, sub(n)] = v[cc]

    def products(p):
        for cp in w_copies(p):
            cp.wait()
        for ab in BOTH:
            @pl.when(p >= 3)
            def _():
                d_copy(p - 2, ab).wait_send()

            @pl.when(p == 2)
            def _():
                for n in range(NS):
                    d_copy(0, ab, n).wait_send()
            for n in range(NS):
                product(p, ab, n)
            d_copy(p, ab).start()

    def stage2(p):
        s = lax.rem(p, 2)
        for ab in BOTH:
            d_copy(p, ab).wait_recv()
            for t in TENSORS:
                rd[p, ab, t] = rd[p, ab, t] + part[s, c, ab, t]

            @pl.when(p < N1)
            def _():
                s2_copy(p, ab).start()

        @pl.when(p >= N1)
        def _():
            for t in TENSORS:
                kx[p - N1, t] = rd[p, 0, t, :, mx]
                ky[p - N1, t] = rd[p, 1, t, my]

        @pl.when(p > N1)
        def _():
            for t in TENSORS:
                sx[p - N1 - 1, t] = rd[p, 0, t, :, 1 - mx]
                sy[p - N1 - 1, t] = rd[p, 1, t, 1 - my]

    def stage3(p):
        for ab in BOTH:
            @pl.when(p == 0)
            def _():
                for n in range(NS):
                    s2_copy(0, ab, n).wait_recv()

            @pl.when(p > 0)
            def _():
                s2_copy(p, ab).wait_recv()
            for t in TENSORS:
                r2[p, ab, t] = r2[p, ab, t] + (rd[p, 0, t, :, mx] if ab == 0 else rd[p, 1, t, my])
            s3_copy(p, ab).start()

    def stage4(p):
        for ab in BOTH:
            s3_copy(p, ab).wait_recv()
            keep = my if ab == 0 else mx
            vals = silu_parts(*(r3[p, ab, t] + r2[p, ab, t, keep] for t in TENSORS))
            for t in TENSORS:
                gat[p, ab, c, my, mx, t] = vals[t]
            net.first(p, ab, False).start()

    def stage5(p):
        for ab in BOTH:
            net.first(p, ab, True).wait_recv()
            net.second(p, ab, False).start()

        @pl.when(p == N1 - 1)
        def _():
            for ab in BOTH:
                s2_copy(N1, ab).start()

    def stage6(p):
        for ab in BOTH:
            net.second(p, ab, True).wait_recv()
        net.third(p, False).start()

    def stage7(p):
        net.third(p, True).wait_recv()
        y_part(acc, gat, lambda q, lo, w: wd[q, lo:lo + w, :], p, 0, FC)
        dx_part(acc, gat, *(lambda q, lo, w, r=r: r[q, :, lo:lo + w] for r in (wg, wu)), p, 0, FC)

    for cp in w_copies(0):
        cp.wait()
    for n in range(NS):
        for ab in BOTH:
            product(0, ab, n)
            d_copy(0, ab, n).start()
    for n in range(NS):
        for ab in BOTH:
            d_copy(0, ab, n).wait_recv()
            rd[0, ab, :, :, :, :, sub(n)] = rd[0, ab, :, :, :, :, sub(n)] + part[0, c, ab, :, :, :, :, sub(n)]
            s2_copy(0, ab, n).start()

    @pl.loop(0, N1 + 5)
    def _(i):
        pl.when((i >= 1) & (i < NP))(lambda: stage2(i))
        pl.when((i >= 1) & (i < N1 + 1))(lambda: stage3(i - 1))
        pl.when((i >= 2) & (i < N1 + 2))(lambda: stage4(i - 2))
        pl.when((i >= 3) & (i < N1 + 3))(lambda: stage5(i - 3))
        pl.when((i >= 4) & (i < N1 + 4))(lambda: stage6(i - 4))
        pl.when(i < NP - 1)(lambda: products(i + 1))
        pl.when(i >= 5)(lambda: stage7(i - 5))

    @pl.loop(0, N1)
    def _(p):
        for ab in BOTH:
            s3_copy(p, ab).wait_send()
            net.first(p, ab, False).wait_send()
            net.second(p, ab, False).wait_send()
        net.third(p, False).wait_send()

    @pl.loop(1, N1)
    def _(p):
        for ab in BOTH:
            s2_copy(p, ab).wait_send()
    for n in range(NS):
        for ab in BOTH:
            s2_copy(0, ab, n).wait_send()
    for p in (NP - 2, NP - 1):
        for ab in BOTH:
            d_copy(p, ab).wait_send()

    for k in everyone:
        x_copy(k, at.mine).wait_send()
    for ab in BOTH:
        s2_copy(N1, ab).wait_send()
        s2_copy(N1, ab).wait_recv()


def second_kernel(wg_hbm, wu_hbm, wd_hbm, xs_ref, xin, acc_in, rows, rx, ry, kx, ky, r2n,
                  y_ref, gx_ref, lwg, lwu, lwd,
                  gat, wg, wu, wd, r2b, r3, acc, fin, rz, ob, oy,
                  w_sem, s3_send, s3_recv, s4_send, s4_recv, s5_send, s5_recv, s5l_send, s5l_recv,
                  s6_send, s6_recv, s6l_send, s6l_recv, o_send, o_recv,
                  z_send, z_recv, p_send, p_recv):
    at = Place()
    c, mx, my = at.c, at.x, at.y
    net = Gather(at, gat, (s4_send, s4_recv), (s5_send, s5_recv), (s6_send, s6_recv),
                 (s5l_send, s5l_recv), (s6l_send, s6l_recv))
    barrier = pltpu.get_barrier_semaphore()
    for nb in (at.x_nb, at.y_nb, at.core_nb, at.z_nb):
        pl.semaphore_signal(barrier, inc=1, device_id=nb, device_id_type=MESH)
    cols = pl.ds(N1 * 2 * FC, NB * 2 * FC)
    w_copies = (pltpu.make_async_copy(wg_hbm.at[:, cols], wg, w_sem.at[0]),
                pltpu.make_async_copy(wu_hbm.at[:, cols], wu, w_sem.at[1]),
                pltpu.make_async_copy(wd_hbm.at[cols, :], wd, w_sem.at[2]))
    for cp in w_copies:
        cp.start()

    def s3_copy(q, ab):
        src = r2b.at[q, 0, :, 1 - my] if ab == 0 else r2b.at[q, 1, :, 1 - mx]
        return remote(src, r3.at[q, ab], s3_send.at[ab, q], s3_recv.at[ab, q], at.y_nb if ab == 0 else at.x_nb)

    def halves(q):
        for ab in BOTH:
            for t in TENSORS:
                got = r2n[ab, t] if q == 0 else (rx, ry)[ab][q - 1, t]
                r2b[q, ab, t] = got + (kx, ky)[ab][q, t]

    def send_quarters(q):
        for ab in BOTH:
            s3_copy(q, ab).start()

    def activate(q):
        for ab in BOTH:
            s3_copy(q, ab).wait_recv()
            keep = my if ab == 0 else mx
            vals = silu_parts(*(r3[q, ab, t] + r2b[q, ab, t, keep] for t in TENSORS))
            for t in TENSORS:
                gat[q, ab, c, my, mx, t] = vals[t]
            net.first(q, ab, False).start()

    def spread(q):
        for ab in BOTH:
            net.first(q, ab, True).wait_recv()
            if q < NB - 1:
                net.second(q, ab, False).start()
            else:
                for n in TENSORS:
                    net.second(q, ab, False, n).start()

    def cross(q):
        for ab in BOTH:
            net.second(q, ab, True).wait_recv()
        net.third(q, False).start()

    def down(q, lo, w):
        return wd[q * 2 * FC + lo:q * 2 * FC + lo + w, :]

    def gate(q, lo, w):
        return wg[:, q * 2 * FC + lo:q * 2 * FC + lo + w]

    def up(q, lo, w):
        return wu[:, q * 2 * FC + lo:q * 2 * FC + lo + w]

    halves(0)
    pl.semaphore_wait(barrier, 4)
    send_quarters(0)
    for q in range(1, NB):
        halves(q)
        if q < NB - 1:
            send_quarters(q)
    acc[...] = acc_in[...]
    for q in range(NB):
        activate(q)
        if q == 0:
            send_quarters(NB - 1)
        else:
            spread(q - 1)
    spread(NB - 1)
    for cp in w_copies:
        cp.wait()
    q = NB - 1

    everyone = range(len(at.others))

    def o_copy(k, slot):
        tt, dd, b = at.others[k]
        return remote(acc.at[1, b], fin.at[slot], o_send.at[k], o_recv.at[k], (tt, dd))

    halves_y = acc.reshape(2, 8, 2, 8, DL)
    z_copy = remote(halves_y.at[0, :, 1 - at.tp], rz, z_send, z_recv, at.z_nb)

    def p_copy(k, slot):
        tt, dd, b = at.others[k]
        return remote(ob.at[b // 2], oy.at[slot], p_send.at[k], p_recv.at[k], (tt, dd))

    def y_rows_out():
        z_copy.wait_recv()
        for b in range(8):
            ob[b] = (xin[2 * b + at.tp, 0].astype(F32) + (halves_y[0, b, at.tp] + rz[b])).astype(BF)
        for k in at.plane:
            p_copy(k, at.dp).start()
        oy[at.dp] = ob[at.mine // 2]

    def finish(n):
        net.third(q, True, n).wait_recv()
        if n == 0:
            y_part(acc, gat, down, q, 0, FC)
            z_copy.start()
        else:
            dx_part(acc, gat, gate, up, q, 0, FC, (n,))
        if n == 2:
            for k in everyone:
                o_copy(k, at.me).start()
            fin[at.me] = acc[1, at.mine]

    def late(k):
        lo = pl.ds(pl.multiple_of(k * FC, FC), FC)
        h, da, db = (gat[k // 2, k % 2, :, :, :, t].reshape(128, FC) for t in TENSORS)
        lwg[:, lo] = _dot(xs_ref[0], da, 0, 0)
        lwu[:, lo] = _dot(xs_ref[0], db, 0, 0)
        lwd[lo, :] = _dot(h, xs_ref[1], 0, 0)

    def cross_last(n):
        for ab in BOTH:
            net.second(q, ab, True, n).wait_recv()
        net.third(q, False, n).start()

    cross(0)
    for p in range(1, NB - 1):
        net.third(p - 1, True).wait_recv()
        y_part(acc, gat, down, p - 1, 0, FC)
        dx_part(acc, gat, gate, up, p - 1, 0, FC)
        cross(p)
    late(0)
    cross_last(0)
    late(1)
    cross_last(1)
    net.third(q - 1, True).wait_recv()
    y_part(acc, gat, down, q - 1, 0, FC)
    cross_last(2)
    finish(0)
    dx_part(acc, gat, gate, up, q - 1, 0, FC)
    finish(1)
    finish(2)
    y_rows_out()

    pl.loop(2, 2 * NB)(late)

    for q in range(NB):
        for ab in BOTH:
            s3_copy(q, ab).wait_send()
            net.first(q, ab, False).wait_send()
            if q < NB - 1:
                net.second(q, ab, False).wait_send()
            else:
                for n in TENSORS:
                    net.second(q, ab, False, n).wait_send()
        if q < NB - 1:
            net.third(q, False).wait_send()
        else:
            for n in TENSORS:
                net.third(q, False, n).wait_send()

    def arrival(k):
        tt, dd, _ = at.others[k]
        return o_copy(k, tt * 8 + dd), p_copy(k, dd)

    for k in at.plane:
        arrival(k)[1].wait_recv()
    for k in everyone:
        arrival(k)[0].wait_recv()
    for dd in range(8):
        cols = slice(dd * DL, (dd + 1) * DL)
        y_ref[:, cols] = oy[dd]
        gx_ref[:, cols] = (rows[1, :, cols].astype(F32) + (fin[dd] + fin[8 + dd])).astype(BF)
    z_copy.wait_send()
    for k in at.plane:
        p_copy(k, at.dp).wait_send()
    for k in everyone:
        o_copy(k, at.me).wait_send()


def early_grads(xs_ref, g_ref, dwg_ref, dwu_ref, dwd_ref):
    q, ab = pl.program_id(0) // 2, lax.rem(pl.program_id(0), 2)
    h, da, db = (g_ref[q, ab, :, :, :, t].reshape(128, FC) for t in TENSORS)
    dwg_ref[...] = _dot(xs_ref[0], da, 0, 0)
    dwu_ref[...] = _dot(xs_ref[0], db, 0, 0)
    dwd_ref[...] = _dot(h, xs_ref[1], 0, 0)


def late_grads(y_ref, gx_ref, lwg, lwu, lwd, a_ref, b_ref, c_ref, yo_ref, gxo_ref, dwg_ref, dwu_ref, dwd_ref, sem, row_sem):
    copies = [pltpu.make_async_copy(y_ref, yo_ref, row_sem.at[0]), pltpu.make_async_copy(gx_ref, gxo_ref, row_sem.at[1])]
    for k in range(NB):
        src = pl.ds(k * 2 * FC, 2 * FC)
        dst = pl.ds((N1 + k) * 2 * FC, 2 * FC)
        copies += [pltpu.make_async_copy(lwg.at[:, src], dwg_ref.at[:, dst], sem.at[0, k]),
                   pltpu.make_async_copy(lwu.at[:, src], dwu_ref.at[:, dst], sem.at[1, k]),
                   pltpu.make_async_copy(lwd.at[src, :], dwd_ref.at[dst, :], sem.at[2, k])]
    for cp in copies:
        cp.start()
    for cp in copies:
        cp.wait()


def local_step(x_loc, wg_loc, wu_loc, wd_loc, gy_loc):
    vm = pl.BlockSpec(memory_space=pltpu.VMEM)
    hb = pl.BlockSpec(memory_space=pl.ANY)
    hbm = pl.BlockSpec(memory_space=pltpu.HBM)
    dma = pltpu.SemaphoreType.DMA
    row = jax.ShapeDtypeStruct((8, D), BF)
    kib = 1024
    half = (3, 2, 16, FC)
    xs, xin, gat1, acc, rows, sx, sy, kx, ky, r2n = pl.pallas_call(
        first_kernel,
        out_shape=(pltpu.VMEM((2, 128, DL), BF), pltpu.VMEM((16, 2, 8, DL), BF), pltpu.VMEM((N1, 2, 2, 2, 2, 3, 16, FC), BF),
                   pltpu.VMEM((2, 16, 8, DL), F32), pltpu.VMEM((2, 8, D), BF),
                   pltpu.VMEM((NB - 1,) + half, F32), pltpu.VMEM((NB - 1,) + half, F32),
                   pltpu.VMEM((NB,) + half, F32), pltpu.VMEM((NB,) + half, F32), pltpu.VMEM((2,) + half, F32)),
        in_specs=[hbm] * 5,
        out_specs=(vm,) * 10,
        scratch_shapes=[
            pltpu.VMEM((NP, DL, 2 * FC), BF),
            pltpu.VMEM((NP, DL, 2 * FC), BF),
            pltpu.VMEM((NP, 2 * FC, DL), BF),
            pltpu.VMEM((NP, 2, 3, 2, 2, 16, FC), F32),
            pltpu.VMEM((N1, 2) + half, F32),
            pltpu.VMEM((8, 2, 8, DL), BF),
            pltpu.VMEM((2, 2, 2, 3, 2, 2, 16, FC), F32),
            pltpu.VMEM((N1, 2, 3, 16, FC), F32),
            dma((2,)), dma((3, NP)), dma((16,)), dma((16,)),
            dma((2, NP)), dma((2, NP)), dma((2, NS)), dma((2, NS)),
            dma((2, NP)), dma((2, NP)), dma((2, NS)), dma((2, NS)),
            dma((2, N1)), dma((2, N1)), dma((2, N1)), dma((2, N1)),
            dma((2, N1)), dma((2, N1)), dma((N1,)), dma((N1,)),
        ],
        compiler_params=pltpu.CompilerParams(
            collective_id=0, has_side_effects=True, vmem_limit_bytes=49000 * kib),
        name="mlp_first",
    )(x_loc, gy_loc, wg_loc, wu_loc, wd_loc)

    rx = lax.ppermute(sx, "dp", [(i, i + 2 if i % 4 < 2 else i - 2) for i in range(8)])
    ry = lax.ppermute(sy, "dp", [(i, (i + 4) % 8) for i in range(8)])

    full = (jax.ShapeDtypeStruct((DL, FF_LOC), F32), jax.ShapeDtypeStruct((DL, FF_LOC), F32),
            jax.ShapeDtypeStruct((FF_LOC, DL), F32))

    dwg, dwu, dwd = pl.pallas_call(
        early_grads,
        grid=(2 * N1,),
        out_shape=full,
        in_specs=[vm, vm],
        out_specs=(pl.BlockSpec((DL, FC), lambda k: (0, k)), pl.BlockSpec((DL, FC), lambda k: (0, k)),
                   pl.BlockSpec((FC, DL), lambda k: (k, 0))),
        cost_estimate=pl.CostEstimate(flops=12 * N1 * 128 * DL * FC, bytes_accessed=24 * N1 * DL * FC,
                                      transcendentals=0),
        compiler_params=pltpu.CompilerParams(dimension_semantics=("arbitrary",), vmem_limit_bytes=9000 * kib),
        name="mlp_early_grads",
    )(xs, gat1)

    y_rows, gx_rows, lwg, lwu, lwd = pl.pallas_call(
        second_kernel,
        out_shape=(pltpu.VMEM((8, D), BF), pltpu.VMEM((8, D), BF), pltpu.VMEM((DL, NB * 2 * FC), F32),
                   pltpu.VMEM((DL, NB * 2 * FC), F32), pltpu.VMEM((NB * 2 * FC, DL), F32)),
        in_specs=[hbm] * 3 + [vm] * 9,
        out_specs=(vm,) * 5,
        scratch_shapes=[
            pltpu.VMEM((NB, 2, 2, 2, 2, 3, 16, FC), BF),
            pltpu.VMEM((DL, NB * 2 * FC), BF),
            pltpu.VMEM((DL, NB * 2 * FC), BF),
            pltpu.VMEM((NB * 2 * FC, DL), BF),
            pltpu.VMEM((NB, 2) + half, F32),
            pltpu.VMEM((NB, 2, 3, 16, FC), F32),
            pltpu.VMEM((2, 16, 8, DL), F32),
            pltpu.VMEM((16, 8, DL), F32), pltpu.VMEM((8, 8, DL), F32),
            pltpu.VMEM((8, 8, DL), BF), pltpu.VMEM((8, 8, DL), BF),
            dma((3,)), dma((2, NB)), dma((2, NB)), dma((2, NB)), dma((2, NB)),
            dma((2, NB)), dma((2, NB)), dma((2, 3)), dma((2, 3)),
            dma((NB,)), dma((NB,)), dma((3,)), dma((3,)),
            dma((16,)), dma((16,)), dma(()), dma(()), dma((16,)), dma((16,)),
        ],
        compiler_params=pltpu.CompilerParams(
            collective_id=1, has_side_effects=True, vmem_limit_bytes=30000 * kib),
        name="mlp_second",
    )(wg_loc, wu_loc, wd_loc, xs, xin, acc, rows, rx, ry, kx, ky, r2n)

    return pl.pallas_call(
        late_grads,
        out_shape=(row, row) + full,
        in_specs=[vm] * 5 + [hbm] * 3,
        out_specs=(hbm,) * 5,
        input_output_aliases={5: 2, 6: 3, 7: 4},
        scratch_shapes=[dma((3, NB)), dma((2,))],
        compiler_params=pltpu.CompilerParams(vmem_limit_bytes=30000 * kib),
        name="mlp_late_grads",
    )(y_rows, gx_rows, lwg, lwu, lwd, dwg, dwu, dwd)


def solution(mesh):
    row_spec = P(("dp", "tp"), None)
    up_spec = P("dp", "tp")
    down_spec = P("tp", "dp")
    return jax.shard_map(local_step, mesh=mesh,
                         in_specs=(row_spec, up_spec, up_spec, down_spec, row_spec),
                         out_specs=(row_spec, row_spec, up_spec, up_spec, down_spec),
                         check_vma=False)
```

```python
import itertools

import jax
import jax.numpy as jnp
from jax import lax
from jax.experimental import pallas as pl
from jax.experimental.pallas import tpu as pltpu
from jax.sharding import PartitionSpec as P

MESH = pl.DeviceIdType.MESH
BF = jnp.bfloat16
F32 = jnp.float32

BOTH = range(2)
TENSORS = range(3)
D = 3072
FF_LOC = 12288
DL = 384
NP = 8
N1 = 5
NB = NP - N1
FC = FF_LOC // (2 * NP)
NS = 3
SUB = FC // NS


def _dot(a, b, ca, cb):
    return lax.dot_general(a, b, (((ca,), (cb,)), ((), ())), preferred_element_type=F32)


def remote(src, dst, send, recv, dev):
    return pltpu.make_async_remote_copy(src_ref=src, dst_ref=dst, send_sem=send, recv_sem=recv,
                                        device_id=dev, device_id_type=MESH)


def sub(n):
    return pl.ds(n * SUB, SUB)


def block(tt, cc, yy, xx):
    return (cc * 4 + yy * 2 + xx) * 2 + tt


class Place:
    def __init__(self):
        tp, dp = lax.axis_index("tp"), lax.axis_index("dp")
        c, x, y = lax.rem(dp, 2), lax.rem(dp // 2, 2), dp // 4
        self.tp, self.dp, self.c, self.x, self.y = tp, dp, c, x, y
        self.me = tp * 8 + dp
        self.core_nb = (tp, y * 4 + x * 2 + (1 - c))
        self.x_nb = (tp, y * 4 + (1 - x) * 2 + c)
        self.y_nb = (tp, (1 - y) * 4 + x * 2 + c)
        self.mine = block(tp, c, y, x)
        flips = sorted(itertools.product(BOTH, repeat=4), key=sum, reverse=True)[:-1]
        self.others = []
        for ft, fy, fx, fc in flips:
            tt, yy, xx, cc = (1 - v if f else v for v, f in zip((tp, y, x, c), (ft, fy, fx, fc)))
            self.others.append((tt, yy * 4 + xx * 2 + cc, block(tt, cc, yy, xx)))

    def greet(self):
        barrier = pltpu.get_barrier_semaphore()
        for tt, dd, _ in self.others:
            pl.semaphore_signal(barrier, inc=1, device_id=(tt, dd), device_id_type=MESH)
        return barrier


def silu_parts(a, b, g):
    s = jax.nn.sigmoid(a)
    silu = a * s
    return ((silu * b).astype(BF), (g * b * (s * (1.0 + a * (1.0 - s)))).astype(BF), (g * silu).astype(BF))


def accumulate(acc, j, v):
    acc[j] = acc[j] + v.reshape(16, 8, DL)


def y_part(acc, gat, wd, q, lo, w):
    v = None
    for ab in BOTH:
        h = gat[q, ab, :, :, :, 0, :, lo:lo + w].reshape(128, w)
        d = _dot(h, wd(q, ab * FC + lo, w), 1, 0)
        v = d if v is None else v + d
    accumulate(acc, 0, v)


def dx_part(acc, gat, wg, wu, q, lo, w, ts=(1, 2)):
    v = None
    for ab in BOTH:
        for t, wt in ((t, (wg, wu)[t - 1]) for t in ts):
            z = gat[q, ab, :, :, :, t, :, lo:lo + w].reshape(128, w)
            d = _dot(z, wt(q, ab * FC + lo, w), 1, 1)
            v = d if v is None else v + d
    accumulate(acc, 1, v)


class Gather:
    def __init__(self, at, gat, s4, s5, s6, s5l=None, s6l=None):
        self.at, self.gat, self.s4, self.s5, self.s6, self.s5l, self.s6l = at, gat, s4, s5, s6, s5l, s6l

    def first(self, q, ab, arriving):
        at = self.at
        y0 = (1 - at.y) if arriving else at.y
        x1 = (1 - at.x) if arriving else at.x
        b = self.gat.at[q, 0, at.c, y0, at.x] if ab == 0 else self.gat.at[q, 1, at.c, at.y, x1]
        return remote(b, b, self.s4[0].at[ab, q], self.s4[1].at[ab, q], at.y_nb if ab == 0 else at.x_nb)

    def second(self, q, ab, arriving, n=None):
        at = self.at
        x0 = (1 - at.x) if arriving else at.x
        y1 = (1 - at.y) if arriving else at.y
        b = self.gat.at[q, 0, at.c, :, x0] if ab == 0 else self.gat.at[q, 1, at.c, y1]
        dev = at.x_nb if ab == 0 else at.y_nb
        if n is None:
            return remote(b, b, self.s5[0].at[ab, q], self.s5[1].at[ab, q], dev)
        b = b.at[:, n]
        return remote(b, b, self.s5l[0].at[ab, n], self.s5l[1].at[ab, n], dev)

    def third(self, q, arriving, n=None):
        at = self.at
        b = self.gat.at[q, :, (1 - at.c) if arriving else at.c]
        if n is None:
            return remote(b, b, self.s6[0].at[q], self.s6[1].at[q], at.core_nb)
        b = b.at[:, :, :, n]
        return remote(b, b, self.s6l[0].at[n], self.s6l[1].at[n], at.core_nb)


def first_kernel(x_hbm, gy_hbm, wg_hbm, wu_hbm, wd_hbm,
                 xs_ref, gat, acc, rows, sx, sy, kx, ky, r2n,
                 wg, wu, wd, rd, r2, st, xin, part, r3,
                 in_sem, w_sem, x_send, x_recv, d_send, d_recv, d0_send, d0_recv, s2_send, s2_recv, s20_send, s20_recv,
                 s3_send, s3_recv, s4_send, s4_recv, s5_send, s5_recv, s6_send, s6_recv):
    at = Place()
    c, mx, my = at.c, at.x, at.y
    net = Gather(at, gat, (s4_send, s4_recv), (s5_send, s5_recv), (s6_send, s6_recv))

    def w_copies(p):
        cols = pl.ds(pl.multiple_of(p * 2 * FC, 2 * FC), 2 * FC)
        return (pltpu.make_async_copy(wg_hbm.at[:, cols], wg.at[p], w_sem.at[0, p]),
                pltpu.make_async_copy(wu_hbm.at[:, cols], wu.at[p], w_sem.at[1, p]),
                pltpu.make_async_copy(wd_hbm.at[cols, :], wd.at[p], w_sem.at[2, p]))

    in_copies = [pltpu.make_async_copy(r, rows.at[j], in_sem.at[j]) for j, r in enumerate((x_hbm, gy_hbm))]
    for cp in in_copies:
        cp.start()
    barrier = at.greet()

    for cp in w_copies(0):
        cp.start()

    acc[...] = jnp.zeros_like(acc)
    for j in BOTH:
        in_copies[j].wait()
        for dd in range(8):
            st[dd, j] = rows[j, :, dd * DL:(dd + 1) * DL]
    pl.semaphore_wait(barrier, 15)

    def x_copy(k, b):
        tt, dd, _ = at.others[k]
        return remote(st.at[dd], xin.at[b], x_send.at[k], x_recv.at[k], (tt, dd))

    everyone = range(len(at.others))
    for k in everyone:
        x_copy(k, at.mine).start()
    xin[at.mine] = st[at.dp]

    @pl.loop(1, NP)
    def _(p):
        for cp in w_copies(p):
            cp.start()

    for k in everyone:
        x_copy(k, at.others[k][2]).wait_recv()

    for j in BOTH:
        xs_ref[j] = xin[:, j].astype(F32).reshape(128, DL).astype(BF)

    def d_copy(p, ab, n=None):
        s = lax.rem(p, 2)
        if n is None:
            return remote(part.at[s, 1 - c, ab], rd.at[p, ab], d_send.at[ab, p], d_recv.at[ab, p], at.core_nb)
        return remote(part.at[s, 1 - c, ab, :, :, :, :, sub(n)], rd.at[p, ab, :, :, :, :, sub(n)],
                      d0_send.at[ab, n], d0_recv.at[ab, n], at.core_nb)

    def s2_copy(p, ab, n=None):
        src = rd.at[p, 0, :, :, 1 - mx] if ab == 0 else rd.at[p, 1, :, 1 - my]
        dst = r2n.at[ab] if p is N1 else r2.at[p, ab]
        dev = at.x_nb if ab == 0 else at.y_nb
        if n is None:
            return remote(src, dst, s2_send.at[ab, p], s2_recv.at[ab, p], dev)
        return remote(src.at[:, :, :, sub(n)], dst.at[:, :, :, sub(n)], s20_send.at[ab, n], s20_recv.at[ab, n], dev)

    def s3_copy(p, ab):
        src = r2.at[p, 0, :, 1 - my] if ab == 0 else r2.at[p, 1, :, 1 - mx]
        return remote(src, r3.at[p, ab], s3_send.at[ab, p], s3_recv.at[ab, p], at.y_nb if ab == 0 else at.x_nb)

    def product(p, ab, n):
        s = lax.rem(p, 2)
        cols = pl.ds(ab * FC + n * SUB, SUB)
        vals = (_dot(xs_ref[0], wg[p, :, cols], 1, 0),
                _dot(xs_ref[0], wu[p, :, cols], 1, 0),
                _dot(xs_ref[1], wd[p, cols, :], 1, 1))
        for t in TENSORS:
            v = vals[t].reshape(2, 2, 2, 16, SUB)
            for cc in BOTH:
                part[s, cc, ab, t, :, :, :, sub(n)] = v[cc]

    def products(p):
        for cp in w_copies(p):
            cp.wait()
        for ab in BOTH:
            @pl.when(p >= 3)
            def _():
                d_copy(p - 2, ab).wait_send()

            @pl.when(p == 2)
            def _():
                for n in range(NS):
                    d_copy(0, ab, n).wait_send()
            for n in range(NS):
                product(p, ab, n)
            d_copy(p, ab).start()

    def stage2(p):
        s = lax.rem(p, 2)
        for ab in BOTH:
            d_copy(p, ab).wait_recv()
            for t in TENSORS:
                rd[p, ab, t] = rd[p, ab, t] + part[s, c, ab, t]

            @pl.when(p < N1)
            def _():
                s2_copy(p, ab).start()

        @pl.when(p >= N1)
        def _():
            for t in TENSORS:
                kx[p - N1, t] = rd[p, 0, t, :, mx]
                ky[p - N1, t] = rd[p, 1, t, my]

        @pl.when(p > N1)
        def _():
            for t in TENSORS:
                sx[p - N1 - 1, t] = rd[p, 0, t, :, 1 - mx]
                sy[p - N1 - 1, t] = rd[p, 1, t, 1 - my]

    def stage3(p):
        for ab in BOTH:
            @pl.when(p == 0)
            def _():
                for n in range(NS):
                    s2_copy(0, ab, n).wait_recv()

            @pl.when(p > 0)
            def _():
                s2_copy(p, ab).wait_recv()
            for t in TENSORS:
                r2[p, ab, t] = r2[p, ab, t] + (rd[p, 0, t, :, mx] if ab == 0 else rd[p, 1, t, my])
            s3_copy(p, ab).start()

    def stage4(p):
        for ab in BOTH:
            s3_copy(p, ab).wait_recv()
            keep = my if ab == 0 else mx
            vals = silu_parts(*(r3[p, ab, t] + r2[p, ab, t, keep] for t in TENSORS))
            for t in TENSORS:
                gat[p, ab, c, my, mx, t] = vals[t]
            net.first(p, ab, False).start()

    def stage5(p):
        for ab in BOTH:
            net.first(p, ab, True).wait_recv()
            net.second(p, ab, False).start()

        @pl.when(p == N1 - 1)
        def _():
            for ab in BOTH:
                s2_copy(N1, ab).start()

    def stage6(p):
        for ab in BOTH:
            net.second(p, ab, True).wait_recv()
        net.third(p, False).start()

    def stage7(p):
        net.third(p, True).wait_recv()
        y_part(acc, gat, lambda q, lo, w: wd[q, lo:lo + w, :], p, 0, FC)
        dx_part(acc, gat, *(lambda q, lo, w, r=r: r[q, :, lo:lo + w] for r in (wg, wu)), p, 0, FC)

    for cp in w_copies(0):
        cp.wait()
    for n in range(NS):
        for ab in BOTH:
            product(0, ab, n)
            d_copy(0, ab, n).start()
    for n in range(NS):
        for ab in BOTH:
            d_copy(0, ab, n).wait_recv()
            rd[0, ab, :, :, :, :, sub(n)] = rd[0, ab, :, :, :, :, sub(n)] + part[0, c, ab, :, :, :, :, sub(n)]
            s2_copy(0, ab, n).start()

    @pl.loop(0, N1 + 5)
    def _(i):
        pl.when((i >= 1) & (i < NP))(lambda: stage2(i))
        pl.when((i >= 1) & (i < N1 + 1))(lambda: stage3(i - 1))
        pl.when((i >= 2) & (i < N1 + 2))(lambda: stage4(i - 2))
        pl.when((i >= 3) & (i < N1 + 3))(lambda: stage5(i - 3))
        pl.when((i >= 4) & (i < N1 + 4))(lambda: stage6(i - 4))
        pl.when(i < NP - 1)(lambda: products(i + 1))
        pl.when(i >= 5)(lambda: stage7(i - 5))

    @pl.loop(0, N1)
    def _(p):
        for ab in BOTH:
            s3_copy(p, ab).wait_send()
            net.first(p, ab, False).wait_send()
            net.second(p, ab, False).wait_send()
        net.third(p, False).wait_send()

    @pl.loop(1, N1)
    def _(p):
        for ab in BOTH:
            s2_copy(p, ab).wait_send()
    for n in range(NS):
        for ab in BOTH:
            s2_copy(0, ab, n).wait_send()
    for p in (NP - 2, NP - 1):
        for ab in BOTH:
            d_copy(p, ab).wait_send()

    for k in everyone:
        x_copy(k, at.mine).wait_send()
    for ab in BOTH:
        s2_copy(N1, ab).wait_send()
        s2_copy(N1, ab).wait_recv()


def second_kernel(wg_hbm, wu_hbm, wd_hbm, xs_ref, acc_in, rows, rx, ry, kx, ky, r2n,
                  y_ref, gx_ref, lwg, lwu, lwd,
                  gat, wg, wu, wd, r2b, r3, acc, fin,
                  w_sem, s3_send, s3_recv, s4_send, s4_recv, s5_send, s5_recv, s5l_send, s5l_recv,
                  s6_send, s6_recv, s6l_send, s6l_recv, o_send, o_recv):
    at = Place()
    c, mx, my = at.c, at.x, at.y
    net = Gather(at, gat, (s4_send, s4_recv), (s5_send, s5_recv), (s6_send, s6_recv),
                 (s5l_send, s5l_recv), (s6l_send, s6l_recv))
    barrier = pltpu.get_barrier_semaphore()
    for nb in (at.x_nb, at.y_nb, at.core_nb, (1 - at.tp, at.dp)):
        pl.semaphore_signal(barrier, inc=1, device_id=nb, device_id_type=MESH)
    cols = pl.ds(N1 * 2 * FC, NB * 2 * FC)
    w_copies = (pltpu.make_async_copy(wg_hbm.at[:, cols], wg, w_sem.at[0]),
                pltpu.make_async_copy(wu_hbm.at[:, cols], wu, w_sem.at[1]),
                pltpu.make_async_copy(wd_hbm.at[cols, :], wd, w_sem.at[2]))
    for cp in w_copies:
        cp.start()

    def s3_copy(q, ab):
        src = r2b.at[q, 0, :, 1 - my] if ab == 0 else r2b.at[q, 1, :, 1 - mx]
        return remote(src, r3.at[q, ab], s3_send.at[ab, q], s3_recv.at[ab, q], at.y_nb if ab == 0 else at.x_nb)

    def halves(q):
        for ab in BOTH:
            for t in TENSORS:
                got = r2n[ab, t] if q == 0 else (rx, ry)[ab][q - 1, t]
                r2b[q, ab, t] = got + (kx, ky)[ab][q, t]

    def send_quarters(q):
        for ab in BOTH:
            s3_copy(q, ab).start()

    def activate(q):
        for ab in BOTH:
            s3_copy(q, ab).wait_recv()
            keep = my if ab == 0 else mx
            vals = silu_parts(*(r3[q, ab, t] + r2b[q, ab, t, keep] for t in TENSORS))
            for t in TENSORS:
                gat[q, ab, c, my, mx, t] = vals[t]
            net.first(q, ab, False).start()

    def spread(q):
        for ab in BOTH:
            net.first(q, ab, True).wait_recv()
            if q < NB - 1:
                net.second(q, ab, False).start()
            else:
                for n in TENSORS:
                    net.second(q, ab, False, n).start()

    def cross(q):
        for ab in BOTH:
            net.second(q, ab, True).wait_recv()
        net.third(q, False).start()

    def down(q, lo, w):
        return wd[q * 2 * FC + lo:q * 2 * FC + lo + w, :]

    def gate(q, lo, w):
        return wg[:, q * 2 * FC + lo:q * 2 * FC + lo + w]

    def up(q, lo, w):
        return wu[:, q * 2 * FC + lo:q * 2 * FC + lo + w]

    halves(0)
    pl.semaphore_wait(barrier, 4)
    send_quarters(0)
    for q in range(1, NB):
        halves(q)
        if q < NB - 1:
            send_quarters(q)
    acc[...] = acc_in[...]
    for q in range(NB):
        activate(q)
        if q == 0:
            send_quarters(NB - 1)
        else:
            spread(q - 1)
    spread(NB - 1)
    for cp in w_copies:
        cp.wait()
    q = NB - 1

    everyone = range(len(at.others))

    def o_copy(j, k, slot):
        tt, dd, b = at.others[k]
        return remote(acc.at[j, b], fin.at[j, slot], o_send.at[j, k], o_recv.at[j, k], (tt, dd))

    def send_out(j):
        for k in everyone:
            o_copy(j, k, at.me).start()
        fin[j, at.me] = acc[j, at.mine]

    def finish(n):
        net.third(q, True, n).wait_recv()
        if n == 0:
            y_part(acc, gat, down, q, 0, FC)
            send_out(0)
        else:
            dx_part(acc, gat, gate, up, q, 0, FC, (n,))
        if n == 2:
            send_out(1)

    def late(k):
        lo = pl.ds(pl.multiple_of(k * FC, FC), FC)
        h, da, db = (gat[k // 2, k % 2, :, :, :, t].reshape(128, FC) for t in TENSORS)
        lwg[:, lo] = _dot(xs_ref[0], da, 0, 0)
        lwu[:, lo] = _dot(xs_ref[0], db, 0, 0)
        lwd[lo, :] = _dot(h, xs_ref[1], 0, 0)

    def cross_last(n):
        for ab in BOTH:
            net.second(q, ab, True, n).wait_recv()
        net.third(q, False, n).start()

    cross(0)
    for p in range(1, NB - 1):
        net.third(p - 1, True).wait_recv()
        y_part(acc, gat, down, p - 1, 0, FC)
        dx_part(acc, gat, gate, up, p - 1, 0, FC)
        cross(p)
    cross_last(0)
    cross_last(1)
    net.third(q - 1, True).wait_recv()
    y_part(acc, gat, down, q - 1, 0, FC)
    cross_last(2)
    finish(0)
    dx_part(acc, gat, gate, up, q - 1, 0, FC)
    finish(1)
    finish(2)

    pl.loop(0, 2 * NB)(late)

    for q in range(NB):
        for ab in BOTH:
            s3_copy(q, ab).wait_send()
            net.first(q, ab, False).wait_send()
            if q < NB - 1:
                net.second(q, ab, False).wait_send()
            else:
                for n in TENSORS:
                    net.second(q, ab, False, n).wait_send()
        if q < NB - 1:
            net.third(q, False).wait_send()
        else:
            for n in TENSORS:
                net.third(q, False, n).wait_send()

    for j, out in enumerate((y_ref, gx_ref)):
        for k in everyone:
            tt, dd, _ = at.others[k]
            o_copy(j, k, tt * 8 + dd).wait_recv()
        for dd in range(8):
            cols = slice(dd * DL, (dd + 1) * DL)
            out[:, cols] = (rows[j, :, cols].astype(F32) + (fin[j, dd] + fin[j, 8 + dd])).astype(BF)

    for k in everyone:
        for j in BOTH:
            o_copy(j, k, at.me).wait_send()


def early_grads(xs_ref, g_ref, dwg_ref, dwu_ref, dwd_ref):
    q, ab = pl.program_id(0) // 2, lax.rem(pl.program_id(0), 2)
    h, da, db = (g_ref[q, ab, :, :, :, t].reshape(128, FC) for t in TENSORS)
    dwg_ref[...] = _dot(xs_ref[0], da, 0, 0)
    dwu_ref[...] = _dot(xs_ref[0], db, 0, 0)
    dwd_ref[...] = _dot(h, xs_ref[1], 0, 0)


def late_grads(y_ref, gx_ref, lwg, lwu, lwd, a_ref, b_ref, c_ref, yo_ref, gxo_ref, dwg_ref, dwu_ref, dwd_ref, sem, row_sem):
    copies = [pltpu.make_async_copy(y_ref, yo_ref, row_sem.at[0]), pltpu.make_async_copy(gx_ref, gxo_ref, row_sem.at[1])]
    for k in range(NB):
        src = pl.ds(k * 2 * FC, 2 * FC)
        dst = pl.ds((N1 + k) * 2 * FC, 2 * FC)
        copies += [pltpu.make_async_copy(lwg.at[:, src], dwg_ref.at[:, dst], sem.at[0, k]),
                   pltpu.make_async_copy(lwu.at[:, src], dwu_ref.at[:, dst], sem.at[1, k]),
                   pltpu.make_async_copy(lwd.at[src, :], dwd_ref.at[dst, :], sem.at[2, k])]
    for cp in copies:
        cp.start()
    for cp in copies:
        cp.wait()


def local_step(x_loc, wg_loc, wu_loc, wd_loc, gy_loc):
    vm = pl.BlockSpec(memory_space=pltpu.VMEM)
    hb = pl.BlockSpec(memory_space=pl.ANY)
    hbm = pl.BlockSpec(memory_space=pltpu.HBM)
    dma = pltpu.SemaphoreType.DMA
    row = jax.ShapeDtypeStruct((8, D), BF)
    kib = 1024
    half = (3, 2, 16, FC)
    xs, gat1, acc, rows, sx, sy, kx, ky, r2n = pl.pallas_call(
        first_kernel,
        out_shape=(pltpu.VMEM((2, 128, DL), BF), pltpu.VMEM((N1, 2, 2, 2, 2, 3, 16, FC), BF),
                   pltpu.VMEM((2, 16, 8, DL), F32), pltpu.VMEM((2, 8, D), BF),
                   pltpu.VMEM((NB - 1,) + half, F32), pltpu.VMEM((NB - 1,) + half, F32),
                   pltpu.VMEM((NB,) + half, F32), pltpu.VMEM((NB,) + half, F32), pltpu.VMEM((2,) + half, F32)),
        in_specs=[hbm] * 5,
        out_specs=(vm,) * 9,
        scratch_shapes=[
            pltpu.VMEM((NP, DL, 2 * FC), BF),
            pltpu.VMEM((NP, DL, 2 * FC), BF),
            pltpu.VMEM((NP, 2 * FC, DL), BF),
            pltpu.VMEM((NP, 2, 3, 2, 2, 16, FC), F32),
            pltpu.VMEM((N1, 2) + half, F32),
            pltpu.VMEM((8, 2, 8, DL), BF),
            pltpu.VMEM((16, 2, 8, DL), BF),
            pltpu.VMEM((2, 2, 2, 3, 2, 2, 16, FC), F32),
            pltpu.VMEM((N1, 2, 3, 16, FC), F32),
            dma((2,)), dma((3, NP)), dma((16,)), dma((16,)),
            dma((2, NP)), dma((2, NP)), dma((2, NS)), dma((2, NS)),
            dma((2, NP)), dma((2, NP)), dma((2, NS)), dma((2, NS)),
            dma((2, N1)), dma((2, N1)), dma((2, N1)), dma((2, N1)),
            dma((2, N1)), dma((2, N1)), dma((N1,)), dma((N1,)),
        ],
        compiler_params=pltpu.CompilerParams(
            collective_id=0, has_side_effects=True, vmem_limit_bytes=49000 * kib),
        name="mlp_first",
    )(x_loc, gy_loc, wg_loc, wu_loc, wd_loc)

    rx = lax.ppermute(sx, "dp", [(i, i + 2 if i % 4 < 2 else i - 2) for i in range(8)])
    ry = lax.ppermute(sy, "dp", [(i, (i + 4) % 8) for i in range(8)])

    full = (jax.ShapeDtypeStruct((DL, FF_LOC), F32), jax.ShapeDtypeStruct((DL, FF_LOC), F32),
            jax.ShapeDtypeStruct((FF_LOC, DL), F32))

    dwg, dwu, dwd = pl.pallas_call(
        early_grads,
        grid=(2 * N1,),
        out_shape=full,
        in_specs=[vm, vm],
        out_specs=(pl.BlockSpec((DL, FC), lambda k: (0, k)), pl.BlockSpec((DL, FC), lambda k: (0, k)),
                   pl.BlockSpec((FC, DL), lambda k: (k, 0))),
        cost_estimate=pl.CostEstimate(flops=12 * N1 * 128 * DL * FC, bytes_accessed=24 * N1 * DL * FC,
                                      transcendentals=0),
        compiler_params=pltpu.CompilerParams(dimension_semantics=("arbitrary",), vmem_limit_bytes=9000 * kib),
        name="mlp_early_grads",
    )(xs, gat1)

    y_rows, gx_rows, lwg, lwu, lwd = pl.pallas_call(
        second_kernel,
        out_shape=(pltpu.VMEM((8, D), BF), pltpu.VMEM((8, D), BF), pltpu.VMEM((DL, NB * 2 * FC), F32),
                   pltpu.VMEM((DL, NB * 2 * FC), F32), pltpu.VMEM((NB * 2 * FC, DL), F32)),
        in_specs=[hbm] * 3 + [vm] * 8,
        out_specs=(vm,) * 5,
        scratch_shapes=[
            pltpu.VMEM((NB, 2, 2, 2, 2, 3, 16, FC), BF),
            pltpu.VMEM((DL, NB * 2 * FC), BF),
            pltpu.VMEM((DL, NB * 2 * FC), BF),
            pltpu.VMEM((NB * 2 * FC, DL), BF),
            pltpu.VMEM((NB, 2) + half, F32),
            pltpu.VMEM((NB, 2, 3, 16, FC), F32),
            pltpu.VMEM((2, 16, 8, DL), F32),
            pltpu.VMEM((2, 16, 8, DL), F32),
            dma((3,)), dma((2, NB)), dma((2, NB)), dma((2, NB)), dma((2, NB)),
            dma((2, NB)), dma((2, NB)), dma((2, 3)), dma((2, 3)),
            dma((NB,)), dma((NB,)), dma((3,)), dma((3,)),
            dma((2, 16)), dma((2, 16)),
        ],
        compiler_params=pltpu.CompilerParams(
            collective_id=1, has_side_effects=True, vmem_limit_bytes=30000 * kib),
        name="mlp_second",
    )(wg_loc, wu_loc, wd_loc, xs, acc, rows, rx, ry, kx, ky, r2n)

    return pl.pallas_call(
        late_grads,
        out_shape=(row, row) + full,
        in_specs=[vm] * 5 + [hbm] * 3,
        out_specs=(hbm,) * 5,
        input_output_aliases={5: 2, 6: 3, 7: 4},
        scratch_shapes=[dma((3, NB)), dma((2,))],
        compiler_params=pltpu.CompilerParams(vmem_limit_bytes=30000 * kib),
        name="mlp_late_grads",
    )(y_rows, gx_rows, lwg, lwu, lwd, dwg, dwu, dwd)


def solution(mesh):
    row_spec = P(("dp", "tp"), None)
    up_spec = P("dp", "tp")
    down_spec = P("tp", "dp")
    return jax.shard_map(local_step, mesh=mesh,
                         in_specs=(row_spec, up_spec, up_spec, down_spec, row_spec),
                         out_specs=(row_spec, row_spec, up_spec, up_spec, down_spec),
                         check_vma=False)
```
